128 devices in a mesh: clusters: 128 (over z, y, x, core).
Axes of the slice: x: 4, y: 4, z: 4, core: 2. Of those that a mesh axis runs over, the one named last changes fastest.
Arguments:
- charges: bfloat16 [8, 524288], P(None, 'clusters'), may hold values from -6 to 6
- leaf_basis: bfloat16 [32, 524288], P(None, 'clusters'), may hold values from -0.75 to 0.75
- leaf_transfer: bfloat16 [1024, 64, 256], P('clusters'), may hold values from -0.375 to 0.375
- mid_transfer: bfloat16 [128, 64, 512], P('clusters'), may hold values from -0.25 to 0.25
- far_source: int32 [8192, 16], P('clusters'), may hold values from 0 to 8191, as said below
- far_coupling: bfloat16 [8192, 32, 512], P('clusters'), may hold values from -0.25 to 0.25
- mid_source: int32 [1024, 8], P('clusters'), may hold values from 0 to 1023, as said below
- mid_coupling: bfloat16 [1024, 64, 512], P('clusters'), may hold values from -0.25 to 0.25
- box_coupling: bfloat16 [128, 64, 192], P('clusters'), may hold values from -0.4375 to 0.4375
- top_transfer: bfloat16 [124, 64, 128], replicated, may hold values from -0.5 to 0.5
- top_coupling: bfloat16 [124, 64, 192], replicated, may hold values from -0.4375 to 0.4375
- near_target: int32 [131072], P('clusters'), may hold values from 0 to 63
- near_source: int32 [131072], P('clusters'), may hold values from 0 to 8191, as said below
- near_count: int32 [128], P('clusters'), may hold values from 256 to 1024, as said below
- near_blocks: bfloat16 [64, 8388608], P(None, 'clusters'), may hold values from -0.25 to 0.25
Outputs:
- potentials: bfloat16 [8, 524288], P(None, 'clusters')
The draws below stay inside these ranges and needn't reach their ends.
Inputs may be any that keep to these rules, and one draw needn't show every extreme that they name: `far_source`: each source leaf lies in the row's box or in a box whose index differs by one; for each box and each box beside it, the far lists of the box's leaves name exactly 4 distinct leaves of the box beside it. `mid_source`: each source cluster lies in the row's box or in a box whose index differs by one. `near_source`: each source leaf lies in the slot's box or in a box whose index differs by one. `near_count`: slots at or after a box's count are not used.
All inputs are finite; a program needn't handle non-finite values.
Results may differ from the reference program's by a relative error of at most 0.0053.
Values may be sent and summed in bfloat16 or wider, within the bound.
No kernel may reach another device: no remote copies, remote signals or barrier semaphores. Data moves between devices by JAX's collectives and lax.ppermute only.
A program may use at most 128 MiB of HBM per device.

```python
import jax
import jax.numpy as jnp
from jax import lax

M = 64
NV = 8
R0 = 32
R = 64
CHILD = 8
K0 = 16
K1 = 8
SLOT = 4
NB_CAP = 1024
BOXES = 128
LEAF_DEV = 64
NL = 8192
NL1 = 1024
POINTS = 524288
NBALL = 131072
LEVELS_TOP = 5
TOPS = 124


def shuffled(subkey, length):
    return jax.random.permutation(subkey, length).astype(jnp.int32)


def draw_far_source(key, part):
    devices = NL // LEAF_DEV
    entries = LEAF_DEV * K0
    kinds = 2 * SLOT
    key_sets, key_extra, key_mix = jax.random.split(jax.random.fold_in(key, 11), 3)
    scores = jax.random.randint(key_sets, (devices, 2, LEAF_DEV), 0, 1 << 20) * LEAF_DEV + jnp.arange(LEAF_DEV, dtype=jnp.int32)
    chosen = jnp.argsort(scores, axis=-1, stable=True)[:, :, :SLOT].astype(jnp.int32)
    forced = jnp.broadcast_to(jnp.arange(kinds, dtype=jnp.int32)[None, :], (devices, kinds))
    extra = jax.random.randint(key_extra, (devices, entries - kinds), 0, 2 * kinds + LEAF_DEV).astype(jnp.int32)
    pooled = jnp.concatenate([forced, extra], axis=1)
    mixing = jax.vmap(lambda subkey: shuffled(subkey, entries))(jax.random.split(key_mix, devices))
    pooled = jnp.take_along_axis(pooled, mixing, axis=1)
    rows = jnp.arange(devices, dtype=jnp.int32)[:, None]
    is_side = pooled < 2 * kinds
    code = pooled % kinds
    side = code // SLOT
    within = code % SLOT
    picked = chosen[rows, side, within]
    neighbour = rows + 2 * side - 1
    valid = is_side & (neighbour >= 0) & (neighbour < devices)
    own_leaf = jnp.where(is_side, picked, pooled - 2 * kinds)
    leaf = jnp.where(valid, neighbour * LEAF_DEV + picked, rows * LEAF_DEV + own_leaf)
    return leaf.reshape(NL, K0).astype(jnp.int32)


def draw_mid_source(key, part):
    devices = NL1 // CHILD
    key_step, key_box, key_mix = jax.random.split(key, 3)
    home = jnp.arange(NL1, dtype=jnp.int32)[:, None] // CHILD
    moves = jax.random.randint(key_step, (NL1, K1), -1, 2).astype(jnp.int32)
    column = jnp.arange(K1, dtype=jnp.int32)[None, :]
    moves = jnp.where(column == 0, -1, jnp.where(column == 1, 1, moves))
    mixing = jax.vmap(lambda subkey: shuffled(subkey, K1))(jax.random.split(key_mix, NL1))
    moves = jnp.take_along_axis(moves, mixing, axis=1)
    target = home + moves
    target = jnp.where(target < 0, home + 1, jnp.where(target >= devices, home - 1, target))
    inside = jax.random.randint(key_box, (NL1, K1), 0, CHILD).astype(jnp.int32)
    return (target * CHILD + inside).astype(jnp.int32)


def draw_near_source(key, part):
    devices = NBALL // NB_CAP
    key_step, key_leaf, key_place = jax.random.split(key, 3)
    home = jnp.arange(NBALL, dtype=jnp.int32) // NB_CAP
    position = jnp.arange(NBALL, dtype=jnp.int32) % NB_CAP
    anchor = jax.random.randint(key_place, (devices,), 0, max(NB_CAP // 4 - 1, 1)).astype(jnp.int32)[home]
    moves = jax.random.randint(key_step, (NBALL,), -1, 2).astype(jnp.int32)
    moves = jnp.where(position == anchor, -1, jnp.where(position == anchor + 1, 1, moves))
    target = home + moves
    target = jnp.where(target < 0, home + 1, jnp.where(target >= devices, home - 1, target))
    inside = jax.random.randint(key_leaf, (NBALL,), 0, LEAF_DEV).astype(jnp.int32)
    return (target * LEAF_DEV + inside).astype(jnp.int32)


def draw_near_count(key, part):
    devices = NBALL // NB_CAP
    key_base, key_top = jax.random.split(key)
    base = jax.random.randint(key_base, (devices,), NB_CAP // 4, NB_CAP // 2 + 1).astype(jnp.int32)
    fullest = jax.random.randint(key_top, (), 0, devices).astype(jnp.int32)
    index = jnp.arange(devices, dtype=jnp.int32)
    full = (index == fullest) | (index == devices - 1)
    return jnp.where(full, NB_CAP, base).astype(jnp.int32)


def place_ends(result, key, low, top_value):
    shape = result.shape
    place = [jax.random.randint(jax.random.fold_in(key, axis), (), 0, shape[axis]) for axis in range(len(shape))]
    result = result.at[tuple(place)].set(low)
    longest = shape.index(max(shape))
    place[longest] = (place[longest] + 1) % shape[longest]
    return result.at[tuple(place)].set(top_value)


def steps_of(rng, dims, cuts, smallest, top_value):
    def one(axis_at, blocks):
        heights = jax.random.uniform(jax.random.fold_in(jax.random.fold_in(rng, 6), axis_at), (blocks,), jnp.float32, smallest / len(cuts), top_value / len(cuts))
        return jnp.repeat(jnp.exp(heights), dims[axis_at] // blocks).reshape((-1,) + (1,) * (len(dims) - axis_at - 1))

    level = one(*cuts[0])
    for cut in cuts[1:]:
        level = level * one(*cut)
    return level


def normal_values(key, shape, width, bound, pieces=(), kind=jnp.bfloat16):
    result = jax.random.normal(key, shape, jnp.float32) * width
    if len(pieces) > 0:
        result = steps_of(key, shape, pieces, -0.22, 0.18) * result
    return jnp.clip(result, min=-bound, max=bound).astype(kind)


def setup_inputs(seed: int = 0) -> dict:
    key_list = jax.random.split(jax.random.key(seed), 16)
    charges = normal_values(key_list[0], (NV, POINTS), 1.0, 6.0, ((1, 128),))
    leaf_basis = normal_values(key_list[1], (R0, POINTS), M ** -0.5, 0.75, ((1, 128),))
    leaf_transfer = normal_values(key_list[2], (NL1, R, CHILD * R0), (CHILD * R0) ** -0.5, 0.375, ((0, 128),))
    mid_transfer = normal_values(key_list[3], (BOXES, R, CHILD * R), (CHILD * R) ** -0.5, 0.25, ((0, 128),))
    far_source = draw_far_source(jax.random.fold_in(key_list[15], 71), 0)
    far_coupling = normal_values(key_list[5], (NL, R0, K0 * R0), (K0 * R0) ** -0.5, 0.25, ((0, 128),))
    mid_source = draw_mid_source(jax.random.fold_in(key_list[15], 71), 0)
    mid_coupling = normal_values(key_list[7], (NL1, R, K1 * R), (K1 * R) ** -0.5, 0.25, ((0, 128),))
    box_coupling = normal_values(key_list[8], (BOXES, R, 3 * R), (3 * R) ** -0.5, 0.4375, ((0, 128),))
    top_transfer = normal_values(key_list[9], (TOPS, R, 2 * R), (2 * R) ** -0.5, 0.5)
    top_coupling = normal_values(key_list[10], (TOPS, R, 3 * R), (3 * R) ** -0.5, 0.4375)
    near_target = place_ends(jax.random.randint(key_list[11], (NBALL,), 0, LEAF_DEV), jax.random.fold_in(key_list[11], 1), 0, LEAF_DEV - 1).astype(jnp.int32)
    near_source = draw_near_source(jax.random.fold_in(key_list[15], 71), 0)
    near_count = draw_near_count(jax.random.fold_in(key_list[15], 71), 0)
    near_blocks = normal_values(key_list[14], (M, NBALL * M), (8 * M) ** -0.5, 0.25, ((1, 128),))
    return dict(charges=charges, leaf_basis=leaf_basis, leaf_transfer=leaf_transfer, mid_transfer=mid_transfer, far_source=far_source, far_coupling=far_coupling, mid_source=mid_source, mid_coupling=mid_coupling, box_coupling=box_coupling, top_transfer=top_transfer, top_coupling=top_coupling, near_target=near_target, near_source=near_source, near_count=near_count, near_blocks=near_blocks)


deepest_level = lax.Precision.HIGHEST


def level_partners(upward):
    count = upward.shape[0]
    padded = jnp.pad(upward, ((3, 3), (0, 0), (0, 0)))
    is_even = (jnp.arange(count) % 2 == 0)[:, None, None]
    back_three = padded[0:count]
    back_two = padded[1:count + 1]
    ahead_two = padded[5:count + 5]
    ahead_three = padded[6:count + 6]
    return jnp.concatenate([jnp.where(is_even, back_two, back_three), jnp.where(is_even, ahead_two, back_two), jnp.where(is_even, ahead_three, ahead_two)], axis=1)


def reference(charges, leaf_basis, leaf_transfer, mid_transfer, far_source, far_coupling, mid_source, mid_coupling, box_coupling, top_transfer, top_coupling, near_target, near_source, near_count, near_blocks):
    leaves = NL
    groups = NL1
    charge_cube = charges.reshape(NV, leaves, M).astype(jnp.float32)
    basis_tensor = leaf_basis.reshape(R0, leaves, M).astype(jnp.float32)
    leaf_up = jnp.einsum('rlm,vlm->lrv', basis_tensor, charge_cube, precision=deepest_level).astype(jnp.bfloat16)
    mid_up = jnp.einsum('crk,ckv->crv', leaf_transfer.astype(jnp.float32), leaf_up.reshape(groups, CHILD * R0, NV).astype(jnp.float32), precision=deepest_level).astype(jnp.bfloat16)
    box_up = jnp.einsum('drk,dkv->drv', mid_transfer.astype(jnp.float32), mid_up.reshape(BOXES, CHILD * R, NV).astype(jnp.float32), precision=deepest_level)
    upward = [box_up]
    for level in range(LEVELS_TOP):
        count = BOXES >> (level + 1)
        start = BOXES - (BOXES >> level)
        parents = top_transfer[start:start + count].astype(jnp.float32)
        upward.append(jnp.einsum('prk,pkv->prv', parents, upward[-1].reshape(count, 2 * R, NV), precision=deepest_level))
    across = []
    for level in range(LEVELS_TOP + 1):
        count = BOXES >> level
        if level == 0:
            matrix_stack = box_coupling
        else:
            start = BOXES - (BOXES >> (level - 1))
            matrix_stack = top_coupling[start:start + count]
        across.append(jnp.einsum('crk,ckv->crv', matrix_stack.astype(jnp.float32), level_partners(upward[level]), precision=deepest_level))
    downward = across[LEVELS_TOP]
    for level in range(LEVELS_TOP - 1, -1, -1):
        count = BOXES >> (level + 1)
        start = BOXES - (BOXES >> level)
        parents = top_transfer[start:start + count].astype(jnp.float32)
        pushed = jnp.einsum('prk,prv->pkv', parents, downward, precision=deepest_level).reshape(2 * count, R, NV)
        downward = across[level] + pushed
    box_down = downward.astype(jnp.bfloat16)
    mid_picked = mid_up[mid_source].reshape(groups, K1 * R, NV).astype(jnp.float32)
    mid_far = jnp.einsum('crk,ckv->crv', mid_coupling.astype(jnp.float32), mid_picked, precision=deepest_level)
    mid_push = jnp.einsum('drk,drv->dkv', mid_transfer.astype(jnp.float32), box_down.astype(jnp.float32), precision=deepest_level).reshape(groups, R, NV)
    mid_down = (mid_far + mid_push).astype(jnp.bfloat16)
    leaf_picked = leaf_up[far_source].reshape(leaves, K0 * R0, NV).astype(jnp.float32)
    leaf_far = jnp.einsum('lrk,lkv->lrv', far_coupling.astype(jnp.float32), leaf_picked, precision=deepest_level)
    leaf_push = jnp.einsum('crk,crv->ckv', leaf_transfer.astype(jnp.float32), mid_down.astype(jnp.float32), precision=deepest_level).reshape(leaves, R0, NV)
    leaf_down = (leaf_far + leaf_push).astype(jnp.bfloat16)
    far_field = jnp.einsum('rlm,lrv->vlm', basis_tensor, leaf_down.astype(jnp.float32), precision=deepest_level)
    block = min(1024, NBALL)
    owners = jnp.arange(NBALL, dtype=jnp.int32) // NB_CAP
    alive = (jnp.arange(NBALL, dtype=jnp.int32) % NB_CAP) < near_count[owners]
    targets = (owners * LEAF_DEV + near_target).astype(jnp.int32)

    def near_step(step, total):
        first = (step * block).astype(jnp.int32)
        sources = lax.dynamic_slice_in_dim(near_source, first, block)
        dests = lax.dynamic_slice_in_dim(targets, first, block)
        weights = lax.dynamic_slice_in_dim(alive, first, block).astype(jnp.float32)
        dense = lax.dynamic_slice_in_dim(near_blocks, (first * M).astype(jnp.int32), block * M, 1).reshape(M, block, M).astype(jnp.float32)
        gathered = jnp.take(charge_cube, sources, axis=1)
        contribution = jnp.einsum('tbs,vbs->vbt', dense, gathered, precision=deepest_level) * weights[None, :, None]
        return total.at[:, dests, :].add(contribution)

    near_field = lax.fori_loop(0, NBALL // block, near_step, jnp.zeros((NV, leaves, M), jnp.float32))
    return (far_field + near_field).astype(jnp.bfloat16).reshape(NV, POINTS)
```

```python
import jax
import jax.numpy as jnp
from jax import lax
from jax.experimental import pallas as pl
from jax.experimental.pallas import tpu as pltpu
from jax.sharding import PartitionSpec as P

F32 = jnp.float32
BF16 = jnp.bfloat16

VECTORS = 8
LEAVES = 64
CAPACITY = 64
RANK_LEAF = 32
RANK = 64
GROUPS = 8
CHILDREN = 8
FAR = 16
MID_FAR = 8
SLOTS = 1024
BOXES = 128
LEVELS = 5
POINTS = LEAVES * CAPACITY
LEAF_LANES = LEAVES * RANK_LEAF
MID_LANES = GROUPS * RANK
PARTS = 8
PART = SLOTS * CAPACITY // PARTS
STEP = 16
LANES = 128


def dot_nt(left, right):
    return lax.dot_general(left, right, (((1,), (1,)), ((), ())), preferred_element_type=F32)


def dot_nn(left, right):
    return lax.dot_general(left, right, (((1,), (0,)), ((), ())), preferred_element_type=F32)


def lane_index(shape):
    return lax.broadcasted_iota(jnp.int32, shape, len(shape) - 1)


def pick_two(lane, first, second):
    return jnp.where(lane < 64, first, second)


def pick_four(lane, a, b, c, d):
    return jnp.where(lane < 64, jnp.where(lane < 32, a, b), jnp.where(lane < 96, c, d))


def up_kernel(charges, basis, leaf_transfer, mid_transfer, coefficients, message):
    lane = lane_index((VECTORS, LANES))
    wide_lane = lane_index((VECTORS, 4 * CAPACITY)) // CAPACITY
    tiles = []
    for g in range(LEAVES // 4):
        span = pl.ds(g * 4 * CAPACITY, 4 * CAPACITY)
        x = charges[:, span].astype(F32)
        rows = jnp.concatenate([jnp.where(wide_lane == j, x, 0.0) for j in range(4)], axis=0)
        b = basis[:, span]
        result = dot_nt(rows.astype(BF16), jnp.concatenate([b, b, b, b], axis=0))
        tiles.append(
            pick_four(lane, *[result[j * VECTORS : (j + 1) * VECTORS] for j in range(4)])
        )
    for g in range(LEAVES // 4):
        coefficients[:, pl.ds(g * LANES, LANES)] = tiles[g].astype(BF16)
    stacked = jnp.concatenate(
        [jnp.concatenate([tiles[2 * c], tiles[2 * c + 1]], axis=1) for c in range(GROUPS)], axis=0
    ).astype(BF16)
    result = dot_nt(stacked, leaf_transfer[...].reshape(GROUPS * RANK, CHILDREN * RANK_LEAF))
    mid = []
    for h in range(GROUPS // 2):
        span = slice(h * LANES, (h + 1) * LANES)
        low = result[16 * h : 16 * h + 8, span]
        high = result[16 * h + 8 : 16 * h + 16, span]
        mid.append(pick_two(lane, low, high).astype(BF16))
        coefficients[:, pl.ds(LEAF_LANES + h * LANES, LANES)] = mid[h]
    box = dot_nt(jnp.concatenate(mid, axis=1), mid_transfer[0])
    box = jnp.concatenate([box, box], axis=1).astype(BF16)
    message[...] = jnp.broadcast_to(box[None], message.shape)


def main_kernel(
    near_source,
    near_target,
    near_count,
    far_source,
    mid_source,
    charges_own,
    charges_pair,
    charges_other,
    coef_own,
    coef_pair,
    coef_other,
    every,
    basis_hbm,
    leaf_transfer_hbm,
    mid_transfer_hbm,
    far_hbm,
    mid_far_hbm,
    box_coupling_hbm,
    top_transfer_hbm,
    top_coupling_hbm,
    near_hbm,
    out,
    x_low,
    x_high,
    leaf_table,
    mid_table,
    acc0,
    acc1,
    acc2,
    acc3,
    leaf_far,
    pairs0,
    pairs1,
    pairs2,
    pairs3,
    pairs4,
    pairs5,
    near,
    basis,
    leaf_transfer,
    mid_transfer,
    far,
    mid_coupling,
    coupling,
    top_transfer,
    near_sem,
    far_sem,
    sem,
    coupling_sem,
):
    device = lax.axis_index("clusters")
    near_copies = [
        pltpu.make_async_copy(
            near_hbm.at[:, pl.ds(k * PART, PART)], near.at[k], near_sem.at[k]
        )
        for k in range(PARTS)
    ]
    far_copy = pltpu.make_async_copy(far_hbm, far, far_sem)
    copies = [
        pltpu.make_async_copy(source, target, sem.at[i])
        for i, (source, target) in enumerate(
            (
                (top_transfer_hbm, top_transfer),
                (mid_far_hbm, mid_coupling),
                (leaf_transfer_hbm, leaf_transfer),
                (mid_transfer_hbm, mid_transfer),
                (basis_hbm, basis),
            )
        )
    ]
    coupling_copies = [pltpu.make_async_copy(box_coupling_hbm.at[0], coupling.at[0], coupling_sem.at[0])]
    for level in range(1, LEVELS + 1):
        start = BOXES - (BOXES >> (level - 1))
        coupling_copies.append(
            pltpu.make_async_copy(
                top_coupling_hbm.at[start + (device >> level)],
                coupling.at[level],
                coupling_sem.at[level],
            )
        )
    copies[0].start()
    for copy in coupling_copies:
        copy.start()
    far_copy.start()
    copies[1].start()
    for copy in near_copies:
        copy.start()
    for copy in copies[2:]:
        copy.start()

    lane = lane_index((VECTORS, LANES))
    zero = jnp.zeros((VECTORS, LANES), F32)
    odd = device % 2
    pair_at = (1 - odd) * 2
    other_at = odd * 2

    def fill_charges(source, region):
        base = region * LEAVES
        for h in range(LEAVES // 2):
            tile = source[:, pl.ds(h * LANES, LANES)].astype(F32)
            turned = pltpu.roll(tile, 64, 1)
            x_low[base + 2 * h] = pick_two(lane, tile, zero)
            x_high[base + 2 * h] = pick_two(lane, zero, turned)
            x_low[base + 2 * h + 1] = pick_two(lane, turned, zero)
            x_high[base + 2 * h + 1] = pick_two(lane, zero, tile)

    def fill_coefficients(source, region):
        base = region * LEAVES
        for h in range(LEAVES // 4):
            tile = source[:, pl.ds(h * LANES, LANES)].astype(F32)
            turns = [tile] + [pltpu.roll(tile, 32 * i, 1) for i in range(1, 4)]
            for j in range(4):
                leaf_table[base + 4 * h + j] = pick_four(
                    lane, *[turns[(group - j) % 4] for group in range(4)]
                )
        base = region * GROUPS
        for h in range(GROUPS // 2):
            tile = source[:, pl.ds(LEAF_LANES + h * LANES, LANES)].astype(F32)
            turned = pltpu.roll(tile, 64, 1)
            mid_table[base + 2 * h] = pick_two(lane, tile, turned)
            mid_table[base + 2 * h + 1] = pick_two(lane, turned, tile)

    copies[0].wait()
    pairs = (pairs0, pairs1, pairs2, pairs3, pairs4, pairs5)
    for level in range(LEVELS + 1):
        pairs[level][0] = zero
        pairs[level][(BOXES >> (level + 1)) + 1] = zero
    for p in range(BOXES // 2):
        pairs0[p + 1] = pick_two(lane, every[2 * p].astype(F32), every[2 * p + 1].astype(F32))
    for level in range(LEVELS):
        start = BOXES - (BOXES >> level)
        for g in range(BOXES >> (level + 3)):
            rows = pairs[level][pl.ds(1 + 4 * g, 4)].reshape(4 * VECTORS, LANES).astype(BF16)
            matrices = top_transfer[pl.ds(start + 4 * g, 4)].reshape(4 * RANK, 2 * RANK)
            result = dot_nt(rows, matrices)
            pairs[level + 1][1 + 2 * g] = pick_two(lane, result[0:8, 0:128], result[8:16, 0:128])
            pairs[level + 1][2 + 2 * g] = pick_two(
                lane, result[16:24, 128:256], result[24:32, 128:256]
            )
    for copy in coupling_copies:
        copy.wait()
    across = []
    for level in range(LEVELS + 1):
        cluster = device >> level
        parent = cluster >> 1
        before = pairs[level][parent]
        after = pltpu.roll(pairs[level][parent + 2], 64, 1)
        middle = jnp.where((cluster & 1) == 1, before, after)
        stacked = jnp.concatenate([pick_two(lane, before, middle), after[:, :64]], axis=1)
        across.append(dot_nt(stacked.astype(BF16), coupling[level]))
    down = across[LEVELS]
    for level in range(LEVELS - 1, -1, -1):
        cluster = device >> level
        start = BOXES - (BOXES >> level)
        pushed = dot_nn(down.astype(BF16), top_transfer[start + (cluster >> 1)])
        pushed = jnp.where((cluster & 1) == 1, pltpu.roll(pushed, 64, 1), pushed)
        down = across[level] + pushed[:, :64]
    box_down = down.astype(BF16)

    fill_coefficients(coef_own, 1)
    fill_coefficients(coef_pair, pair_at)
    fill_coefficients(coef_other, other_at)
    copies[1].wait()
    mid_base = (device - 1) * GROUPS
    rows = []
    for c in range(GROUPS):
        rows.append(
            jnp.concatenate(
                [
                    pick_two(
                        lane,
                        mid_table[mid_source[c, 2 * q] - mid_base],
                        mid_table[mid_source[c, 2 * q + 1] - mid_base],
                    )
                    for q in range(MID_FAR // 2)
                ],
                axis=1,
            )
        )
    mid_result = dot_nt(
        jnp.concatenate(rows, axis=0).astype(BF16),
        mid_coupling[...].reshape(GROUPS * RANK, MID_FAR * RANK),
    )
    copies[3].wait()
    mid_push = dot_nn(box_down, mid_transfer[0])
    mid_down = []
    for h in range(GROUPS // 2):
        span = slice(h * LANES, (h + 1) * LANES)
        far_tile = pick_two(
            lane, mid_result[16 * h : 16 * h + 8, span], mid_result[16 * h + 8 : 16 * h + 16, span]
        )
        mid_down.append((far_tile + mid_push[:, span]).astype(BF16).astype(F32))

    leaf_base = (device - 1) * LEAVES
    far_copy.wait()

    def far_step(group, carry):
        rows = []
        for i in range(8):
            leaf = group * 8 + i
            rows.append(
                jnp.concatenate(
                    [
                        pick_four(
                            lane,
                            *[
                                leaf_table[far_source[leaf, 4 * q + m] - leaf_base]
                                for m in range(4)
                            ],
                        )
                        for q in range(FAR // 4)
                    ],
                    axis=1,
                )
            )
        result = dot_nt(
            jnp.concatenate(rows, axis=0).astype(BF16),
            far[pl.ds(group * 8, 8)].reshape(8 * RANK_LEAF, FAR * RANK_LEAF),
        )
        for h in range(2):
            leaf_far[group * 2 + h] = pick_four(
                lane,
                *[
                    result[(4 * h + j) * 8 : (4 * h + j + 1) * 8, h * LANES : (h + 1) * LANES]
                    for j in range(4)
                ],
            )
        return carry

    lax.fori_loop(0, LEAVES // 8, far_step, 0)

    fill_charges(charges_own, 1)
    fill_charges(charges_pair, pair_at)
    fill_charges(charges_other, other_at)
    accumulators = (acc0, acc1, acc2, acc3)
    for acc in accumulators:
        acc[...] = jnp.zeros(acc.shape, F32)
    live = near_count[0]
    per_part = SLOTS // PARTS
    zeros_half = jnp.zeros((2 * VECTORS, LANES), BF16)

    for k in range(PARTS):
        near_copies[k].wait()
        steps = jnp.clip((live - k * per_part + STEP - 1) // STEP, 0, per_part // STEP)

        def near_step(step, carry, k=k):
            first = k * per_part + step * STEP
            for i in range(STEP // 4):
                sources = [near_source[first + 4 * i + j] - leaf_base for j in range(4)]
                top = jnp.concatenate([x_low[sources[0]], x_high[sources[1]]], axis=0)
                bottom = jnp.concatenate([x_low[sources[2]], x_high[sources[3]]], axis=0)
                rows = jnp.concatenate(
                    [
                        jnp.concatenate([top.astype(BF16), zeros_half], axis=1),
                        jnp.concatenate([zeros_half, bottom.astype(BF16)], axis=1),
                    ],
                    axis=0,
                )
                at = pl.multiple_of((step * STEP + 4 * i) * CAPACITY, 4 * CAPACITY)
                result = dot_nt(rows, near[k, :, pl.ds(at, 4 * CAPACITY)])
                for j in range(4):
                    slot = first + 4 * i + j
                    target = jnp.where(slot < live, near_target[slot], LEAVES)
                    accumulators[j][target] += result[j * 8 : (j + 1) * 8]
            return carry

        lax.fori_loop(0, steps, near_step, 0)

    copies[2].wait()
    rows = []
    for c in range(GROUPS):
        tile = mid_down[c // 2]
        half = pick_two(lane, tile, zero) if c % 2 == 0 else pick_two(lane, zero, tile)
        rows.append(
            jnp.concatenate([half if h == c // 2 else zero for h in range(GROUPS // 2)], axis=1)
        )
    leaf_push = dot_nn(
        jnp.concatenate(rows, axis=0).astype(BF16),
        leaf_transfer[...].reshape(GROUPS * RANK, CHILDREN * RANK_LEAF),
    )
    copies[4].wait()
    lane_group = lane // RANK_LEAF
    for g in range(LEAVES // 4):
        push = leaf_push[(g // 2) * 8 : (g // 2) * 8 + 8, (g % 2) * LANES : (g % 2 + 1) * LANES]
        leaf_down = leaf_far[g] + push
        rows = jnp.concatenate(
            [jnp.where(lane_group == j, leaf_down, 0.0) for j in range(4)], axis=0
        ).astype(BF16)
        b = basis[:, pl.ds(g * 4 * CAPACITY, 4 * CAPACITY)]
        result = dot_nn(rows, jnp.concatenate([b, b, b, b], axis=0))
        for h in range(2):
            span = slice(h * LANES, (h + 1) * LANES)
            far_tile = pick_two(
                lane, result[16 * h : 16 * h + 8, span], result[16 * h + 8 : 16 * h + 16, span]
            )
            leaf = 4 * g + 2 * h
            low = acc0[leaf] + acc1[leaf] + (acc2[leaf] + acc3[leaf])
            high = acc0[leaf + 1] + acc1[leaf + 1] + (acc2[leaf + 1] + acc3[leaf + 1])
            near_tile = jnp.concatenate([low, high], axis=1)
            out[:, pl.ds((2 * g + h) * LANES, LANES)] = (far_tile + near_tile).astype(BF16)


def body(
    charges,
    leaf_basis,
    leaf_transfer,
    mid_transfer,
    far_source,
    far_coupling,
    mid_source,
    mid_coupling,
    box_coupling,
    top_transfer,
    top_coupling,
    near_target,
    near_source,
    near_count,
    near_blocks,
):
    pair = [(i, i ^ 1) for i in range(BOXES)]
    other = [(i, min(max(((i + 1) ^ 1) - 1, 0), BOXES - 1)) for i in range(BOXES)]
    charges_pair = lax.ppermute(charges, "clusters", pair)
    charges_other = lax.ppermute(charges, "clusters", other)
    vmem = pl.BlockSpec(memory_space=pltpu.VMEM)
    smem = pl.BlockSpec(memory_space=pltpu.SMEM)
    anywhere = pl.BlockSpec(memory_space=pl.ANY)
    coefficients, message = pl.pallas_call(
        up_kernel,
        out_shape=(
            jax.ShapeDtypeStruct((VECTORS, LEAF_LANES + MID_LANES), BF16),
            jax.ShapeDtypeStruct((BOXES, VECTORS, LANES), BF16),
        ),
        in_specs=[vmem] * 4,
        out_specs=(vmem, vmem),
        cost_estimate=pl.CostEstimate(flops=10**9, bytes_accessed=10**6, transcendentals=0),
        name="upward",
    )(charges, leaf_basis, leaf_transfer, mid_transfer)
    coef_pair = lax.ppermute(coefficients, "clusters", pair)
    coef_other = lax.ppermute(coefficients, "clusters", other)
    every = lax.all_to_all(message, "clusters", 0, 0)
    table = pltpu.VMEM((3 * LEAVES, VECTORS, LANES), F32)
    accumulator = pltpu.VMEM((LEAVES + 1, VECTORS, CAPACITY), F32)
    return pl.pallas_call(
        main_kernel,
        out_shape=jax.ShapeDtypeStruct((VECTORS, POINTS), BF16),
        in_specs=[smem] * 5 + [vmem] * 7 + [anywhere] * 9,
        out_specs=vmem,
        scratch_shapes=[
            table,
            table,
            table,
            pltpu.VMEM((3 * GROUPS, VECTORS, LANES), F32),
            accumulator,
            accumulator,
            accumulator,
            accumulator,
            pltpu.VMEM((LEAVES // 4, VECTORS, LANES), F32),
        ]
        + [
            pltpu.VMEM(((BOXES >> (level + 1)) + 2, VECTORS, LANES), F32)
            for level in range(LEVELS + 1)
        ]
        + [
            pltpu.VMEM((PARTS, CAPACITY, PART), BF16),
            pltpu.VMEM((RANK_LEAF, POINTS), BF16),
            pltpu.VMEM((GROUPS, RANK, CHILDREN * RANK_LEAF), BF16),
            pltpu.VMEM((1, RANK, GROUPS * RANK), BF16),
            pltpu.VMEM((LEAVES, RANK_LEAF, FAR * RANK_LEAF), BF16),
            pltpu.VMEM((GROUPS, RANK, MID_FAR * RANK), BF16),
            pltpu.VMEM((LEVELS + 1, RANK, 3 * RANK), BF16),
            pltpu.VMEM((BOXES - 4, RANK, 2 * RANK), BF16),
            pltpu.SemaphoreType.DMA((PARTS,)),
            pltpu.SemaphoreType.DMA,
            pltpu.SemaphoreType.DMA((5,)),
            pltpu.SemaphoreType.DMA((LEVELS + 1,)),
        ],
        cost_estimate=pl.CostEstimate(flops=10**9, bytes_accessed=10**7, transcendentals=0),
        compiler_params=pltpu.CompilerParams(vmem_limit_bytes=48 * 1024 * 1024),
        name="main",
    )(
        near_source,
        near_target,
        near_count,
        far_source,
        mid_source,
        charges,
        charges_pair,
        charges_other,
        coefficients,
        coef_pair,
        coef_other,
        every,
        leaf_basis,
        leaf_transfer,
        mid_transfer,
        far_coupling,
        mid_coupling,
        box_coupling,
        top_transfer,
        top_coupling,
        near_blocks,
    )


def solution(mesh):
    in_specs = (
        P(None, "clusters"),
        P(None, "clusters"),
        P("clusters", None, None),
        P("clusters", None, None),
        P("clusters", None),
        P("clusters", None, None),
        P("clusters", None),
        P("clusters", None, None),
        P("clusters", None, None),
        P(),
        P(),
        P("clusters"),
        P("clusters"),
        P("clusters"),
        P(None, "clusters"),
    )
    out_specs = P(None, "clusters")
    return jax.shard_map(body, mesh=mesh, in_specs=in_specs, out_specs=out_specs, check_vma=False)
```

```python
import jax
import jax.numpy as jnp
from jax import lax
from jax.experimental import pallas as pl
from jax.experimental.pallas import tpu as pltpu
from jax.sharding import PartitionSpec as P

F32 = jnp.float32
BF16 = jnp.bfloat16

VECTORS = 8
LEAVES = 64
CAPACITY = 64
RANK_LEAF = 32
RANK = 64
GROUPS = 8
CHILDREN = 8
FAR = 16
MID_FAR = 8
SLOTS = 1024
BOXES = 128
LEVELS = 5
POINTS = LEAVES * CAPACITY
LEAF_LANES = LEAVES * RANK_LEAF
MID_LANES = GROUPS * RANK
PARTS = 8
PART = SLOTS * CAPACITY // PARTS
BLOCK = SLOTS // PARTS
WIDE = POINTS + LEAF_LANES + MID_LANES
LANES = 128
VMEM_LIMIT = 60 * 1024 * 1024


def dot_nt(left, right):
    return lax.dot_general(left, right, (((1,), (1,)), ((), ())), preferred_element_type=F32)


def dot_nn(left, right):
    return lax.dot_general(left, right, (((1,), (0,)), ((), ())), preferred_element_type=F32)


def lane_index(shape):
    return lax.broadcasted_iota(jnp.int32, shape, len(shape) - 1)


def pick_two(lane, first, second):
    return jnp.where(lane < 64, first, second)


def pick_four(lane, a, b, c, d):
    return jnp.where(lane < 64, jnp.where(lane < 32, a, b), jnp.where(lane < 96, c, d))


def up_kernel(
    charges, basis, leaf_hbm, mid_hbm, packed, message, leaf_transfer, mid_transfer, sem
):
    leaf_copy = pltpu.make_async_copy(leaf_hbm, leaf_transfer, sem.at[0])
    mid_copy = pltpu.make_async_copy(mid_hbm, mid_transfer, sem.at[1])
    leaf_copy.start()
    mid_copy.start()
    lane = lane_index((VECTORS, LANES))
    wide_lane = lane_index((VECTORS, 4 * CAPACITY)) // CAPACITY
    packed[:, pl.ds(0, POINTS)] = charges[...]
    tiles = []
    for g in range(LEAVES // 4):
        span = pl.ds(g * 4 * CAPACITY, 4 * CAPACITY)
        x = charges[:, span].astype(F32)
        rows = jnp.concatenate([jnp.where(wide_lane == j, x, 0.0) for j in range(4)], axis=0)
        b = basis[:, span]
        result = dot_nt(rows.astype(BF16), jnp.concatenate([b, b, b, b], axis=0))
        tiles.append(
            pick_four(lane, *[result[j * VECTORS : (j + 1) * VECTORS] for j in range(4)])
        )
    for g in range(LEAVES // 4):
        packed[:, pl.ds(POINTS + g * LANES, LANES)] = tiles[g].astype(BF16)
    stacked = jnp.concatenate(
        [jnp.concatenate([tiles[2 * c], tiles[2 * c + 1]], axis=1) for c in range(GROUPS)], axis=0
    ).astype(BF16)
    leaf_copy.wait()
    result = dot_nt(stacked, leaf_transfer[...].reshape(GROUPS * RANK, CHILDREN * RANK_LEAF))
    mid = []
    for h in range(GROUPS // 2):
        span = slice(h * LANES, (h + 1) * LANES)
        low = result[16 * h : 16 * h + 8, span]
        high = result[16 * h + 8 : 16 * h + 16, span]
        mid.append(pick_two(lane, low, high).astype(BF16))
        packed[:, pl.ds(POINTS + LEAF_LANES + h * LANES, LANES)] = mid[h]
    mid_copy.wait()
    box = dot_nt(jnp.concatenate(mid, axis=1), mid_transfer[0])
    box = jnp.concatenate([box, box], axis=1).astype(BF16)
    message[...] = jnp.broadcast_to(box[None], message.shape)


def side_kernel(
    near_source,
    near_target,
    near_count,
    far_source,
    mid_source,
    own,
    pair,
    other,
    far_hbm,
    mid_far_hbm,
    top_coupling_hbm,
    near_hbm,
    near_out,
    leaf_far,
    mid_far,
    coupling,
    x_low,
    x_high,
    leaf_table,
    mid_table,
    acc0,
    acc1,
    acc2,
    acc3,
    chosen_low,
    chosen_high,
    near,
    far,
    mid_coupling,
    top_coupling,
    source_rows,
    target_rows,
    far_rows,
    mid_rows,
    near_from,
    near_to,
    far_from,
    mid_from,
    near_sem,
    sem,
    index_sem,
):
    device = lax.axis_index("clusters")

    def near_copy(k):
        return pltpu.make_async_copy(
            near_hbm.at[:, pl.ds(pl.multiple_of(k * PART, PART), PART)], near.at[k], near_sem.at[k]
        )

    far_copy = pltpu.make_async_copy(far_hbm, far, sem.at[0])
    mid_copy = pltpu.make_async_copy(mid_far_hbm, mid_coupling, sem.at[1])
    top_copy = pltpu.make_async_copy(top_coupling_hbm, top_coupling, sem.at[2])
    for k in range(PARTS):
        near_copy(k).start()
    far_copy.start()
    mid_copy.start()
    top_copy.start()

    live = near_count[0]
    leaf_base = (device - 1) * LEAVES
    shape = (VECTORS, LANES)
    slot = lax.broadcasted_iota(jnp.int32, shape, 0) * LANES + lane_index(shape)
    used = slot < live
    source_rows[...] = jnp.where(used, near_source[...] - leaf_base, LEAVES) * VECTORS
    target_rows[...] = jnp.where(used, near_target[...], LEAVES) * VECTORS
    far_rows[...] = (far_source[...] - leaf_base) * VECTORS
    mid_rows[...] = (mid_source[...] - (device - 1) * GROUPS) * VECTORS
    index_copies = [
        pltpu.make_async_copy(a, b, index_sem.at[i])
        for i, (a, b) in enumerate(
            (
                (source_rows, near_from),
                (target_rows, near_to),
                (far_rows, far_from),
                (mid_rows, mid_from),
            )
        )
    ]
    for copy in index_copies:
        copy.start()

    lane = lane_index((VECTORS, LANES))
    zero = jnp.zeros((VECTORS, LANES), F32)
    odd = device % 2

    def rows_of(first):
        return pl.ds(pl.multiple_of(first, VECTORS), VECTORS)

    for source, region in ((own, 1), (pair, (1 - odd) * 2), (other, odd * 2)):
        base = region * LEAVES * VECTORS
        for h in range(LEAVES // 2):
            tile = source[:, pl.ds(h * LANES, LANES)].astype(F32)
            turned = pltpu.roll(tile, 64, 1)
            at = base + 2 * h * VECTORS
            x_low[rows_of(at), :] = pick_two(lane, tile, zero)
            x_high[rows_of(at), :] = pick_two(lane, zero, turned)
            x_low[rows_of(at + VECTORS), :] = pick_two(lane, turned, zero)
            x_high[rows_of(at + VECTORS), :] = pick_two(lane, zero, tile)
        for h in range(LEAVES // 4):
            tile = source[:, pl.ds(POINTS + h * LANES, LANES)].astype(F32)
            turns = [tile] + [pltpu.roll(tile, 32 * i, 1) for i in range(1, 4)]
            for j in range(4):
                leaf_table[rows_of(base + (4 * h + j) * VECTORS), :] = pick_four(
                    lane, *[turns[(group - j) % 4] for group in range(4)]
                )
        base = region * GROUPS * VECTORS
        for h in range(GROUPS // 2):
            tile = source[:, pl.ds(POINTS + LEAF_LANES + h * LANES, LANES)].astype(F32)
            turned = pltpu.roll(tile, 64, 1)
            at = base + 2 * h * VECTORS
            mid_table[rows_of(at), :] = pick_two(lane, tile, turned)
            mid_table[rows_of(at + VECTORS), :] = pick_two(lane, turned, tile)
    accumulators = (acc0, acc1, acc2, acc3)
    for acc in accumulators:
        acc[...] = jnp.zeros(acc.shape, F32)
    for copy in index_copies:
        copy.wait()

    zeros_half = jnp.zeros((2 * VECTORS, LANES), BF16)
    blocks = (live + BLOCK - 1) // BLOCK

    def near_step(k, carry):
        near_copy(k).wait()
        for i in range(BLOCK // 4):
            at = [rows_of(near_from[k, 4 * i + j]) for j in range(4)]
            top = jnp.concatenate([x_low[at[0], :], x_high[at[1], :]], axis=0)
            bottom = jnp.concatenate([x_low[at[2], :], x_high[at[3], :]], axis=0)
            rows = jnp.concatenate(
                [
                    jnp.concatenate([top.astype(BF16), zeros_half], axis=1),
                    jnp.concatenate([zeros_half, bottom.astype(BF16)], axis=1),
                ],
                axis=0,
            )
            result = dot_nt(rows, near[k, :, 4 * i * CAPACITY : 4 * (i + 1) * CAPACITY])
            for j in range(4):
                to = rows_of(near_to[k, 4 * i + j])
                accumulators[j][to, :] += result[j * 8 : (j + 1) * 8]
        return carry

    lax.fori_loop(0, blocks, near_step, 0)

    def unused_step(k, carry):
        near_copy(k).wait()
        return carry

    lax.fori_loop(blocks, PARTS, unused_step, 0)
    for h in range(LEAVES // 2):
        low = rows_of(2 * h * VECTORS)
        high = rows_of((2 * h + 1) * VECTORS)
        near_out[:, pl.ds(h * LANES, LANES)] = jnp.concatenate(
            [
                acc0[low, :] + acc1[low, :] + (acc2[low, :] + acc3[low, :]),
                acc0[high, :] + acc1[high, :] + (acc2[high, :] + acc3[high, :]),
            ],
            axis=1,
        )

    far_copy.wait()
    for group in range(LEAVES // 8):
        rows = []
        for i in range(8):
            leaf = group * 8 + i
            rows.append(
                jnp.concatenate(
                    [
                        pick_four(
                            lane,
                            *[leaf_table[rows_of(far_from[4 * q + m, leaf]), :] for m in range(4)],
                        )
                        for q in range(FAR // 4)
                    ],
                    axis=1,
                )
            )
        result = dot_nt(
            jnp.concatenate(rows, axis=0).astype(BF16),
            far[group * 8 : group * 8 + 8].reshape(8 * RANK_LEAF, FAR * RANK_LEAF),
        )
        for h in range(2):
            leaf_far[group * 2 + h] = pick_four(
                lane,
                *[
                    result[(4 * h + j) * 8 : (4 * h + j + 1) * 8, h * LANES : (h + 1) * LANES]
                    for j in range(4)
                ],
            )
    mid_copy.wait()
    rows = []
    for c in range(GROUPS):
        rows.append(
            jnp.concatenate(
                [
                    pick_two(
                        lane,
                        mid_table[rows_of(mid_from[c, 2 * q]), :],
                        mid_table[rows_of(mid_from[c, 2 * q + 1]), :],
                    )
                    for q in range(MID_FAR // 2)
                ],
                axis=1,
            )
        )
    result = dot_nt(
        jnp.concatenate(rows, axis=0).astype(BF16),
        mid_coupling[...].reshape(GROUPS * RANK, MID_FAR * RANK),
    )
    for h in range(GROUPS // 2):
        span = slice(h * LANES, (h + 1) * LANES)
        mid_far[h] = pick_two(
            lane, result[16 * h : 16 * h + 8, span], result[16 * h + 8 : 16 * h + 16, span]
        )

    top_copy.wait()
    tops = top_coupling.shape[2]
    level = lax.broadcasted_iota(jnp.int32, (VECTORS, tops), 0) + 1
    column = BOXES - lax.shift_right_logical(jnp.full_like(level, BOXES), level - 1)
    column = column + lax.shift_right_logical(jnp.full_like(level, 1) * device, level)
    wanted = (lane_index((VECTORS, tops)) == column).astype(F32).astype(BF16)
    for r in range(RANK):
        result = dot_nt(wanted, top_coupling[r])
        chosen_low[r * VECTORS : (r + 1) * VECTORS, :] = result[:, :LANES]
        chosen_high[r * VECTORS : (r + 1) * VECTORS, 0:RANK] = result[:, LANES:]
    for k in range(LEVELS):
        rows = pl.ds(k, RANK, stride=VECTORS)
        coupling[k, :, 0:LANES] = chosen_low[rows, :].astype(BF16)
        coupling[k, :, LANES : LANES + RANK] = chosen_high[rows, :][:, :RANK].astype(BF16)


def down_kernel(
    every,
    top_hbm,
    box_coupling,
    coupling_hbm,
    mid_hbm,
    mid_far,
    leaf_hbm,
    leaf_far,
    basis_hbm,
    near_hbm,
    out,
    top_transfer,
    coupling,
    mid_transfer,
    leaf_transfer,
    basis,
    near_field,
    sem,
    pairs0,
    pairs1,
    pairs2,
    pairs3,
    pairs4,
    pairs5,
):
    half = pl.ds(0, BOXES // 2)
    rest = pl.ds(BOXES // 2, BOXES // 2 - 4)
    copies = [
        pltpu.make_async_copy(source, target, sem.at[i])
        for i, (source, target) in enumerate(
            (
                (top_hbm.at[half], top_transfer.at[half]),
                (top_hbm.at[rest], top_transfer.at[rest]),
                (coupling_hbm, coupling),
                (mid_hbm, mid_transfer),
                (leaf_hbm, leaf_transfer),
                (basis_hbm, basis),
                (near_hbm, near_field),
            )
        )
    ]
    for copy in copies:
        copy.start()
    device = lax.axis_index("clusters")
    lane = lane_index((VECTORS, LANES))
    zero = jnp.zeros((VECTORS, LANES), F32)

    pairs = (pairs0, pairs1, pairs2, pairs3, pairs4, pairs5)
    for level in range(LEVELS + 1):
        pairs[level][0] = zero
        pairs[level][(BOXES >> (level + 1)) + 1] = zero
    for p in range(BOXES // 2):
        pairs0[p + 1] = pick_two(lane, every[2 * p].astype(F32), every[2 * p + 1].astype(F32))
    for level in range(LEVELS):
        if level < 2:
            copies[level].wait()
        start = BOXES - (BOXES >> level)
        for g in range(BOXES >> (level + 3)):
            rows = pairs[level][pl.ds(1 + 4 * g, 4)].reshape(4 * VECTORS, LANES).astype(BF16)
            matrices = top_transfer[pl.ds(start + 4 * g, 4)].reshape(4 * RANK, 2 * RANK)
            result = dot_nt(rows, matrices)
            pairs[level + 1][1 + 2 * g] = pick_two(lane, result[0:8, 0:128], result[8:16, 0:128])
            pairs[level + 1][2 + 2 * g] = pick_two(
                lane, result[16:24, 128:256], result[24:32, 128:256]
            )
    copies[2].wait()
    across = []
    for level in range(LEVELS + 1):
        cluster = device >> level
        parent = cluster >> 1
        before = pairs[level][parent]
        after = pltpu.roll(pairs[level][parent + 2], 64, 1)
        middle = jnp.where((cluster & 1) == 1, before, after)
        stacked = jnp.concatenate([pick_two(lane, before, middle), after[:, :64]], axis=1)
        matrix = box_coupling[0] if level == 0 else coupling[level - 1]
        across.append(dot_nt(stacked.astype(BF16), matrix))
    down = across[LEVELS]
    for level in range(LEVELS - 1, -1, -1):
        cluster = device >> level
        start = BOXES - (BOXES >> level)
        pushed = dot_nn(down.astype(BF16), top_transfer[start + (cluster >> 1)])
        pushed = jnp.where((cluster & 1) == 1, pltpu.roll(pushed, 64, 1), pushed)
        down = across[level] + pushed[:, :64]

    copies[3].wait()
    mid_push = dot_nn(down.astype(BF16), mid_transfer[0])
    rows = []
    for c in range(GROUPS):
        h = c // 2
        tile = mid_far[h] + mid_push[:, h * LANES : (h + 1) * LANES]
        half = pick_two(lane, tile, zero) if c % 2 == 0 else pick_two(lane, zero, tile)
        rows.append(jnp.concatenate([half if i == h else zero for i in range(GROUPS // 2)], axis=1))
    copies[4].wait()
    leaf_push = dot_nn(
        jnp.concatenate(rows, axis=0).astype(BF16),
        leaf_transfer[...].reshape(GROUPS * RANK, CHILDREN * RANK_LEAF),
    )
    copies[5].wait()
    copies[6].wait()
    lane_group = lane // RANK_LEAF
    for g in range(LEAVES // 4):
        push = leaf_push[(g // 2) * 8 : (g // 2) * 8 + 8, (g % 2) * LANES : (g % 2 + 1) * LANES]
        leaf_down = leaf_far[g] + push
        rows = jnp.concatenate(
            [jnp.where(lane_group == j, leaf_down, 0.0) for j in range(4)], axis=0
        ).astype(BF16)
        b = basis[:, pl.ds(g * 4 * CAPACITY, 4 * CAPACITY)]
        result = dot_nn(rows, jnp.concatenate([b, b, b, b], axis=0))
        for h in range(2):
            span = slice(h * LANES, (h + 1) * LANES)
            far_tile = pick_two(
                lane, result[16 * h : 16 * h + 8, span], result[16 * h + 8 : 16 * h + 16, span]
            )
            at = pl.ds((2 * g + h) * LANES, LANES)
            out[:, at] = (far_tile + near_field[:, at]).astype(BF16)


def body(
    charges,
    leaf_basis,
    leaf_transfer,
    mid_transfer,
    far_source,
    far_coupling,
    mid_source,
    mid_coupling,
    box_coupling,
    top_transfer,
    top_coupling,
    near_target,
    near_source,
    near_count,
    near_blocks,
):
    pair = [(i, i ^ 1) for i in range(BOXES)]
    other = [(i, min(max(((i + 1) ^ 1) - 1, 0), BOXES - 1)) for i in range(BOXES)]
    vmem = pl.BlockSpec(memory_space=pltpu.VMEM)
    smem = pl.BlockSpec(memory_space=pltpu.SMEM)
    hbm = pl.BlockSpec(memory_space=pltpu.HBM)
    shape = jax.ShapeDtypeStruct
    packed, message = pl.pallas_call(
        up_kernel,
        out_shape=(shape((VECTORS, WIDE), BF16), shape((BOXES, VECTORS, LANES), BF16)),
        in_specs=[vmem] * 2 + [hbm] * 2,
        out_specs=(vmem, vmem),
        scratch_shapes=[
            pltpu.VMEM((GROUPS, RANK, CHILDREN * RANK_LEAF), BF16),
            pltpu.VMEM((1, RANK, GROUPS * RANK), BF16),
            pltpu.SemaphoreType.DMA((2,)),
        ],
        cost_estimate=pl.CostEstimate(flops=10**9, bytes_accessed=10**6, transcendentals=0),
        name="upward",
    )(charges, leaf_basis, leaf_transfer, mid_transfer)
    packed_other = lax.ppermute(packed, "clusters", other)
    packed_pair = lax.ppermute(packed, "clusters", pair)
    every = lax.all_to_all(message, "clusters", 0, 0)
    table = pltpu.VMEM((3 * LEAVES * VECTORS, LANES), F32)
    accumulator = pltpu.VMEM(((LEAVES + 1) * VECTORS, CAPACITY), F32)
    near_field, leaf_far, mid_far, coupling = pl.pallas_call(
        side_kernel,
        out_shape=(
            shape((VECTORS, POINTS), F32),
            shape((LEAVES // 4, VECTORS, LANES), F32),
            shape((GROUPS // 2, VECTORS, LANES), F32),
            shape((LEVELS, RANK, 3 * RANK), BF16),
        ),
        in_specs=[vmem] * 2 + [smem] + [vmem] * 5 + [hbm] * 4,
        out_specs=(vmem,) * 4,
        scratch_shapes=[
            table,
            table,
            table,
            pltpu.VMEM((3 * GROUPS * VECTORS, LANES), F32),
            accumulator,
            accumulator,
            accumulator,
            accumulator,
            pltpu.VMEM((RANK * VECTORS, LANES), F32),
            pltpu.VMEM((RANK * VECTORS, LANES), F32),
            pltpu.VMEM((PARTS, CAPACITY, PART), BF16),
            pltpu.VMEM((LEAVES, RANK_LEAF, FAR * RANK_LEAF), BF16),
            pltpu.VMEM((GROUPS, RANK, MID_FAR * RANK), BF16),
            pltpu.VMEM((RANK, 3 * RANK, BOXES - 4), BF16),
            pltpu.VMEM((VECTORS, LANES), jnp.int32),
            pltpu.VMEM((VECTORS, LANES), jnp.int32),
            pltpu.VMEM((FAR, LEAVES), jnp.int32),
            pltpu.VMEM((GROUPS, MID_FAR), jnp.int32),
            pltpu.SMEM((VECTORS, LANES), jnp.int32),
            pltpu.SMEM((VECTORS, LANES), jnp.int32),
            pltpu.SMEM((FAR, LEAVES), jnp.int32),
            pltpu.SMEM((GROUPS, MID_FAR), jnp.int32),
            pltpu.SemaphoreType.DMA((PARTS,)),
            pltpu.SemaphoreType.DMA((3,)),
            pltpu.SemaphoreType.DMA((4,)),
        ],
        cost_estimate=pl.CostEstimate(flops=2 * 10**9, bytes_accessed=10**7, transcendentals=0),
        compiler_params=pltpu.CompilerParams(vmem_limit_bytes=VMEM_LIMIT),
        name="side",
    )(
        near_source.reshape(VECTORS, LANES),
        near_target.reshape(VECTORS, LANES),
        near_count,
        far_source.T,
        mid_source,
        packed,
        packed_pair,
        packed_other,
        far_coupling,
        mid_coupling,
        jnp.transpose(top_coupling, (1, 2, 0)),
        near_blocks,
    )
    return pl.pallas_call(
        down_kernel,
        out_shape=shape((VECTORS, POINTS), BF16),
        in_specs=[vmem, hbm, vmem, hbm, hbm, vmem, hbm, vmem, hbm, hbm],
        out_specs=vmem,
        scratch_shapes=[
            pltpu.VMEM((BOXES - 4, RANK, 2 * RANK), BF16),
            pltpu.VMEM((LEVELS, RANK, 3 * RANK), BF16),
            pltpu.VMEM((1, RANK, GROUPS * RANK), BF16),
            pltpu.VMEM((GROUPS, RANK, CHILDREN * RANK_LEAF), BF16),
            pltpu.VMEM((RANK_LEAF, POINTS), BF16),
            pltpu.VMEM((VECTORS, POINTS), F32),
            pltpu.SemaphoreType.DMA((7,)),
        ]
        + [
            pltpu.VMEM(((BOXES >> (level + 1)) + 2, VECTORS, LANES), F32)
            for level in range(LEVELS + 1)
        ],
        cost_estimate=pl.CostEstimate(flops=10**9, bytes_accessed=10**6, transcendentals=0),
        name="down",
    )(
        every,
        top_transfer,
        box_coupling,
        coupling,
        mid_transfer,
        mid_far,
        leaf_transfer,
        leaf_far,
        leaf_basis,
        near_field,
    )


def solution(mesh):
    in_specs = (
        P(None, "clusters"),
        P(None, "clusters"),
        P("clusters", None, None),
        P("clusters", None, None),
        P("clusters", None),
        P("clusters", None, None),
        P("clusters", None),
        P("clusters", None, None),
        P("clusters", None, None),
        P(),
        P(),
        P("clusters"),
        P("clusters"),
        P("clusters"),
        P(None, "clusters"),
    )
    out_specs = P(None, "clusters")
    return jax.shard_map(body, mesh=mesh, in_specs=in_specs, out_specs=out_specs, check_vma=False)
```

```python
import jax
import jax.numpy as jnp
from jax import lax
from jax.experimental import pallas as pl
from jax.experimental.pallas import tpu as pltpu
from jax.sharding import PartitionSpec as P

F32 = jnp.float32
BF16 = jnp.bfloat16

VECTORS = 8
LEAVES = 64
CAPACITY = 64
RANK_LEAF = 32
RANK = 64
GROUPS = 8
CHILDREN = 8
FAR = 16
MID_FAR = 8
SLOTS = 1024
BOXES = 128
LEVELS = 5
POINTS = LEAVES * CAPACITY
LEAF_LANES = LEAVES * RANK_LEAF
MID_LANES = GROUPS * RANK
PARTS = 8
PART = SLOTS * CAPACITY // PARTS
BLOCK = SLOTS // PARTS
WIDE = POINTS + LEAF_LANES + MID_LANES
LANES = 128
VMEM_LIMIT = 60 * 1024 * 1024
MESSAGES = 16
LEAF_AT = LEAVES // 2
MID_AT = LEAF_AT + LEAVES // 4
FIELDS = MID_AT + GROUPS // 2


def dot_nt(left, right):
    return lax.dot_general(left, right, (((1,), (1,)), ((), ())), preferred_element_type=F32)


def dot_nn(left, right):
    return lax.dot_general(left, right, (((1,), (0,)), ((), ())), preferred_element_type=F32)


def lane_index(shape):
    return lax.broadcasted_iota(jnp.int32, shape, len(shape) - 1)


def pick_two(lane, first, second):
    return jnp.where(lane < 64, first, second)


def pick_four(lane, a, b, c, d):
    return jnp.where(lane < 64, jnp.where(lane < 32, a, b), jnp.where(lane < 96, c, d))


def rows_of(first):
    return pl.ds(pl.multiple_of(first, VECTORS), VECTORS)


def up_kernel(
    charges_hbm,
    basis_hbm,
    leaf_hbm,
    mid_hbm,
    packed_hbm,
    message_hbm,
    charges,
    basis,
    leaf_transfer,
    mid_transfer,
    coefficients,
    message,
    sem,
    out_sem,
):
    copies = [
        pltpu.make_async_copy(a, b, sem.at[i])
        for i, (a, b) in enumerate(
            (
                (charges_hbm, charges),
                (basis_hbm, basis),
                (leaf_hbm, leaf_transfer),
                (mid_hbm, mid_transfer),
            )
        )
    ]
    for copy in copies:
        copy.start()
    lane = lane_index((VECTORS, LANES))
    wide_lane = lane_index((VECTORS, 4 * CAPACITY)) // CAPACITY
    copies[0].wait()
    charges_out = pltpu.make_async_copy(
        charges, packed_hbm.at[:, pl.ds(0, POINTS)], out_sem.at[0]
    )
    charges_out.start()
    copies[1].wait()
    tiles = []
    for g in range(LEAVES // 4):
        span = pl.ds(g * 4 * CAPACITY, 4 * CAPACITY)
        x = charges[:, span].astype(F32)
        rows = jnp.concatenate([jnp.where(wide_lane == j, x, 0.0) for j in range(4)], axis=0)
        result = dot_nt(rows.astype(BF16), basis[:, span])
        tiles.append(
            jnp.concatenate([result[j * VECTORS : (j + 1) * VECTORS] for j in range(4)], axis=1)
        )
    for g in range(LEAVES // 4):
        coefficients[:, pl.ds(g * LANES, LANES)] = tiles[g].astype(BF16)
    stacked = jnp.concatenate(
        [jnp.concatenate([tiles[2 * c], tiles[2 * c + 1]], axis=1) for c in range(GROUPS)], axis=0
    ).astype(BF16)
    copies[2].wait()
    result = dot_nt(stacked, leaf_transfer[...].reshape(GROUPS * RANK, CHILDREN * RANK_LEAF))
    mid = []
    for h in range(GROUPS // 2):
        span = slice(h * LANES, (h + 1) * LANES)
        low = result[16 * h : 16 * h + 8, span]
        high = result[16 * h + 8 : 16 * h + 16, span]
        mid.append(pick_two(lane, low, high).astype(BF16))
        coefficients[:, pl.ds(LEAF_LANES + h * LANES, LANES)] = mid[h]
    coefficients_out = pltpu.make_async_copy(
        coefficients, packed_hbm.at[:, pl.ds(POINTS, LEAF_LANES + MID_LANES)], out_sem.at[1]
    )
    coefficients_out.start()
    copies[3].wait()
    box = dot_nt(jnp.concatenate(mid, axis=1), mid_transfer[0])
    box = jnp.concatenate([box, box], axis=1).astype(BF16)
    message[...] = jnp.broadcast_to(box[None], message.shape)
    messages_out = [
        pltpu.make_async_copy(
            message, message_hbm.at[pl.ds(i * MESSAGES, MESSAGES)], out_sem.at[2 + i]
        )
        for i in range(BOXES // MESSAGES)
    ]
    for copy in messages_out:
        copy.start()
    charges_out.wait()
    coefficients_out.wait()
    for copy in messages_out:
        copy.wait()


def side_kernel(
    near_source_hbm,
    near_target_hbm,
    near_count_hbm,
    far_source_hbm,
    mid_source_hbm,
    own_hbm,
    pair_hbm,
    other_hbm,
    far_hbm,
    mid_far_hbm,
    top_coupling_hbm,
    top_transfer_hbm,
    box_coupling_hbm,
    near_hbm,
    field_hbm,
    coupling_hbm,
    near_source,
    near_target,
    far_source,
    mid_source,
    own,
    pair,
    other,
    far,
    mid_coupling,
    top_coupling,
    parents,
    box_coupling,
    near,
    field,
    coupling,
    x_low,
    x_high,
    leaf_table,
    mid_table,
    acc0,
    acc1,
    acc2,
    acc3,
    chosen_low,
    chosen_high,
    source_rows,
    target_rows,
    far_rows,
    mid_rows,
    near_count,
    near_from,
    near_to,
    far_from,
    mid_from,
    near_sem,
    sem,
    parent_sem,
    index_sem,
    out_sem,
):
    device = lax.axis_index("clusters")

    def near_copy(k):
        return pltpu.make_async_copy(
            near_hbm.at[:, pl.ds(pl.multiple_of(k * PART, PART), PART)], near.at[k], near_sem.at[k]
        )

    copies = [
        pltpu.make_async_copy(a, b, sem.at[i])
        for i, (a, b) in enumerate(
            (
                (near_count_hbm, near_count),
                (near_source_hbm, near_source),
                (near_target_hbm, near_target),
                (far_source_hbm, far_source),
                (mid_source_hbm, mid_source),
                (own_hbm, own),
                (pair_hbm, pair),
                (other_hbm, other),
                (box_coupling_hbm, box_coupling),
                (far_hbm, far),
                (mid_far_hbm, mid_coupling),
                (top_coupling_hbm, top_coupling),
            )
        )
    ]
    parent_copies = []
    for level in range(LEVELS):
        start = BOXES - (BOXES >> level)
        parent_copies.append(
            pltpu.make_async_copy(
                top_transfer_hbm.at[start + (device >> (level + 1))],
                parents.at[level],
                parent_sem.at[level],
            )
        )
    for copy in copies[:8]:
        copy.start()
    near_copy(0).start()
    near_copy(1).start()
    for copy in parent_copies:
        copy.start()
    copies[8].start()

    for copy in copies[:5]:
        copy.wait()
    live = near_count[0, 0]
    leaf_base = (device - 1) * LEAVES
    shape = (VECTORS, LANES)
    slot = lax.broadcasted_iota(jnp.int32, shape, 0) * LANES + lane_index(shape)
    used = slot < live
    source_rows[...] = jnp.where(used, near_source[...] - leaf_base, LEAVES) * VECTORS
    target_rows[...] = jnp.where(used, near_target[...], LEAVES) * VECTORS
    far_rows[...] = (far_source[...] - leaf_base) * VECTORS
    mid_rows[...] = (mid_source[...] - (device - 1) * GROUPS) * VECTORS
    index_copies = [
        pltpu.make_async_copy(a, b, index_sem.at[i])
        for i, (a, b) in enumerate(
            (
                (source_rows, near_from),
                (target_rows, near_to),
                (far_rows, far_from),
                (mid_rows, mid_from),
            )
        )
    ]
    for copy in index_copies:
        copy.start()
    blocks = jnp.clip((live + BLOCK - 1) // BLOCK, 2, PARTS)
    for k in (2, 3):

        @pl.when(k < blocks)
        def _(k=k):
            near_copy(k).start()

    lane = lane_index((VECTORS, LANES))
    zero = jnp.zeros((VECTORS, LANES), F32)
    odd = device % 2
    accumulators = (acc0, acc1, acc2, acc3)
    for acc in accumulators:
        acc[...] = jnp.zeros(acc.shape, F32)
    for copy in copies[5:8]:
        copy.wait()
    for source, region in ((own, 1), (pair, (1 - odd) * 2), (other, odd * 2)):
        base = region * LEAVES * VECTORS
        for h in range(LEAVES // 2):
            tile = source[:, pl.ds(h * LANES, LANES)].astype(F32)
            turned = pltpu.roll(tile, 64, 1)
            at = base + 2 * h * VECTORS
            x_low[rows_of(at), :] = pick_two(lane, tile, zero)
            x_high[rows_of(at), :] = pick_two(lane, zero, turned)
            x_low[rows_of(at + VECTORS), :] = pick_two(lane, turned, zero)
            x_high[rows_of(at + VECTORS), :] = pick_two(lane, zero, tile)
        for h in range(LEAVES // 4):
            tile = source[:, pl.ds(POINTS + h * LANES, LANES)].astype(F32)
            turns = [tile] + [pltpu.roll(tile, 32 * i, 1) for i in range(1, 4)]
            for j in range(4):
                leaf_table[rows_of(base + (4 * h + j) * VECTORS), :] = pick_four(
                    lane, *[turns[(group - j) % 4] for group in range(4)]
                )
        base = region * GROUPS * VECTORS
        for h in range(GROUPS // 2):
            tile = source[:, pl.ds(POINTS + LEAF_LANES + h * LANES, LANES)].astype(F32)
            turned = pltpu.roll(tile, 64, 1)
            at = base + 2 * h * VECTORS
            mid_table[rows_of(at), :] = pick_two(lane, tile, turned)
            mid_table[rows_of(at + VECTORS), :] = pick_two(lane, turned, tile)
    for copy in index_copies:
        copy.wait()

    zeros_half = jnp.zeros((2 * VECTORS, LANES), BF16)

    def near_step(k, carry):
        @pl.when(k + 4 < blocks)
        def _():
            near_copy(k + 4).start()

        @pl.when(k == 0)
        def _():
            copies[9].start()
            copies[10].start()

        @pl.when(k == 1)
        def _():
            copies[11].start()

        near_copy(k).wait()
        for i in range(BLOCK // 4):
            at = [rows_of(near_from[k, 4 * i + j]) for j in range(4)]
            top = jnp.concatenate([x_low[at[0], :], x_high[at[1], :]], axis=0)
            bottom = jnp.concatenate([x_low[at[2], :], x_high[at[3], :]], axis=0)
            rows = jnp.concatenate(
                [
                    jnp.concatenate([top.astype(BF16), zeros_half], axis=1),
                    jnp.concatenate([zeros_half, bottom.astype(BF16)], axis=1),
                ],
                axis=0,
            )
            result = dot_nt(rows, near[k, :, 4 * i * CAPACITY : 4 * (i + 1) * CAPACITY])
            for j in range(4):
                to = rows_of(near_to[k, 4 * i + j])
                accumulators[j][to, :] += result[j * 8 : (j + 1) * 8]
        return carry

    lax.fori_loop(0, blocks, near_step, 0)
    for h in range(LEAVES // 2):
        low = rows_of(2 * h * VECTORS)
        high = rows_of((2 * h + 1) * VECTORS)
        field[h] = jnp.concatenate(
            [
                acc0[low, :] + acc1[low, :] + (acc2[low, :] + acc3[low, :]),
                acc0[high, :] + acc1[high, :] + (acc2[high, :] + acc3[high, :]),
            ],
            axis=1,
        )

    for copy in parent_copies:
        copy.wait()
    square = (RANK, RANK)
    product = (
        lax.broadcasted_iota(jnp.int32, square, 0) == lax.broadcasted_iota(jnp.int32, square, 1)
    ).astype(F32)
    products = []
    for level in range(LEVELS):
        parent = parents[level].astype(F32)
        own_half = jnp.where(
            ((device >> level) & 1) == 1, pltpu.roll(parent, RANK, 1), parent
        )[:, :RANK]
        product = dot_nt(product.astype(BF16), own_half.astype(BF16))
        products.append(product.astype(BF16))

    copies[9].wait()
    for group in range(LEAVES // 8):
        rows = []
        for i in range(8):
            leaf = group * 8 + i
            rows.append(
                jnp.concatenate(
                    [
                        pick_four(
                            lane,
                            *[leaf_table[rows_of(far_from[4 * q + m, leaf]), :] for m in range(4)],
                        )
                        for q in range(FAR // 4)
                    ],
                    axis=1,
                )
            )
        result = dot_nt(
            jnp.concatenate(rows, axis=0).astype(BF16),
            far[group * 8 : group * 8 + 8].reshape(8 * RANK_LEAF, FAR * RANK_LEAF),
        )
        for h in range(2):
            field[LEAF_AT + group * 2 + h] = pick_four(
                lane,
                *[
                    result[(4 * h + j) * 8 : (4 * h + j + 1) * 8, h * LANES : (h + 1) * LANES]
                    for j in range(4)
                ],
            )
    copies[10].wait()
    rows = []
    for c in range(GROUPS):
        rows.append(
            jnp.concatenate(
                [
                    pick_two(
                        lane,
                        mid_table[rows_of(mid_from[c, 2 * q]), :],
                        mid_table[rows_of(mid_from[c, 2 * q + 1]), :],
                    )
                    for q in range(MID_FAR // 2)
                ],
                axis=1,
            )
        )
    result = dot_nt(
        jnp.concatenate(rows, axis=0).astype(BF16),
        mid_coupling[...].reshape(GROUPS * RANK, MID_FAR * RANK),
    )
    for h in range(GROUPS // 2):
        span = slice(h * LANES, (h + 1) * LANES)
        field[MID_AT + h] = pick_two(
            lane, result[16 * h : 16 * h + 8, span], result[16 * h + 8 : 16 * h + 16, span]
        )
    field_out = pltpu.make_async_copy(field, field_hbm, out_sem.at[0])
    field_out.start()

    copies[11].wait()
    tops = top_coupling.shape[2]
    level = lax.broadcasted_iota(jnp.int32, (VECTORS, tops), 0) + 1
    column = BOXES - lax.shift_right_logical(jnp.full_like(level, BOXES), level - 1)
    column = column + lax.shift_right_logical(jnp.full_like(level, 1) * device, level)
    wanted = (lane_index((VECTORS, tops)) == column).astype(F32).astype(BF16)
    for r in range(RANK):
        result = dot_nt(wanted, top_coupling[r])
        chosen_low[r * VECTORS : (r + 1) * VECTORS, :] = result[:, :LANES]
        chosen_high[r * VECTORS : (r + 1) * VECTORS, 0:RANK] = result[:, LANES:]
    copies[8].wait()
    coupling[0] = box_coupling[0]
    for k in range(LEVELS):
        rows = pl.ds(k, RANK, stride=VECTORS)
        chosen = jnp.concatenate([chosen_low[rows, :], chosen_high[rows, :][:, :RANK]], axis=1)
        coupling[k + 1] = dot_nn(products[k], chosen.astype(BF16)).astype(BF16)
    coupling_out = pltpu.make_async_copy(coupling, coupling_hbm, out_sem.at[1])
    coupling_out.start()
    field_out.wait()
    coupling_out.wait()


def down_kernel(
    every_hbm,
    top_hbm,
    coupling_hbm,
    mid_hbm,
    leaf_hbm,
    field_hbm,
    basis_hbm,
    out,
    every,
    top_transfer,
    coupling,
    mid_transfer,
    leaf_transfer,
    field,
    basis,
    sem,
    pairs0,
    pairs1,
    pairs2,
    pairs3,
    pairs4,
    pairs5,
):
    half = pl.ds(0, BOXES // 2)
    rest = pl.ds(BOXES // 2, BOXES // 2 - 4)
    copies = [
        pltpu.make_async_copy(source, target, sem.at[i])
        for i, (source, target) in enumerate(
            (
                (every_hbm, every),
                (top_hbm.at[half], top_transfer.at[half]),
                (top_hbm.at[rest], top_transfer.at[rest]),
                (coupling_hbm, coupling),
                (mid_hbm, mid_transfer),
                (leaf_hbm, leaf_transfer),
                (field_hbm, field),
                (basis_hbm, basis),
            )
        )
    ]
    for copy in copies:
        copy.start()
    device = lax.axis_index("clusters")
    lane = lane_index((VECTORS, LANES))
    zero = jnp.zeros((VECTORS, LANES), F32)
    empty = jnp.zeros((2 * VECTORS, LANES), BF16)

    pairs = (pairs0, pairs1, pairs2, pairs3, pairs4, pairs5)
    for level in range(LEVELS + 1):
        pairs[level][0] = zero
        pairs[level][(BOXES >> (level + 1)) + 1] = zero
    copies[0].wait()
    for p in range(BOXES // 2):
        pairs0[p + 1] = pick_two(lane, every[2 * p].astype(F32), every[2 * p + 1].astype(F32))
    for level in range(LEVELS):
        if level < 2:
            copies[1 + level].wait()
        start = BOXES - (BOXES >> level)
        count = BOXES >> (level + 1)
        for g in range(0, count, 8):
            left, right = [], []
            for quad in range(g, min(g + 8, count), 4):
                low = jnp.concatenate([pairs[level][1 + quad], pairs[level][2 + quad]], axis=0)
                high = jnp.concatenate([pairs[level][3 + quad], pairs[level][4 + quad]], axis=0)
                left.append(jnp.concatenate([low.astype(BF16), empty], axis=1))
                left.append(jnp.concatenate([empty, high.astype(BF16)], axis=1))
                at = start + quad
                right.append(jnp.concatenate([top_transfer[at], top_transfer[at + 2]], axis=1))
                right.append(jnp.concatenate([top_transfer[at + 1], top_transfer[at + 3]], axis=1))
            result = dot_nt(jnp.concatenate(left, axis=0), jnp.concatenate(right, axis=0))
            for i in range(len(left)):
                span = slice((i // 2) * LANES, (i // 2 + 1) * LANES)
                pairs[level + 1][1 + g // 2 + i] = pick_two(
                    lane, result[16 * i : 16 * i + 8, span], result[16 * i + 8 : 16 * i + 16, span]
                )
    copies[3].wait()
    down = jnp.zeros((VECTORS, RANK), F32)
    for level in range(LEVELS + 1):
        cluster = device >> level
        parent = cluster >> 1
        before = pairs[level][parent]
        after = pltpu.roll(pairs[level][parent + 2], 64, 1)
        middle = jnp.where((cluster & 1) == 1, before, after)
        stacked = jnp.concatenate([pick_two(lane, before, middle), after[:, :64]], axis=1)
        down = down + dot_nt(stacked.astype(BF16), coupling[level])

    copies[4].wait()
    mid_push = dot_nn(down.astype(BF16), mid_transfer[0])
    copies[5].wait()
    copies[6].wait()
    rows = []
    for c in range(GROUPS):
        h = c // 2
        tile = field[MID_AT + h] + mid_push[:, h * LANES : (h + 1) * LANES]
        half_tile = pick_two(lane, tile, zero) if c % 2 == 0 else pick_two(lane, zero, tile)
        rows.append(
            jnp.concatenate([half_tile if i == h else zero for i in range(GROUPS // 2)], axis=1)
        )
    leaf_push = dot_nn(
        jnp.concatenate(rows, axis=0).astype(BF16),
        leaf_transfer[...].reshape(GROUPS * RANK, CHILDREN * RANK_LEAF),
    )
    copies[7].wait()
    lane_group = lane // RANK_LEAF
    for g in range(LEAVES // 4):
        push = leaf_push[(g // 2) * 8 : (g // 2) * 8 + 8, (g % 2) * LANES : (g % 2 + 1) * LANES]
        leaf_down = field[LEAF_AT + g] + push
        rows = jnp.concatenate(
            [jnp.where(lane_group == j, leaf_down, 0.0) for j in range(4)], axis=0
        ).astype(BF16)
        b = basis[:, pl.ds(g * 4 * CAPACITY, 4 * CAPACITY)]
        result = dot_nn(rows, jnp.concatenate([b, b, b, b], axis=0))
        for h in range(2):
            span = slice(h * LANES, (h + 1) * LANES)
            far_tile = pick_two(
                lane, result[16 * h : 16 * h + 8, span], result[16 * h + 8 : 16 * h + 16, span]
            )
            out[:, pl.ds((2 * g + h) * LANES, LANES)] = (far_tile + field[2 * g + h]).astype(BF16)


def body(
    charges,
    leaf_basis,
    leaf_transfer,
    mid_transfer,
    far_source,
    far_coupling,
    mid_source,
    mid_coupling,
    box_coupling,
    top_transfer,
    top_coupling,
    near_target,
    near_source,
    near_count,
    near_blocks,
):
    pair = [(i, i ^ 1) for i in range(BOXES)]
    other = [(i, min(max(((i + 1) ^ 1) - 1, 0), BOXES - 1)) for i in range(BOXES)]
    vmem = pl.BlockSpec(memory_space=pltpu.VMEM)
    hbm = pl.BlockSpec(memory_space=pltpu.HBM)
    shape = jax.ShapeDtypeStruct
    scratch = pltpu.VMEM
    dma = pltpu.SemaphoreType.DMA
    packed, message = pl.pallas_call(
        up_kernel,
        out_shape=(shape((VECTORS, WIDE), BF16), shape((BOXES, VECTORS, LANES), BF16)),
        in_specs=[hbm] * 4,
        out_specs=(hbm, hbm),
        scratch_shapes=[
            scratch((VECTORS, POINTS), BF16),
            scratch((RANK_LEAF, POINTS), BF16),
            scratch((GROUPS, RANK, CHILDREN * RANK_LEAF), BF16),
            scratch((1, RANK, GROUPS * RANK), BF16),
            scratch((VECTORS, LEAF_LANES + MID_LANES), BF16),
            scratch((MESSAGES, VECTORS, LANES), BF16),
            dma((4,)),
            dma((2 + BOXES // MESSAGES,)),
        ],
        cost_estimate=pl.CostEstimate(flops=10**9, bytes_accessed=10**6, transcendentals=0),
        compiler_params=pltpu.CompilerParams(vmem_limit_bytes=VMEM_LIMIT),
        name="upward",
    )(charges, leaf_basis, leaf_transfer, mid_transfer)
    packed_other = lax.ppermute(packed, "clusters", other)
    packed_pair = lax.ppermute(packed, "clusters", pair)
    every = lax.all_to_all(message, "clusters", 0, 0)
    table = scratch((3 * LEAVES * VECTORS, LANES), F32)
    accumulator = scratch(((LEAVES + 1) * VECTORS, CAPACITY), F32)
    indices = [
        (VECTORS, LANES),
        (VECTORS, LANES),
        (FAR, LEAVES),
        (GROUPS, MID_FAR),
    ]
    wide = scratch((VECTORS, WIDE), BF16)
    field, coupling = pl.pallas_call(
        side_kernel,
        out_shape=(
            shape((FIELDS, VECTORS, LANES), F32),
            shape((LEVELS + 1, RANK, 3 * RANK), BF16),
        ),
        in_specs=[hbm] * 14,
        out_specs=(hbm, hbm),
        scratch_shapes=[scratch(i, jnp.int32) for i in indices]
        + [
            wide,
            wide,
            wide,
            scratch((LEAVES, RANK_LEAF, FAR * RANK_LEAF), BF16),
            scratch((GROUPS, RANK, MID_FAR * RANK), BF16),
            scratch((RANK, 3 * RANK, BOXES - 4), BF16),
            scratch((LEVELS, RANK, 2 * RANK), BF16),
            scratch((1, RANK, 3 * RANK), BF16),
            scratch((PARTS, CAPACITY, PART), BF16),
            scratch((FIELDS, VECTORS, LANES), F32),
            scratch((LEVELS + 1, RANK, 3 * RANK), BF16),
            table,
            table,
            table,
            scratch((3 * GROUPS * VECTORS, LANES), F32),
            accumulator,
            accumulator,
            accumulator,
            accumulator,
            scratch((RANK * VECTORS, LANES), F32),
            scratch((RANK * VECTORS, LANES), F32),
        ]
        + [scratch(i, jnp.int32) for i in indices]
        + [pltpu.SMEM((1, 1), jnp.int32)]
        + [pltpu.SMEM(i, jnp.int32) for i in indices]
        + [dma((PARTS,)), dma((12,)), dma((LEVELS,)), dma((4,)), dma((2,))],
        cost_estimate=pl.CostEstimate(flops=2 * 10**9, bytes_accessed=10**7, transcendentals=0),
        compiler_params=pltpu.CompilerParams(vmem_limit_bytes=VMEM_LIMIT),
        name="side",
    )(
        near_source.reshape(VECTORS, LANES),
        near_target.reshape(VECTORS, LANES),
        near_count.reshape(1, 1),
        far_source.T,
        mid_source,
        packed,
        packed_pair,
        packed_other,
        far_coupling,
        mid_coupling,
        jnp.transpose(top_coupling, (1, 2, 0)),
        top_transfer,
        box_coupling,
        near_blocks,
    )
    return pl.pallas_call(
        down_kernel,
        out_shape=shape((VECTORS, POINTS), BF16),
        in_specs=[hbm] * 7,
        out_specs=vmem,
        scratch_shapes=[
            scratch((BOXES, VECTORS, LANES), BF16),
            scratch((BOXES - 4, RANK, 2 * RANK), BF16),
            scratch((LEVELS + 1, RANK, 3 * RANK), BF16),
            scratch((1, RANK, GROUPS * RANK), BF16),
            scratch((GROUPS, RANK, CHILDREN * RANK_LEAF), BF16),
            scratch((FIELDS, VECTORS, LANES), F32),
            scratch((RANK_LEAF, POINTS), BF16),
            dma((8,)),
        ]
        + [
            scratch(((BOXES >> (level + 1)) + 2, VECTORS, LANES), F32)
            for level in range(LEVELS + 1)
        ],
        cost_estimate=pl.CostEstimate(flops=10**9, bytes_accessed=10**6, transcendentals=0),
        compiler_params=pltpu.CompilerParams(vmem_limit_bytes=VMEM_LIMIT),
        name="down",
    )(every, top_transfer, coupling, mid_transfer, leaf_transfer, field, leaf_basis)


def solution(mesh):
    in_specs = (
        P(None, "clusters"),
        P(None, "clusters"),
        P("clusters", None, None),
        P("clusters", None, None),
        P("clusters", None),
        P("clusters", None, None),
        P("clusters", None),
        P("clusters", None, None),
        P("clusters", None, None),
        P(),
        P(),
        P("clusters"),
        P("clusters"),
        P("clusters"),
        P(None, "clusters"),
    )
    out_specs = P(None, "clusters")
    return jax.shard_map(body, mesh=mesh, in_specs=in_specs, out_specs=out_specs, check_vma=False)
```

```python
import jax
import jax.numpy as jnp
from jax import lax
from jax.experimental import pallas as pl
from jax.experimental.pallas import tpu as pltpu
from jax.sharding import PartitionSpec as P

F32 = jnp.float32
BF16 = jnp.bfloat16

VECTORS = 8
LEAVES = 64
CAPACITY = 64
RANK_LEAF = 32
RANK = 64
GROUPS = 8
CHILDREN = 8
FAR = 16
MID_FAR = 8
SLOTS = 1024
BOXES = 128
LEVELS = 5
POINTS = LEAVES * CAPACITY
LEAF_LANES = LEAVES * RANK_LEAF
MID_LANES = GROUPS * RANK
PARTS = 8
PART = SLOTS * CAPACITY // PARTS
BLOCK = SLOTS // PARTS
WIDE = POINTS + LEAF_LANES + MID_LANES
LANES = 128
VMEM_LIMIT = 60 * 1024 * 1024
MESSAGES = 16
LEAF_AT = LEAVES // 2
MID_AT = LEAF_AT + LEAVES // 4
FIELDS = MID_AT + GROUPS // 2


def dot_nt(left, right):
    return lax.dot_general(left, right, (((1,), (1,)), ((), ())), preferred_element_type=F32)


def dot_nn(left, right):
    return lax.dot_general(left, right, (((1,), (0,)), ((), ())), preferred_element_type=F32)


def lane_index(shape):
    return lax.broadcasted_iota(jnp.int32, shape, len(shape) - 1)


def pick_two(lane, first, second):
    return jnp.where(lane < 64, first, second)


def pick_four(lane, a, b, c, d):
    return jnp.where(lane < 64, jnp.where(lane < 32, a, b), jnp.where(lane < 96, c, d))


def turn(tile, groups):
    return tile if groups % 4 == 0 else pltpu.roll(tile, RANK_LEAF * (groups % 4), 1)


def rows_of(first):
    return pl.ds(pl.multiple_of(first, VECTORS), VECTORS)


def up_kernel(
    charges_hbm,
    basis_hbm,
    leaf_hbm,
    mid_hbm,
    packed_hbm,
    message_hbm,
    charges,
    basis,
    leaf_transfer,
    mid_transfer,
    coefficients,
    message,
    sem,
    out_sem,
):
    copies = [
        pltpu.make_async_copy(a, b, sem.at[i])
        for i, (a, b) in enumerate(
            (
                (charges_hbm, charges),
                (basis_hbm, basis),
                (leaf_hbm, leaf_transfer),
                (mid_hbm, mid_transfer),
            )
        )
    ]
    for copy in copies:
        copy.start()
    lane = lane_index((VECTORS, LANES))
    wide_lane = lane_index((VECTORS, 4 * CAPACITY)) // CAPACITY
    copies[0].wait()
    charges_out = pltpu.make_async_copy(
        charges, packed_hbm.at[:, pl.ds(0, POINTS)], out_sem.at[0]
    )
    charges_out.start()
    copies[1].wait()
    tiles = []
    for first in range(0, LEAVES // 4, 8):
        rows, weights = [], []
        for g in range(first, first + 8):
            span = pl.ds(g * 4 * CAPACITY, 4 * CAPACITY)
            x = charges[:, span].astype(F32)
            rows += [jnp.where(wide_lane == j, x, 0.0) for j in range(4)]
            weights.append(basis[:, span])
        result = dot_nt(
            jnp.concatenate(rows, axis=0).astype(BF16), jnp.concatenate(weights, axis=0)
        )
        for g in range(8):
            tile = result[32 * g : 32 * (g + 1), (g // 4) * LANES : (g // 4 + 1) * LANES]
            tiles.append(
                pick_four(lane, *[turn(tile[8 * j : 8 * (j + 1)], j - g % 4) for j in range(4)])
            )
    for g in range(LEAVES // 4):
        coefficients[:, pl.ds(g * LANES, LANES)] = tiles[g].astype(BF16)
    stacked = jnp.concatenate(
        [jnp.concatenate([tiles[2 * c], tiles[2 * c + 1]], axis=1) for c in range(GROUPS)], axis=0
    ).astype(BF16)
    copies[2].wait()
    result = dot_nt(stacked, leaf_transfer[...].reshape(GROUPS * RANK, CHILDREN * RANK_LEAF))
    mid = []
    for h in range(GROUPS // 2):
        span = slice(h * LANES, (h + 1) * LANES)
        low = result[16 * h : 16 * h + 8, span]
        high = result[16 * h + 8 : 16 * h + 16, span]
        mid.append(pick_two(lane, low, high).astype(BF16))
        coefficients[:, pl.ds(LEAF_LANES + h * LANES, LANES)] = mid[h]
    coefficients_out = pltpu.make_async_copy(
        coefficients, packed_hbm.at[:, pl.ds(POINTS, LEAF_LANES + MID_LANES)], out_sem.at[1]
    )
    coefficients_out.start()
    copies[3].wait()
    box = dot_nt(jnp.concatenate(mid, axis=1), mid_transfer[0])
    box = jnp.concatenate([box[:4], box[4:]], axis=1)
    box = jnp.concatenate([box, box], axis=0).astype(BF16)
    message[...] = jnp.broadcast_to(box[None], message.shape)
    messages_out = [
        pltpu.make_async_copy(
            message, message_hbm.at[pl.ds(i * MESSAGES, MESSAGES)], out_sem.at[2 + i]
        )
        for i in range(BOXES // 2 // MESSAGES)
    ]
    for copy in messages_out:
        copy.start()
    charges_out.wait()
    coefficients_out.wait()
    for copy in messages_out:
        copy.wait()


def side_kernel(
    near_source_hbm,
    near_target_hbm,
    near_count_hbm,
    far_source_hbm,
    mid_source_hbm,
    own_hbm,
    pair_hbm,
    other_hbm,
    far_hbm,
    mid_far_hbm,
    top_coupling_hbm,
    top_transfer_hbm,
    box_coupling_hbm,
    near_hbm,
    field_hbm,
    coupling_hbm,
    near_source,
    near_target,
    far_source,
    mid_source,
    own,
    pair,
    other,
    far,
    mid_coupling,
    top_coupling,
    parents,
    box_coupling,
    near,
    field,
    coupling,
    x_low,
    x_high,
    leaf_table,
    mid_table,
    acc0,
    acc1,
    acc2,
    acc3,
    chosen_low,
    chosen_high,
    source_rows,
    target_rows,
    far_rows,
    mid_rows,
    near_count,
    near_from,
    near_to,
    far_from,
    mid_from,
    near_sem,
    sem,
    parent_sem,
    index_sem,
    out_sem,
):
    device = lax.axis_index("clusters")

    def near_copy(k):
        return pltpu.make_async_copy(
            near_hbm.at[:, pl.ds(pl.multiple_of(k * PART, PART), PART)], near.at[k], near_sem.at[k]
        )

    copies = [
        pltpu.make_async_copy(a, b, sem.at[i])
        for i, (a, b) in enumerate(
            (
                (near_count_hbm, near_count),
                (near_source_hbm, near_source),
                (near_target_hbm, near_target),
                (far_source_hbm, far_source),
                (mid_source_hbm, mid_source),
                (own_hbm, own),
                (pair_hbm, pair),
                (other_hbm, other),
                (box_coupling_hbm, box_coupling),
                (far_hbm, far),
                (mid_far_hbm, mid_coupling),
                (top_coupling_hbm, top_coupling),
            )
        )
    ]
    parent_copies = []
    for level in range(LEVELS):
        start = BOXES - (BOXES >> level)
        parent_copies.append(
            pltpu.make_async_copy(
                top_transfer_hbm.at[start + (device >> (level + 1))],
                parents.at[level],
                parent_sem.at[level],
            )
        )
    for copy in copies[:8]:
        copy.start()
    near_copy(0).start()
    near_copy(1).start()
    for copy in parent_copies:
        copy.start()
    copies[8].start()

    for copy in copies[:5]:
        copy.wait()
    live = near_count[0, 0]
    leaf_base = (device - 1) * LEAVES
    shape = (VECTORS, LANES)
    slot = lax.broadcasted_iota(jnp.int32, shape, 0) * LANES + lane_index(shape)
    used = slot < live
    source_rows[...] = jnp.where(used, near_source[...] - leaf_base, LEAVES) * VECTORS
    target_rows[...] = jnp.where(used, near_target[...], LEAVES) * VECTORS
    far_rows[...] = (far_source[...] - leaf_base) * VECTORS
    mid_rows[...] = (mid_source[...] - (device - 1) * GROUPS) * VECTORS
    index_copies = [
        pltpu.make_async_copy(a, b, index_sem.at[i])
        for i, (a, b) in enumerate(
            (
                (source_rows, near_from),
                (target_rows, near_to),
                (far_rows, far_from),
                (mid_rows, mid_from),
            )
        )
    ]
    for copy in index_copies:
        copy.start()
    blocks = jnp.clip((live + BLOCK - 1) // BLOCK, 2, PARTS)
    for k in (2, 3):

        @pl.when(k < blocks)
        def _(k=k):
            near_copy(k).start()

    lane = lane_index((VECTORS, LANES))
    zero = jnp.zeros((VECTORS, LANES), F32)
    odd = device % 2
    accumulators = (acc0, acc1, acc2, acc3)
    for acc in accumulators:
        acc[...] = jnp.zeros(acc.shape, F32)
    for copy in copies[5:8]:
        copy.wait()
    for source, region in ((own, 1), (pair, (1 - odd) * 2), (other, odd * 2)):
        base = region * LEAVES * VECTORS
        for h in range(LEAVES // 2):
            tile = source[:, pl.ds(h * LANES, LANES)].astype(F32)
            turned = pltpu.roll(tile, 64, 1)
            at = base + 2 * h * VECTORS
            x_low[rows_of(at), :] = pick_two(lane, tile, zero)
            x_high[rows_of(at), :] = pick_two(lane, zero, turned)
            x_low[rows_of(at + VECTORS), :] = pick_two(lane, turned, zero)
            x_high[rows_of(at + VECTORS), :] = pick_two(lane, zero, tile)
        for h in range(LEAVES // 4):
            tile = source[:, pl.ds(POINTS + h * LANES, LANES)].astype(F32)
            turns = [tile] + [pltpu.roll(tile, 32 * i, 1) for i in range(1, 4)]
            for j in range(4):
                leaf_table[rows_of(base + (4 * h + j) * VECTORS), :] = pick_four(
                    lane, *[turns[(group - j) % 4] for group in range(4)]
                )
        base = region * GROUPS * VECTORS
        for h in range(GROUPS // 2):
            tile = source[:, pl.ds(POINTS + LEAF_LANES + h * LANES, LANES)].astype(F32)
            turned = pltpu.roll(tile, 64, 1)
            at = base + 2 * h * VECTORS
            mid_table[rows_of(at), :] = pick_two(lane, tile, turned)
            mid_table[rows_of(at + VECTORS), :] = pick_two(lane, turned, tile)
    for copy in index_copies:
        copy.wait()

    zeros_half = jnp.zeros((2 * VECTORS, LANES), BF16)

    def near_step(k, carry):
        @pl.when(k + 4 < blocks)
        def _():
            near_copy(k + 4).start()

        @pl.when(k == 0)
        def _():
            copies[9].start()
            copies[10].start()

        @pl.when(k == 1)
        def _():
            copies[11].start()

        near_copy(k).wait()
        for i in range(BLOCK // 16):
            rows, weights = [], []
            for g in range(4):
                first = 16 * i + 4 * g
                at = [rows_of(near_from[k, first + j]) for j in range(4)]
                top = jnp.concatenate([x_low[at[0], :], x_high[at[1], :]], axis=0)
                bottom = jnp.concatenate([x_low[at[2], :], x_high[at[3], :]], axis=0)
                rows.append(jnp.concatenate([top.astype(BF16), zeros_half], axis=1))
                rows.append(jnp.concatenate([zeros_half, bottom.astype(BF16)], axis=1))
                weights.append(near[k, :, first * CAPACITY : (first + 4) * CAPACITY])
            result = dot_nt(jnp.concatenate(rows, axis=0), jnp.concatenate(weights, axis=0))
            for g in range(4):
                for j in range(4):
                    to = rows_of(near_to[k, 16 * i + 4 * g + j])
                    at = 32 * g + 8 * j
                    accumulators[g][to, :] += result[
                        at : at + 8, (g // 2) * LANES : (g // 2 + 1) * LANES
                    ]
        return carry

    lax.fori_loop(0, blocks, near_step, 0)
    for h in range(LEAVES // 2):
        low = rows_of(2 * h * VECTORS)
        high = rows_of((2 * h + 1) * VECTORS)
        placed = pick_two(lane, acc0[low, :] + acc2[low, :], acc1[high, :] + acc3[high, :])
        moved = pick_two(lane, acc0[high, :] + acc2[high, :], acc1[low, :] + acc3[low, :])
        field[h] = placed + pltpu.roll(moved, CAPACITY, 1)

    for copy in parent_copies:
        copy.wait()
    square = (RANK, RANK)
    product = (
        lax.broadcasted_iota(jnp.int32, square, 0) == lax.broadcasted_iota(jnp.int32, square, 1)
    ).astype(F32)
    products = []
    for level in range(LEVELS):
        parent = parents[level].astype(F32)
        own_half = jnp.where(
            ((device >> level) & 1) == 1, pltpu.roll(parent, RANK, 1), parent
        )[:, :RANK]
        product = dot_nt(product.astype(BF16), own_half.astype(BF16))
        products.append(product.astype(BF16))

    copies[9].wait()
    for group in range(LEAVES // 8):
        rows = []
        for i in range(8):
            leaf = group * 8 + i
            rows.append(
                jnp.concatenate(
                    [
                        pick_four(
                            lane,
                            *[leaf_table[rows_of(far_from[4 * q + m, leaf]), :] for m in range(4)],
                        )
                        for q in range(FAR // 4)
                    ],
                    axis=1,
                )
            )
        result = dot_nt(
            jnp.concatenate(rows, axis=0).astype(BF16),
            far[group * 8 : group * 8 + 8].reshape(8 * RANK_LEAF, FAR * RANK_LEAF),
        )
        for h in range(2):
            field[LEAF_AT + group * 2 + h] = pick_four(
                lane,
                *[
                    result[(4 * h + j) * 8 : (4 * h + j + 1) * 8, h * LANES : (h + 1) * LANES]
                    for j in range(4)
                ],
            )
    copies[10].wait()
    rows = []
    for c in range(GROUPS):
        rows.append(
            jnp.concatenate(
                [
                    pick_two(
                        lane,
                        mid_table[rows_of(mid_from[c, 2 * q]), :],
                        mid_table[rows_of(mid_from[c, 2 * q + 1]), :],
                    )
                    for q in range(MID_FAR // 2)
                ],
                axis=1,
            )
        )
    result = dot_nt(
        jnp.concatenate(rows, axis=0).astype(BF16),
        mid_coupling[...].reshape(GROUPS * RANK, MID_FAR * RANK),
    )
    for h in range(GROUPS // 2):
        span = slice(h * LANES, (h + 1) * LANES)
        field[MID_AT + h] = pick_two(
            lane, result[16 * h : 16 * h + 8, span], result[16 * h + 8 : 16 * h + 16, span]
        )
    field_out = pltpu.make_async_copy(field, field_hbm, out_sem.at[0])
    field_out.start()

    copies[11].wait()
    tops = top_coupling.shape[2]
    level = lax.broadcasted_iota(jnp.int32, (VECTORS, tops), 0) + 1
    column = BOXES - lax.shift_right_logical(jnp.full_like(level, BOXES), level - 1)
    column = column + lax.shift_right_logical(jnp.full_like(level, 1) * device, level)
    wanted = (lane_index((VECTORS, tops)) == column).astype(F32).astype(BF16)
    for r in range(RANK):
        result = dot_nt(wanted, top_coupling[r])
        chosen_low[r * VECTORS : (r + 1) * VECTORS, :] = result[:, :LANES]
        chosen_high[r * VECTORS : (r + 1) * VECTORS, 0:RANK] = result[:, LANES:]
    copies[8].wait()
    coupling[0] = box_coupling[0]
    for k in range(LEVELS):
        rows = pl.ds(k, RANK, stride=VECTORS)
        chosen = jnp.concatenate([chosen_low[rows, :], chosen_high[rows, :][:, :RANK]], axis=1)
        coupling[k + 1] = dot_nn(products[k], chosen.astype(BF16)).astype(BF16)
    coupling_out = pltpu.make_async_copy(coupling, coupling_hbm, out_sem.at[1])
    coupling_out.start()
    field_out.wait()
    coupling_out.wait()


def down_kernel(
    every_hbm,
    top_hbm,
    coupling_hbm,
    mid_hbm,
    leaf_hbm,
    field_hbm,
    basis_hbm,
    out,
    every,
    top_transfer,
    coupling,
    mid_transfer,
    leaf_transfer,
    field,
    basis,
    sem,
    pairs0,
    pairs1,
    pairs2,
    pairs3,
    pairs4,
    pairs5,
):
    half = pl.ds(0, BOXES // 2)
    rest = pl.ds(BOXES // 2, BOXES // 2 - 4)
    copies = [
        pltpu.make_async_copy(source, target, sem.at[i])
        for i, (source, target) in enumerate(
            (
                (every_hbm, every),
                (top_hbm.at[half], top_transfer.at[half]),
                (top_hbm.at[rest], top_transfer.at[rest]),
                (coupling_hbm, coupling),
                (mid_hbm, mid_transfer),
                (leaf_hbm, leaf_transfer),
                (field_hbm, field),
                (basis_hbm, basis),
            )
        )
    ]
    for copy in copies:
        copy.start()
    device = lax.axis_index("clusters")
    lane = lane_index((VECTORS, LANES))
    zero = jnp.zeros((VECTORS, LANES), F32)
    empty = jnp.zeros((2 * VECTORS, LANES), BF16)

    pairs = (pairs0, pairs1, pairs2, pairs3, pairs4, pairs5)
    for level in range(LEVELS + 1):
        pairs[level][0] = zero
        pairs[level][(BOXES >> (level + 1)) + 1] = zero
    copies[0].wait()
    kept = (lane < RANK) == (lax.broadcasted_iota(jnp.int32, (VECTORS, LANES), 0) < 4)
    for p in range(BOXES // 2):
        tile = every[p].astype(F32)
        pairs0[p + 1] = jnp.where(kept, tile, pltpu.roll(pltpu.roll(tile, RANK, 1), 4, 0))
    for level in range(LEVELS):
        if level < 2:
            copies[1 + level].wait()
        start = BOXES - (BOXES >> level)
        count = BOXES >> (level + 1)
        for g in range(0, count, 8):
            left, right = [], []
            for quad in range(g, min(g + 8, count), 4):
                low = jnp.concatenate([pairs[level][1 + quad], pairs[level][2 + quad]], axis=0)
                high = jnp.concatenate([pairs[level][3 + quad], pairs[level][4 + quad]], axis=0)
                left.append(jnp.concatenate([low.astype(BF16), empty], axis=1))
                left.append(jnp.concatenate([empty, high.astype(BF16)], axis=1))
                at = start + quad
                right.append(jnp.concatenate([top_transfer[at], top_transfer[at + 2]], axis=1))
                right.append(jnp.concatenate([top_transfer[at + 1], top_transfer[at + 3]], axis=1))
            result = dot_nt(jnp.concatenate(left, axis=0), jnp.concatenate(right, axis=0))
            for i in range(len(left)):
                span = slice((i // 2) * LANES, (i // 2 + 1) * LANES)
                pairs[level + 1][1 + g // 2 + i] = pick_two(
                    lane, result[16 * i : 16 * i + 8, span], result[16 * i + 8 : 16 * i + 16, span]
                )
    copies[3].wait()
    down = jnp.zeros((VECTORS, RANK), F32)
    for level in range(LEVELS + 1):
        cluster = device >> level
        parent = cluster >> 1
        before = pairs[level][parent]
        after = pltpu.roll(pairs[level][parent + 2], 64, 1)
        middle = jnp.where((cluster & 1) == 1, before, after)
        stacked = jnp.concatenate([pick_two(lane, before, middle), after[:, :64]], axis=1)
        down = down + dot_nt(stacked.astype(BF16), coupling[level])

    copies[4].wait()
    mid_push = dot_nn(down.astype(BF16), mid_transfer[0])
    copies[5].wait()
    copies[6].wait()
    rows = []
    for c in range(GROUPS):
        h = c // 2
        tile = field[MID_AT + h] + mid_push[:, h * LANES : (h + 1) * LANES]
        half_tile = pick_two(lane, tile, zero) if c % 2 == 0 else pick_two(lane, zero, tile)
        rows.append(
            jnp.concatenate([half_tile if i == h else zero for i in range(GROUPS // 2)], axis=1)
        )
    leaf_push = dot_nn(
        jnp.concatenate(rows, axis=0).astype(BF16),
        leaf_transfer[...].reshape(GROUPS * RANK, CHILDREN * RANK_LEAF),
    )
    copies[7].wait()
    lane_group = lane // RANK_LEAF
    for first in range(0, LEAVES // 4, 8):
        rows, weights = [], []
        for g in range(first, first + 8):
            push = leaf_push[(g // 2) * 8 : (g // 2) * 8 + 8, (g % 2) * LANES : (g % 2 + 1) * LANES]
            leaf_down = field[LEAF_AT + g] + push
            for j in range(4):
                block = jnp.where(lane_group == g % 4, turn(leaf_down, g % 4 - j), 0.0)
                rows.append(
                    jnp.concatenate([block, zero] if g % 8 < 4 else [zero, block], axis=1)
                )
            weights.append(basis[:, pl.ds(g * 4 * CAPACITY, 4 * CAPACITY)])
        result = dot_nn(
            jnp.concatenate(rows, axis=0).astype(BF16), jnp.concatenate(weights, axis=0)
        )
        for g in range(first, first + 8):
            for h in range(2):
                span = slice(h * LANES, (h + 1) * LANES)
                at = 32 * (g % 8) + 16 * h
                far_tile = pick_two(lane, result[at : at + 8, span], result[at + 8 : at + 16, span])
                out[:, pl.ds((2 * g + h) * LANES, LANES)] = (far_tile + field[2 * g + h]).astype(
                    BF16
                )


def body(
    charges,
    leaf_basis,
    leaf_transfer,
    mid_transfer,
    far_source,
    far_coupling,
    mid_source,
    mid_coupling,
    box_coupling,
    top_transfer,
    top_coupling,
    near_target,
    near_source,
    near_count,
    near_blocks,
):
    pair = [(i, i ^ 1) for i in range(BOXES)]
    other = [(i, min(max(((i + 1) ^ 1) - 1, 0), BOXES - 1)) for i in range(BOXES)]
    vmem = pl.BlockSpec(memory_space=pltpu.VMEM)
    hbm = pl.BlockSpec(memory_space=pltpu.HBM)
    shape = jax.ShapeDtypeStruct
    scratch = pltpu.VMEM
    dma = pltpu.SemaphoreType.DMA
    packed, message = pl.pallas_call(
        up_kernel,
        out_shape=(shape((VECTORS, WIDE), BF16), shape((BOXES // 2, VECTORS, LANES), BF16)),
        in_specs=[hbm] * 4,
        out_specs=(hbm, hbm),
        scratch_shapes=[
            scratch((VECTORS, POINTS), BF16),
            scratch((RANK_LEAF, POINTS), BF16),
            scratch((GROUPS, RANK, CHILDREN * RANK_LEAF), BF16),
            scratch((1, RANK, GROUPS * RANK), BF16),
            scratch((VECTORS, LEAF_LANES + MID_LANES), BF16),
            scratch((MESSAGES, VECTORS, LANES), BF16),
            dma((4,)),
            dma((2 + BOXES // 2 // MESSAGES,)),
        ],
        cost_estimate=pl.CostEstimate(flops=10**9, bytes_accessed=10**6, transcendentals=0),
        compiler_params=pltpu.CompilerParams(vmem_limit_bytes=VMEM_LIMIT),
        name="upward",
    )(charges, leaf_basis, leaf_transfer, mid_transfer)
    packed_other = lax.ppermute(packed, "clusters", other)
    packed_pair = lax.ppermute(packed, "clusters", pair)
    every = lax.all_to_all(message.reshape(BOXES, VECTORS // 2, LANES), "clusters", 0, 0)
    table = scratch((3 * LEAVES * VECTORS, LANES), F32)
    accumulator = scratch(((LEAVES + 1) * VECTORS, LANES), F32)
    indices = [
        (VECTORS, LANES),
        (VECTORS, LANES),
        (FAR, LEAVES),
        (GROUPS, MID_FAR),
    ]
    wide = scratch((VECTORS, WIDE), BF16)
    field, coupling = pl.pallas_call(
        side_kernel,
        out_shape=(
            shape((FIELDS, VECTORS, LANES), F32),
            shape((LEVELS + 1, RANK, 3 * RANK), BF16),
        ),
        in_specs=[hbm] * 14,
        out_specs=(hbm, hbm),
        scratch_shapes=[scratch(i, jnp.int32) for i in indices]
        + [
            wide,
            wide,
            wide,
            scratch((LEAVES, RANK_LEAF, FAR * RANK_LEAF), BF16),
            scratch((GROUPS, RANK, MID_FAR * RANK), BF16),
            scratch((RANK, 3 * RANK, BOXES - 4), BF16),
            scratch((LEVELS, RANK, 2 * RANK), BF16),
            scratch((1, RANK, 3 * RANK), BF16),
            scratch((PARTS, CAPACITY, PART), BF16),
            scratch((FIELDS, VECTORS, LANES), F32),
            scratch((LEVELS + 1, RANK, 3 * RANK), BF16),
            table,
            table,
            table,
            scratch((3 * GROUPS * VECTORS, LANES), F32),
            accumulator,
            accumulator,
            accumulator,
            accumulator,
            scratch((RANK * VECTORS, LANES), F32),
            scratch((RANK * VECTORS, LANES), F32),
        ]
        + [scratch(i, jnp.int32) for i in indices]
        + [pltpu.SMEM((1, 1), jnp.int32)]
        + [pltpu.SMEM(i, jnp.int32) for i in indices]
        + [dma((PARTS,)), dma((12,)), dma((LEVELS,)), dma((4,)), dma((2,))],
        cost_estimate=pl.CostEstimate(flops=2 * 10**9, bytes_accessed=10**7, transcendentals=0),
        compiler_params=pltpu.CompilerParams(vmem_limit_bytes=VMEM_LIMIT),
        name="side",
    )(
        near_source.reshape(VECTORS, LANES),
        near_target.reshape(VECTORS, LANES),
        near_count.reshape(1, 1),
        far_source.T,
        mid_source,
        packed,
        packed_pair,
        packed_other,
        far_coupling,
        mid_coupling,
        jnp.transpose(top_coupling, (1, 2, 0)),
        top_transfer,
        box_coupling,
        near_blocks,
    )
    return pl.pallas_call(
        down_kernel,
        out_shape=shape((VECTORS, POINTS), BF16),
        in_specs=[hbm] * 7,
        out_specs=vmem,
        scratch_shapes=[
            scratch((BOXES // 2, VECTORS, LANES), BF16),
            scratch((BOXES - 4, RANK, 2 * RANK), BF16),
            scratch((LEVELS + 1, RANK, 3 * RANK), BF16),
            scratch((1, RANK, GROUPS * RANK), BF16),
            scratch((GROUPS, RANK, CHILDREN * RANK_LEAF), BF16),
            scratch((FIELDS, VECTORS, LANES), F32),
            scratch((RANK_LEAF, POINTS), BF16),
            dma((8,)),
        ]
        + [
            scratch(((BOXES >> (level + 1)) + 2, VECTORS, LANES), F32)
            for level in range(LEVELS + 1)
        ],
        cost_estimate=pl.CostEstimate(flops=10**9, bytes_accessed=10**6, transcendentals=0),
        compiler_params=pltpu.CompilerParams(vmem_limit_bytes=VMEM_LIMIT),
        name="down",
    )(every.reshape(BOXES // 2, VECTORS, LANES), top_transfer, coupling, mid_transfer, leaf_transfer, field, leaf_basis)


def solution(mesh):
    in_specs = (
        P(None, "clusters"),
        P(None, "clusters"),
        P("clusters", None, None),
        P("clusters", None, None),
        P("clusters", None),
        P("clusters", None, None),
        P("clusters", None),
        P("clusters", None, None),
        P("clusters", None, None),
        P(),
        P(),
        P("clusters"),
        P("clusters"),
        P("clusters"),
        P(None, "clusters"),
    )
    out_specs = P(None, "clusters")
    return jax.shard_map(body, mesh=mesh, in_specs=in_specs, out_specs=out_specs, check_vma=False)
```

```python
import jax
import jax.numpy as jnp
from jax import lax
from jax.experimental import pallas as pl
from jax.experimental.pallas import tpu as pltpu
from jax.sharding import PartitionSpec as P

F32 = jnp.float32
BF16 = jnp.bfloat16

VECTORS = 8
LEAVES = 64
CAPACITY = 64
RANK_LEAF = 32
RANK = 64
GROUPS = 8
CHILDREN = 8
FAR = 16
MID_FAR = 8
SLOTS = 1024
BOXES = 128
LEVELS = 5
POINTS = LEAVES * CAPACITY
LEAF_LANES = LEAVES * RANK_LEAF
MID_LANES = GROUPS * RANK
PARTS = 4
PART = SLOTS * CAPACITY // PARTS
BLOCK = SLOTS // PARTS
WIDE = POINTS + LEAF_LANES + MID_LANES
LANES = 128
VMEM_LIMIT = 60 * 1024 * 1024
UP_LIMIT = 60 * 1024 * 1024
SIDE_LIMIT = 51500 * 1024
DOWN_LIMIT = 54400 * 1024
MESSAGES = 16
LEAF_AT = LEAVES // 2
MID_AT = LEAF_AT + LEAVES // 4
FIELDS = MID_AT + GROUPS // 2


HBM = pl.BlockSpec(memory_space=pltpu.HBM)


def dot_nt(left, right):
    return lax.dot_general(left, right, (((1,), (1,)), ((), ())), preferred_element_type=F32)


def dot_nn(left, right):
    return lax.dot_general(left, right, (((1,), (0,)), ((), ())), preferred_element_type=F32)


def lane_index(shape):
    return lax.broadcasted_iota(jnp.int32, shape, len(shape) - 1)


def pick_two(lane, first, second):
    return jnp.where(lane < 64, first, second)


def pick_four(lane, a, b, c, d):
    return jnp.where(lane < 64, jnp.where(lane < 32, a, b), jnp.where(lane < 96, c, d))


def turn(tile, groups):
    return tile if groups % 4 == 0 else pltpu.roll(tile, RANK_LEAF * (groups % 4), 1)


def rows_of(first):
    return pl.ds(pl.multiple_of(first, VECTORS), VECTORS)


def up_kernel(
    charges_hbm,
    basis_hbm,
    leaf_hbm,
    mid_hbm,
    top_hbm,
    packed_hbm,
    message_hbm,
    parents_hbm,
    charges,
    basis,
    leaf_transfer,
    mid_transfer,
    coefficients,
    message,
    parents,
    sem,
    out_sem,
    parent_sem,
):
    device = lax.axis_index("clusters")
    copies = [
        pltpu.make_async_copy(a, b, sem.at[i])
        for i, (a, b) in enumerate(
            (
                (charges_hbm, charges),
                (basis_hbm, basis),
                (leaf_hbm, leaf_transfer),
                (mid_hbm, mid_transfer),
            )
        )
    ]
    for copy in copies:
        copy.start()
    parent_copies = []
    for level in range(LEVELS):
        start = BOXES - (BOXES >> level)
        parent_copies.append(
            pltpu.make_async_copy(
                top_hbm.at[start + (device >> (level + 1))],
                parents.at[level],
                parent_sem.at[level],
            )
        )
        parent_copies[level].start()
    lane = lane_index((VECTORS, LANES))
    wide_lane = lane_index((VECTORS, 4 * CAPACITY)) // CAPACITY
    copies[0].wait()
    charges_out = pltpu.make_async_copy(
        charges, packed_hbm.at[:, pl.ds(0, POINTS)], out_sem.at[0]
    )
    charges_out.start()
    copies[1].wait()
    tiles = []
    for first in range(0, LEAVES // 4, 8):
        rows, weights = [], []
        for g in range(first, first + 8):
            span = pl.ds(g * 4 * CAPACITY, 4 * CAPACITY)
            x = charges[:, span].astype(F32)
            rows += [jnp.where(wide_lane == j, x, 0.0) for j in range(4)]
            weights.append(basis[:, span])
        result = dot_nt(
            jnp.concatenate(rows, axis=0).astype(BF16), jnp.concatenate(weights, axis=0)
        )
        for g in range(8):
            tile = result[32 * g : 32 * (g + 1), (g // 4) * LANES : (g // 4 + 1) * LANES]
            tiles.append(
                pick_four(lane, *[turn(tile[8 * j : 8 * (j + 1)], j - g % 4) for j in range(4)])
            )
    for g in range(LEAVES // 4):
        coefficients[:, pl.ds(g * LANES, LANES)] = tiles[g].astype(BF16)
    stacked = jnp.concatenate(
        [jnp.concatenate([tiles[2 * c], tiles[2 * c + 1]], axis=1) for c in range(GROUPS)], axis=0
    ).astype(BF16)
    copies[2].wait()
    result = dot_nt(stacked, leaf_transfer[...].reshape(GROUPS * RANK, CHILDREN * RANK_LEAF))
    mid = []
    for h in range(GROUPS // 2):
        span = slice(h * LANES, (h + 1) * LANES)
        low = result[16 * h : 16 * h + 8, span]
        high = result[16 * h + 8 : 16 * h + 16, span]
        mid.append(pick_two(lane, low, high).astype(BF16))
        coefficients[:, pl.ds(LEAF_LANES + h * LANES, LANES)] = mid[h]
    coefficients_out = pltpu.make_async_copy(
        coefficients, packed_hbm.at[:, pl.ds(POINTS, LEAF_LANES + MID_LANES)], out_sem.at[1]
    )
    coefficients_out.start()
    for copy in parent_copies:
        copy.wait()
    parents_out = pltpu.make_async_copy(parents, parents_hbm, parent_sem.at[LEVELS])
    parents_out.start()
    copies[3].wait()
    box = dot_nt(jnp.concatenate(mid, axis=1), mid_transfer[0])
    box = jnp.concatenate([box[:4], box[4:]], axis=1)
    box = jnp.concatenate([box, box], axis=0).astype(BF16)
    message[...] = jnp.broadcast_to(box[None], message.shape)
    messages_out = [
        pltpu.make_async_copy(
            message, message_hbm.at[pl.ds(i * MESSAGES, MESSAGES)], out_sem.at[2 + i]
        )
        for i in range(BOXES // 2 // MESSAGES)
    ]
    for copy in messages_out:
        copy.start()
    charges_out.wait()
    coefficients_out.wait()
    parents_out.wait()
    for copy in messages_out:
        copy.wait()


def side_kernel(
    near_source_hbm,
    near_target_hbm,
    near_count_hbm,
    far_source_hbm,
    mid_source_hbm,
    own_hbm,
    pair_hbm,
    other_hbm,
    far,
    mid_coupling,
    top_coupling_hbm,
    parents_hbm,
    box_coupling_hbm,
    near_hbm,
    field_hbm,
    coupling_hbm,
    near_source,
    near_target,
    far_source,
    mid_source,
    own,
    pair,
    other,
    top_coupling,
    parents,
    box_coupling,
    near,
    field,
    coupling,
    x_low,
    x_high,
    leaf_table,
    mid_table,
    acc0,
    acc1,
    acc2,
    acc3,
    chosen_low,
    chosen_high,
    source_rows,
    target_rows,
    far_rows,
    mid_rows,
    near_count,
    near_from,
    near_to,
    far_from,
    mid_from,
    near_sem,
    sem,
    parent_sem,
    index_sem,
    out_sem,
):
    device = lax.axis_index("clusters")

    def near_copy(k):
        return pltpu.make_async_copy(
            near_hbm.at[:, pl.ds(pl.multiple_of(k * PART, PART), PART)], near.at[k], near_sem.at[k]
        )

    copies = [
        pltpu.make_async_copy(a, b, sem.at[i])
        for i, (a, b) in enumerate(
            (
                (near_count_hbm, near_count),
                (near_source_hbm, near_source),
                (near_target_hbm, near_target),
                (far_source_hbm, far_source),
                (mid_source_hbm, mid_source),
                (own_hbm, own),
                (pair_hbm, pair),
                (other_hbm, other),
                (box_coupling_hbm, box_coupling),
                (top_coupling_hbm, top_coupling),
            )
        )
    ]
    parent_copies = [pltpu.make_async_copy(parents_hbm, parents, parent_sem)]
    for copy in copies[:8]:
        copy.start()
    near_copy(0).start()
    for copy in parent_copies:
        copy.start()
    copies[8].start()

    for copy in copies[:5]:
        copy.wait()
    live = near_count[0, 0]
    leaf_base = (device - 1) * LEAVES
    shape = (VECTORS, LANES)
    slot = lax.broadcasted_iota(jnp.int32, shape, 0) * LANES + lane_index(shape)
    used = slot < live
    source_rows[...] = jnp.where(used, near_source[...] - leaf_base, LEAVES) * VECTORS
    target_rows[...] = jnp.where(used, near_target[...], LEAVES) * VECTORS
    far_rows[...] = (far_source[...] - leaf_base) * VECTORS
    mid_rows[...] = (mid_source[...] - (device - 1) * GROUPS) * VECTORS
    index_copies = [
        pltpu.make_async_copy(a, b, index_sem.at[i])
        for i, (a, b) in enumerate(
            (
                (source_rows, near_from),
                (target_rows, near_to),
                (far_rows, far_from),
                (mid_rows, mid_from),
            )
        )
    ]
    for copy in index_copies:
        copy.start()
    blocks = jnp.clip((live + BLOCK - 1) // BLOCK, 1, PARTS)

    @pl.when(blocks > 1)
    def _():
        near_copy(1).start()

    lane = lane_index((VECTORS, LANES))
    zero = jnp.zeros((VECTORS, LANES), F32)
    odd = device % 2
    accumulators = (acc0, acc1, acc2, acc3)
    for acc in accumulators:
        acc[...] = jnp.zeros(acc.shape, F32)
    for copy in copies[5:8]:
        copy.wait()
    for source, region in ((own, 1), (pair, (1 - odd) * 2), (other, odd * 2)):
        base = region * LEAVES * VECTORS
        for h in range(LEAVES // 2):
            tile = source[:, pl.ds(h * LANES, LANES)].astype(F32)
            turned = pltpu.roll(tile, 64, 1)
            at = base + 2 * h * VECTORS
            x_low[rows_of(at), :] = pick_two(lane, tile, zero)
            x_high[rows_of(at), :] = pick_two(lane, zero, turned)
            x_low[rows_of(at + VECTORS), :] = pick_two(lane, turned, zero)
            x_high[rows_of(at + VECTORS), :] = pick_two(lane, zero, tile)
        for h in range(LEAVES // 4):
            tile = source[:, pl.ds(POINTS + h * LANES, LANES)].astype(F32)
            turns = [tile] + [pltpu.roll(tile, 32 * i, 1) for i in range(1, 4)]
            for j in range(4):
                leaf_table[rows_of(base + (4 * h + j) * VECTORS), :] = pick_four(
                    lane, *[turns[(group - j) % 4] for group in range(4)]
                )
        base = region * GROUPS * VECTORS
        for h in range(GROUPS // 2):
            tile = source[:, pl.ds(POINTS + LEAF_LANES + h * LANES, LANES)].astype(F32)
            turned = pltpu.roll(tile, 64, 1)
            at = base + 2 * h * VECTORS
            mid_table[rows_of(at), :] = pick_two(lane, tile, turned)
            mid_table[rows_of(at + VECTORS), :] = pick_two(lane, turned, tile)
    for copy in index_copies:
        copy.wait()

    zeros_half = jnp.zeros((2 * VECTORS, LANES), BF16)

    def near_step(k, carry):
        @pl.when(k + 2 < blocks)
        def _():
            near_copy(k + 2).start()

        @pl.when(k == 0)
        def _():
            copies[9].start()

        near_copy(k).wait()
        sources = [near_from.at[2 * k + i] for i in range(2)]
        targets = [near_to.at[2 * k + i] for i in range(2)]
        for i in range(BLOCK // 16):
            rows, weights = [], []
            for g in range(4):
                first = 16 * i + 4 * g
                at = [rows_of(sources[first // LANES][first % LANES + j]) for j in range(4)]
                top = jnp.concatenate([x_low[at[0], :], x_high[at[1], :]], axis=0)
                bottom = jnp.concatenate([x_low[at[2], :], x_high[at[3], :]], axis=0)
                rows.append(jnp.concatenate([top.astype(BF16), zeros_half], axis=1))
                rows.append(jnp.concatenate([zeros_half, bottom.astype(BF16)], axis=1))
                weights.append(near[k, :, first * CAPACITY : (first + 4) * CAPACITY])
            result = dot_nt(jnp.concatenate(rows, axis=0), jnp.concatenate(weights, axis=0))
            for g in range(4):
                first = 16 * i + 4 * g
                for j in range(4):
                    to = rows_of(targets[first // LANES][first % LANES + j])
                    at = 32 * g + 8 * j
                    accumulators[g][to, :] += result[
                        at : at + 8, (g // 2) * LANES : (g // 2 + 1) * LANES
                    ]
        return carry

    lax.fori_loop(0, blocks, near_step, 0)
    for h in range(LEAVES // 2):
        low = rows_of(2 * h * VECTORS)
        high = rows_of((2 * h + 1) * VECTORS)
        placed = pick_two(lane, acc0[low, :] + acc2[low, :], acc1[high, :] + acc3[high, :])
        moved = pick_two(lane, acc0[high, :] + acc2[high, :], acc1[low, :] + acc3[low, :])
        field[h] = placed + pltpu.roll(moved, CAPACITY, 1)

    for copy in parent_copies:
        copy.wait()
    square = (RANK, RANK)
    product = (
        lax.broadcasted_iota(jnp.int32, square, 0) == lax.broadcasted_iota(jnp.int32, square, 1)
    ).astype(F32)
    products = []
    for level in range(LEVELS):
        parent = parents[level].astype(F32)
        own_half = jnp.where(
            ((device >> level) & 1) == 1, pltpu.roll(parent, RANK, 1), parent
        )[:, :RANK]
        product = dot_nt(product.astype(BF16), own_half.astype(BF16))
        products.append(product.astype(BF16))

    for group in range(LEAVES // 8):
        rows = []
        for i in range(8):
            leaf = group * 8 + i
            rows.append(
                jnp.concatenate(
                    [
                        pick_four(
                            lane,
                            *[leaf_table[rows_of(far_from[4 * q + m, leaf]), :] for m in range(4)],
                        )
                        for q in range(FAR // 4)
                    ],
                    axis=1,
                )
            )
        result = dot_nt(
            jnp.concatenate(rows, axis=0).astype(BF16),
            far[group * 8 : group * 8 + 8].reshape(8 * RANK_LEAF, FAR * RANK_LEAF),
        )
        for h in range(2):
            field[LEAF_AT + group * 2 + h] = pick_four(
                lane,
                *[
                    result[(4 * h + j) * 8 : (4 * h + j + 1) * 8, h * LANES : (h + 1) * LANES]
                    for j in range(4)
                ],
            )
    rows = []
    for c in range(GROUPS):
        rows.append(
            jnp.concatenate(
                [
                    pick_two(
                        lane,
                        mid_table[rows_of(mid_from[c, 2 * q]), :],
                        mid_table[rows_of(mid_from[c, 2 * q + 1]), :],
                    )
                    for q in range(MID_FAR // 2)
                ],
                axis=1,
            )
        )
    result = dot_nt(
        jnp.concatenate(rows, axis=0).astype(BF16),
        mid_coupling[...].reshape(GROUPS * RANK, MID_FAR * RANK),
    )
    for h in range(GROUPS // 2):
        span = slice(h * LANES, (h + 1) * LANES)
        field[MID_AT + h] = pick_two(
            lane, result[16 * h : 16 * h + 8, span], result[16 * h + 8 : 16 * h + 16, span]
        )
    field_out = pltpu.make_async_copy(field, field_hbm, out_sem.at[0])
    field_out.start()

    copies[9].wait()
    level = lax.broadcasted_iota(jnp.int32, (VECTORS, LANES), 0) + 1
    column = BOXES - lax.shift_right_logical(jnp.full_like(level, BOXES), level - 1)
    column = column + lax.shift_right_logical(jnp.full_like(level, 1) * device, level)
    wanted = (lane_index(level.shape) == column).astype(F32)
    nothing = jnp.zeros_like(wanted)
    wanted = jnp.concatenate(
        [
            jnp.concatenate([wanted, nothing], axis=1),
            jnp.concatenate([nothing, wanted], axis=1),
        ],
        axis=0,
    ).astype(BF16)
    missing = jnp.zeros((3 * RANK, 4), BF16)
    for r in range(0, RANK, 2):
        columns = [
            jnp.concatenate([top_coupling[r + i], missing], axis=1) for i in range(2)
        ]
        result = dot_nt(wanted, jnp.concatenate(columns, axis=1))
        rows = slice(r * VECTORS, (r + 2) * VECTORS)
        chosen_low[rows, :] = result[:, :LANES]
        chosen_high[rows, 0:RANK] = result[:, LANES:]
    copies[8].wait()
    coupling[0] = box_coupling[0]
    for k in range(LEVELS):
        rows = pl.ds(k, RANK, stride=VECTORS)
        chosen = jnp.concatenate([chosen_low[rows, :], chosen_high[rows, :][:, :RANK]], axis=1)
        coupling[k + 1] = dot_nn(products[k], chosen.astype(BF16)).astype(BF16)
    coupling_out = pltpu.make_async_copy(coupling, coupling_hbm, out_sem.at[1])
    coupling_out.start()
    field_out.wait()
    coupling_out.wait()


def down_kernel(
    every,
    top_hbm,
    coupling,
    mid_hbm,
    leaf_hbm,
    field,
    basis_hbm,
    out,
    top_transfer,
    mid_transfer,
    leaf_transfer,
    basis,
    sem,
    pairs0,
    pairs1,
    pairs2,
    pairs3,
    pairs4,
    pairs5,
):
    half = pl.ds(0, BOXES // 2)
    rest = pl.ds(BOXES // 2, BOXES // 2 - 4)
    copies = [
        pltpu.make_async_copy(source, target, sem.at[i])
        for i, (source, target) in enumerate(
            (
                (top_hbm.at[half], top_transfer.at[half]),
                (top_hbm.at[rest], top_transfer.at[rest]),
                (mid_hbm, mid_transfer),
                (leaf_hbm, leaf_transfer),
                (basis_hbm, basis),
            )
        )
    ]
    for copy in copies:
        copy.start()
    device = lax.axis_index("clusters")
    lane = lane_index((VECTORS, LANES))
    zero = jnp.zeros((VECTORS, LANES), F32)
    empty = jnp.zeros((2 * VECTORS, LANES), BF16)

    pairs = (pairs0, pairs1, pairs2, pairs3, pairs4, pairs5)
    for level in range(LEVELS + 1):
        pairs[level][0] = zero
        pairs[level][(BOXES >> (level + 1)) + 1] = zero
    kept = (lane < RANK) == (lax.broadcasted_iota(jnp.int32, (VECTORS, LANES), 0) < 4)
    for p in range(BOXES // 2):
        tile = every[p].astype(F32)
        pairs0[p + 1] = jnp.where(kept, tile, pltpu.roll(pltpu.roll(tile, RANK, 1), 4, 0))
    for level in range(LEVELS):
        if level < 2:
            copies[level].wait()
        start = BOXES - (BOXES >> level)
        count = BOXES >> (level + 1)
        for g in range(0, count, 8):
            left, right = [], []
            for quad in range(g, min(g + 8, count), 4):
                low = jnp.concatenate([pairs[level][1 + quad], pairs[level][2 + quad]], axis=0)
                high = jnp.concatenate([pairs[level][3 + quad], pairs[level][4 + quad]], axis=0)
                left.append(jnp.concatenate([low.astype(BF16), empty], axis=1))
                left.append(jnp.concatenate([empty, high.astype(BF16)], axis=1))
                at = start + quad
                right.append(jnp.concatenate([top_transfer[at], top_transfer[at + 2]], axis=1))
                right.append(jnp.concatenate([top_transfer[at + 1], top_transfer[at + 3]], axis=1))
            result = dot_nt(jnp.concatenate(left, axis=0), jnp.concatenate(right, axis=0))
            for i in range(len(left)):
                span = slice((i // 2) * LANES, (i // 2 + 1) * LANES)
                pairs[level + 1][1 + g // 2 + i] = pick_two(
                    lane, result[16 * i : 16 * i + 8, span], result[16 * i + 8 : 16 * i + 16, span]
                )
    down = jnp.zeros((VECTORS, RANK), F32)
    for level in range(LEVELS + 1):
        cluster = device >> level
        parent = cluster >> 1
        before = pairs[level][parent]
        after = pltpu.roll(pairs[level][parent + 2], 64, 1)
        middle = jnp.where((cluster & 1) == 1, before, after)
        stacked = jnp.concatenate([pick_two(lane, before, middle), after[:, :64]], axis=1)
        down = down + dot_nt(stacked.astype(BF16), coupling[level])

    copies[2].wait()
    mid_push = dot_nn(down.astype(BF16), mid_transfer[0])
    copies[3].wait()
    rows = []
    for c in range(GROUPS):
        h = c // 2
        tile = field[MID_AT + h] + mid_push[:, h * LANES : (h + 1) * LANES]
        half_tile = pick_two(lane, tile, zero) if c % 2 == 0 else pick_two(lane, zero, tile)
        rows.append(
            jnp.concatenate([half_tile if i == h else zero for i in range(GROUPS // 2)], axis=1)
        )
    leaf_push = dot_nn(
        jnp.concatenate(rows, axis=0).astype(BF16),
        leaf_transfer[...].reshape(GROUPS * RANK, CHILDREN * RANK_LEAF),
    )
    copies[4].wait()
    lane_group = lane // RANK_LEAF
    for first in range(0, LEAVES // 4, 8):
        rows, weights = [], []
        for g in range(first, first + 8):
            push = leaf_push[(g // 2) * 8 : (g // 2) * 8 + 8, (g % 2) * LANES : (g % 2 + 1) * LANES]
            leaf_down = field[LEAF_AT + g] + push
            for j in range(4):
                block = jnp.where(lane_group == g % 4, turn(leaf_down, g % 4 - j), 0.0)
                rows.append(
                    jnp.concatenate([block, zero] if g % 8 < 4 else [zero, block], axis=1)
                )
            weights.append(basis[:, pl.ds(g * 4 * CAPACITY, 4 * CAPACITY)])
        result = dot_nn(
            jnp.concatenate(rows, axis=0).astype(BF16), jnp.concatenate(weights, axis=0)
        )
        for g in range(first, first + 8):
            for h in range(2):
                span = slice(h * LANES, (h + 1) * LANES)
                at = 32 * (g % 8) + 16 * h
                far_tile = pick_two(lane, result[at : at + 8, span], result[at + 8 : at + 16, span])
                out[:, pl.ds((2 * g + h) * LANES, LANES)] = (far_tile + field[2 * g + h]).astype(
                    BF16
                )


def up_call(*operands):
    hbm, shape, scratch = HBM, jax.ShapeDtypeStruct, pltpu.VMEM
    dma = pltpu.SemaphoreType.DMA
    return pl.pallas_call(
        up_kernel,
        out_shape=(
            shape((VECTORS, WIDE), BF16),
            shape((BOXES // 2, VECTORS, LANES), BF16),
            shape((LEVELS, RANK, 2 * RANK), BF16),
        ),
        in_specs=[hbm] * 5,
        out_specs=(hbm, hbm, hbm),
        scratch_shapes=[
            scratch((VECTORS, POINTS), BF16),
            scratch((RANK_LEAF, POINTS), BF16),
            scratch((GROUPS, RANK, CHILDREN * RANK_LEAF), BF16),
            scratch((1, RANK, GROUPS * RANK), BF16),
            scratch((VECTORS, LEAF_LANES + MID_LANES), BF16),
            scratch((MESSAGES, VECTORS, LANES), BF16),
            scratch((LEVELS, RANK, 2 * RANK), BF16),
            dma((4,)),
            dma((2 + BOXES // 2 // MESSAGES,)),
            dma((LEVELS + 1,)),
        ],
        cost_estimate=pl.CostEstimate(flops=10**9, bytes_accessed=10**6, transcendentals=0),
        compiler_params=pltpu.CompilerParams(vmem_limit_bytes=UP_LIMIT),
        name="upward",
    )(*operands)


def side_call(
    near_source,
    near_target,
    near_count,
    far_source,
    mid_source,
    packed,
    packed_pair,
    packed_other,
    far_coupling,
    mid_coupling,
    top_coupling,
    parents,
    box_coupling,
    near_blocks,
):
    hbm, shape, scratch = HBM, jax.ShapeDtypeStruct, pltpu.VMEM
    dma = pltpu.SemaphoreType.DMA
    table = scratch((3 * LEAVES * VECTORS, LANES), F32)
    accumulator = scratch(((LEAVES + 1) * VECTORS, LANES), F32)
    indices = [
        (VECTORS, LANES),
        (VECTORS, LANES),
        (FAR, LEAVES),
        (GROUPS, MID_FAR),
    ]
    wide = scratch((VECTORS, WIDE), BF16)
    return pl.pallas_call(
        side_kernel,
        out_shape=(
            shape((FIELDS, VECTORS, LANES), F32),
            shape((LEVELS + 1, RANK, 3 * RANK), BF16),
        ),
        in_specs=[hbm] * 8 + [pl.BlockSpec(memory_space=pltpu.VMEM)] * 2 + [hbm] * 4,
        out_specs=(hbm, hbm),
        scratch_shapes=[scratch(i, jnp.int32) for i in indices]
        + [
            wide,
            wide,
            wide,
            scratch((RANK, 3 * RANK, BOXES - 4), BF16),
            scratch((LEVELS, RANK, 2 * RANK), BF16),
            scratch((1, RANK, 3 * RANK), BF16),
            scratch((PARTS, CAPACITY, PART), BF16),
            scratch((FIELDS, VECTORS, LANES), F32),
            scratch((LEVELS + 1, RANK, 3 * RANK), BF16),
            table,
            table,
            table,
            scratch((3 * GROUPS * VECTORS, LANES), F32),
            accumulator,
            accumulator,
            accumulator,
            accumulator,
            scratch((RANK * VECTORS, LANES), F32),
            scratch((RANK * VECTORS, LANES), F32),
        ]
        + [scratch(i, jnp.int32) for i in indices]
        + [pltpu.SMEM((1, 1), jnp.int32)]
        + [pltpu.SMEM(i, jnp.int32) for i in indices]
        + [dma((PARTS,)), dma((10,)), dma, dma((4,)), dma((2,))],
        cost_estimate=pl.CostEstimate(flops=2 * 10**9, bytes_accessed=10**7, transcendentals=0),
        compiler_params=pltpu.CompilerParams(vmem_limit_bytes=SIDE_LIMIT),
        name="side",
    )(
        near_source.reshape(VECTORS, LANES),
        near_target.reshape(VECTORS, LANES),
        near_count.reshape(1, 1),
        far_source.T,
        mid_source,
        packed,
        packed_pair,
        packed_other,
        far_coupling,
        mid_coupling,
        jnp.transpose(top_coupling, (1, 2, 0)),
        parents,
        box_coupling,
        near_blocks,
    )


def down_call(*operands):
    hbm, shape, scratch = HBM, jax.ShapeDtypeStruct, pltpu.VMEM
    dma = pltpu.SemaphoreType.DMA
    vmem = pl.BlockSpec(memory_space=pltpu.VMEM)
    return pl.pallas_call(
        down_kernel,
        out_shape=shape((VECTORS, POINTS), BF16),
        in_specs=[vmem, hbm, vmem, hbm, hbm, vmem, hbm],
        out_specs=pl.BlockSpec(memory_space=pltpu.VMEM),
        scratch_shapes=[
            scratch((BOXES - 4, RANK, 2 * RANK), BF16),
            scratch((1, RANK, GROUPS * RANK), BF16),
            scratch((GROUPS, RANK, CHILDREN * RANK_LEAF), BF16),
            scratch((RANK_LEAF, POINTS), BF16),
            dma((5,)),
        ]
        + [
            scratch(((BOXES >> (level + 1)) + 2, VECTORS, LANES), F32)
            for level in range(LEVELS + 1)
        ],
        cost_estimate=pl.CostEstimate(flops=10**9, bytes_accessed=10**6, transcendentals=0),
        compiler_params=pltpu.CompilerParams(vmem_limit_bytes=DOWN_LIMIT),
        name="down",
    )(*operands)


def body(
    charges,
    leaf_basis,
    leaf_transfer,
    mid_transfer,
    far_source,
    far_coupling,
    mid_source,
    mid_coupling,
    box_coupling,
    top_transfer,
    top_coupling,
    near_target,
    near_source,
    near_count,
    near_blocks,
):
    pair = [(i, i ^ 1) for i in range(BOXES)]
    other = [(i, min(max(((i + 1) ^ 1) - 1, 0), BOXES - 1)) for i in range(BOXES)]
    packed, message, parents = up_call(
        charges, leaf_basis, leaf_transfer, mid_transfer, top_transfer
    )
    packed_other = lax.ppermute(packed, "clusters", other)
    packed_pair = lax.ppermute(packed, "clusters", pair)
    every = lax.all_to_all(message.reshape(BOXES, VECTORS // 2, LANES), "clusters", 0, 0)
    field, coupling = side_call(
        near_source,
        near_target,
        near_count,
        far_source,
        mid_source,
        packed,
        packed_pair,
        packed_other,
        far_coupling,
        mid_coupling,
        top_coupling,
        parents,
        box_coupling,
        near_blocks,
    )
    return down_call(
        every.reshape(BOXES // 2, VECTORS, LANES),
        top_transfer,
        coupling,
        mid_transfer,
        leaf_transfer,
        field,
        leaf_basis,
    )


def solution(mesh):
    in_specs = (
        P(None, "clusters"),
        P(None, "clusters"),
        P("clusters", None, None),
        P("clusters", None, None),
        P("clusters", None),
        P("clusters", None, None),
        P("clusters", None),
        P("clusters", None, None),
        P("clusters", None, None),
        P(),
        P(),
        P("clusters"),
        P("clusters"),
        P("clusters"),
        P(None, "clusters"),
    )
    out_specs = P(None, "clusters")
    return jax.shard_map(body, mesh=mesh, in_specs=in_specs, out_specs=out_specs, check_vma=False)
```

```python
import jax
import jax.numpy as jnp
from jax import lax
from jax.experimental import pallas as pl
from jax.experimental.pallas import tpu as pltpu
from jax.sharding import PartitionSpec as P

F32 = jnp.float32
BF16 = jnp.bfloat16

VECTORS = 8
LEAVES = 64
CAPACITY = 64
RANK_LEAF = 32
RANK = 64
GROUPS = 8
CHILDREN = 8
FAR = 16
MID_FAR = 8
SLOTS = 1024
BOXES = 128
LEVELS = 5
POINTS = LEAVES * CAPACITY
LEAF_LANES = LEAVES * RANK_LEAF
MID_LANES = GROUPS * RANK
PARTS = 4
PART = SLOTS * CAPACITY // PARTS
BLOCK = SLOTS // PARTS
WIDE = POINTS + LEAF_LANES + MID_LANES
LANES = 128
VMEM_LIMIT = 60 * 1024 * 1024
LOCAL = WIDE + LEVELS * RANK * LANES // VECTORS
UP_LIMIT = 60 * 1024 * 1024
SIDE_LIMIT = 51500 * 1024
DOWN_LIMIT = 54400 * 1024
MESSAGES = 16
LEAF_AT = LEAVES // 2
MID_AT = LEAF_AT + LEAVES // 4
FIELDS = MID_AT + GROUPS // 2


HBM = pl.BlockSpec(memory_space=pltpu.HBM)


def dot_nt(left, right):
    return lax.dot_general(left, right, (((1,), (1,)), ((), ())), preferred_element_type=F32)


def dot_nn(left, right):
    return lax.dot_general(left, right, (((1,), (0,)), ((), ())), preferred_element_type=F32)


def lane_index(shape):
    return lax.broadcasted_iota(jnp.int32, shape, len(shape) - 1)


def pick_two(lane, first, second):
    return jnp.where(lane < 64, first, second)


def pick_four(lane, a, b, c, d):
    return jnp.where(lane < 64, jnp.where(lane < 32, a, b), jnp.where(lane < 96, c, d))


def turn(tile, groups):
    return tile if groups % 4 == 0 else pltpu.roll(tile, RANK_LEAF * (groups % 4), 1)


def rows_of(first):
    return pl.ds(pl.multiple_of(first, VECTORS), VECTORS)


def up_kernel(
    charges_hbm,
    basis_hbm,
    leaf_hbm,
    mid_hbm,
    top_hbm,
    packed_hbm,
    message_hbm,
    local_hbm,
    charges,
    basis,
    leaf_transfer,
    mid_transfer,
    coefficients,
    message,
    parents,
    local,
    sem,
    out_sem,
    parent_sem,
):
    device = lax.axis_index("clusters")
    copies = [
        pltpu.make_async_copy(a, b, sem.at[i])
        for i, (a, b) in enumerate(
            (
                (charges_hbm, charges),
                (basis_hbm, basis),
                (leaf_hbm, leaf_transfer),
                (mid_hbm, mid_transfer),
            )
        )
    ]
    for copy in copies:
        copy.start()
    parent_copies = []
    for level in range(LEVELS):
        start = BOXES - (BOXES >> level)
        parent_copies.append(
            pltpu.make_async_copy(
                top_hbm.at[start + (device >> (level + 1))],
                parents.at[level],
                parent_sem.at[level],
            )
        )
        parent_copies[level].start()
    lane = lane_index((VECTORS, LANES))
    wide_lane = lane_index((VECTORS, 4 * CAPACITY)) // CAPACITY
    copies[0].wait()
    charges_out = pltpu.make_async_copy(
        charges, packed_hbm.at[:, pl.ds(0, POINTS)], out_sem.at[0]
    )
    charges_out.start()
    copies[1].wait()
    tiles = []
    for first in range(0, LEAVES // 4, 8):
        rows, weights = [], []
        for g in range(first, first + 8):
            span = pl.ds(g * 4 * CAPACITY, 4 * CAPACITY)
            x = charges[:, span].astype(F32)
            rows += [jnp.where(wide_lane == j, x, 0.0) for j in range(4)]
            weights.append(basis[:, span])
        result = dot_nt(
            jnp.concatenate(rows, axis=0).astype(BF16), jnp.concatenate(weights, axis=0)
        )
        for g in range(8):
            tile = result[32 * g : 32 * (g + 1), (g // 4) * LANES : (g // 4 + 1) * LANES]
            tiles.append(
                pick_four(lane, *[turn(tile[8 * j : 8 * (j + 1)], j - g % 4) for j in range(4)])
            )
    for g in range(LEAVES // 4):
        coefficients[:, pl.ds(g * LANES, LANES)] = tiles[g].astype(BF16)
    stacked = jnp.concatenate(
        [jnp.concatenate([tiles[2 * c], tiles[2 * c + 1]], axis=1) for c in range(GROUPS)], axis=0
    ).astype(BF16)
    copies[2].wait()
    result = dot_nt(stacked, leaf_transfer[...].reshape(GROUPS * RANK, CHILDREN * RANK_LEAF))
    mid = []
    for h in range(GROUPS // 2):
        span = slice(h * LANES, (h + 1) * LANES)
        low = result[16 * h : 16 * h + 8, span]
        high = result[16 * h + 8 : 16 * h + 16, span]
        mid.append(pick_two(lane, low, high).astype(BF16))
        coefficients[:, pl.ds(LEAF_LANES + h * LANES, LANES)] = mid[h]
    coefficients_out = pltpu.make_async_copy(
        coefficients, packed_hbm.at[:, pl.ds(POINTS, LEAF_LANES + MID_LANES)], out_sem.at[1]
    )
    coefficients_out.start()
    for copy in parent_copies:
        copy.wait()
    local[:, pl.ds(0, POINTS)] = charges[...]
    local[:, pl.ds(POINTS, LEAF_LANES + MID_LANES)] = coefficients[...]
    for level in range(LEVELS):
        for i in range(RANK // VECTORS):
            at = WIDE + (level * (RANK // VECTORS) + i) * LANES
            local[:, pl.ds(at, LANES)] = parents[level, i * VECTORS : (i + 1) * VECTORS, :]
    local_out = pltpu.make_async_copy(local, local_hbm, parent_sem.at[LEVELS])
    local_out.start()
    copies[3].wait()
    box = dot_nt(jnp.concatenate(mid, axis=1), mid_transfer[0])
    box = jnp.concatenate([box[:4], box[4:]], axis=1)
    box = jnp.concatenate([box, box], axis=0).astype(BF16)
    message[...] = jnp.broadcast_to(box[None], message.shape)
    messages_out = [
        pltpu.make_async_copy(
            message, message_hbm.at[pl.ds(i * MESSAGES, MESSAGES)], out_sem.at[2 + i]
        )
        for i in range(BOXES // 2 // MESSAGES)
    ]
    for copy in messages_out:
        copy.start()
    charges_out.wait()
    coefficients_out.wait()
    local_out.wait()
    for copy in messages_out:
        copy.wait()


def side_kernel(
    near_source_hbm,
    near_target_hbm,
    near_count_hbm,
    far_source_hbm,
    mid_source_hbm,
    own_hbm,
    pair_hbm,
    other_hbm,
    far,
    mid_coupling,
    top_coupling_hbm,
    box_coupling_hbm,
    near_hbm,
    field_hbm,
    coupling_hbm,
    near_source,
    near_target,
    far_source,
    mid_source,
    own,
    pair,
    other,
    top_coupling,
    box_coupling,
    near,
    field,
    coupling,
    x_low,
    x_high,
    leaf_table,
    mid_table,
    acc0,
    acc1,
    acc2,
    acc3,
    chosen_low,
    chosen_high,
    source_rows,
    target_rows,
    far_rows,
    mid_rows,
    near_count,
    near_from,
    near_to,
    far_from,
    mid_from,
    near_sem,
    sem,
    index_sem,
    out_sem,
):
    device = lax.axis_index("clusters")

    def near_copy(k):
        return pltpu.make_async_copy(
            near_hbm.at[:, pl.ds(pl.multiple_of(k * PART, PART), PART)], near.at[k], near_sem.at[k]
        )

    copies = [
        pltpu.make_async_copy(a, b, sem.at[i])
        for i, (a, b) in enumerate(
            (
                (near_count_hbm, near_count),
                (near_source_hbm, near_source),
                (near_target_hbm, near_target),
                (far_source_hbm, far_source),
                (mid_source_hbm, mid_source),
                (own_hbm, own),
                (pair_hbm, pair),
                (other_hbm, other),
                (box_coupling_hbm, box_coupling),
                (top_coupling_hbm, top_coupling),
            )
        )
    ]
    for copy in copies[:8]:
        copy.start()
    copies[9].start()
    near_copy(0).start()
    copies[8].start()

    for copy in copies[:5]:
        copy.wait()
    live = near_count[0, 0]
    leaf_base = (device - 1) * LEAVES
    shape = (VECTORS, LANES)
    slot = lax.broadcasted_iota(jnp.int32, shape, 0) * LANES + lane_index(shape)
    used = slot < live
    source_rows[...] = jnp.where(used, near_source[...] - leaf_base, LEAVES) * VECTORS
    target_rows[...] = jnp.where(used, near_target[...], LEAVES) * VECTORS
    far_rows[...] = (far_source[...] - leaf_base) * VECTORS
    mid_rows[...] = (mid_source[...] - (device - 1) * GROUPS) * VECTORS
    index_copies = [
        pltpu.make_async_copy(a, b, index_sem.at[i])
        for i, (a, b) in enumerate(
            (
                (source_rows, near_from),
                (target_rows, near_to),
                (far_rows, far_from),
                (mid_rows, mid_from),
            )
        )
    ]
    for copy in index_copies:
        copy.start()
    blocks = jnp.clip((live + BLOCK - 1) // BLOCK, 1, PARTS)

    lane = lane_index((VECTORS, LANES))
    zero = jnp.zeros((VECTORS, LANES), F32)
    odd = device % 2
    accumulators = (acc0, acc1, acc2, acc3)
    for acc in accumulators:
        acc[...] = jnp.zeros(acc.shape, F32)
    for copy in copies[5:8]:
        copy.wait()
    for source, region in ((own, 1), (pair, (1 - odd) * 2), (other, odd * 2)):
        base = region * LEAVES * VECTORS
        for h in range(LEAVES // 2):
            tile = source[:, pl.ds(h * LANES, LANES)].astype(F32)
            turned = pltpu.roll(tile, 64, 1)
            at = base + 2 * h * VECTORS
            x_low[rows_of(at), :] = pick_two(lane, tile, zero)
            x_high[rows_of(at), :] = pick_two(lane, zero, turned)
            x_low[rows_of(at + VECTORS), :] = pick_two(lane, turned, zero)
            x_high[rows_of(at + VECTORS), :] = pick_two(lane, zero, tile)
        for h in range(LEAVES // 4):
            tile = source[:, pl.ds(POINTS + h * LANES, LANES)].astype(F32)
            turns = [tile] + [pltpu.roll(tile, 32 * i, 1) for i in range(1, 4)]
            for j in range(4):
                leaf_table[rows_of(base + (4 * h + j) * VECTORS), :] = pick_four(
                    lane, *[turns[(group - j) % 4] for group in range(4)]
                )
        base = region * GROUPS * VECTORS
        for h in range(GROUPS // 2):
            tile = source[:, pl.ds(POINTS + LEAF_LANES + h * LANES, LANES)].astype(F32)
            turned = pltpu.roll(tile, 64, 1)
            at = base + 2 * h * VECTORS
            mid_table[rows_of(at), :] = pick_two(lane, tile, turned)
            mid_table[rows_of(at + VECTORS), :] = pick_two(lane, turned, tile)
    for copy in index_copies:
        copy.wait()

    @pl.when(blocks > 1)
    def _():
        near_copy(1).start()

    square = (RANK, RANK)
    product = (
        lax.broadcasted_iota(jnp.int32, square, 0) == lax.broadcasted_iota(jnp.int32, square, 1)
    ).astype(F32)
    products = []
    for level in range(LEVELS):
        at = WIDE + level * RANK * LANES // VECTORS
        parent = jnp.concatenate(
            [own[:, pl.ds(at + i * LANES, LANES)].astype(F32) for i in range(RANK // VECTORS)],
            axis=0,
        )
        own_half = jnp.where(
            ((device >> level) & 1) == 1, pltpu.roll(parent, RANK, 1), parent
        )[:, :RANK]
        product = dot_nt(product.astype(BF16), own_half.astype(BF16))
        products.append(product.astype(BF16))

    for group in range(LEAVES // 8):
        rows = []
        for i in range(8):
            leaf = group * 8 + i
            rows.append(
                jnp.concatenate(
                    [
                        pick_four(
                            lane,
                            *[leaf_table[rows_of(far_from[4 * q + m, leaf]), :] for m in range(4)],
                        )
                        for q in range(FAR // 4)
                    ],
                    axis=1,
                )
            )
        result = dot_nt(
            jnp.concatenate(rows, axis=0).astype(BF16),
            far[group * 8 : group * 8 + 8].reshape(8 * RANK_LEAF, FAR * RANK_LEAF),
        )
        for h in range(2):
            field[LEAF_AT + group * 2 + h] = pick_four(
                lane,
                *[
                    result[(4 * h + j) * 8 : (4 * h + j + 1) * 8, h * LANES : (h + 1) * LANES]
                    for j in range(4)
                ],
            )
    rows = []
    for c in range(GROUPS):
        rows.append(
            jnp.concatenate(
                [
                    pick_two(
                        lane,
                        mid_table[rows_of(mid_from[c, 2 * q]), :],
                        mid_table[rows_of(mid_from[c, 2 * q + 1]), :],
                    )
                    for q in range(MID_FAR // 2)
                ],
                axis=1,
            )
        )
    result = dot_nt(
        jnp.concatenate(rows, axis=0).astype(BF16),
        mid_coupling[...].reshape(GROUPS * RANK, MID_FAR * RANK),
    )
    for h in range(GROUPS // 2):
        span = slice(h * LANES, (h + 1) * LANES)
        field[MID_AT + h] = pick_two(
            lane, result[16 * h : 16 * h + 8, span], result[16 * h + 8 : 16 * h + 16, span]
        )
    @pl.when(blocks > 2)
    def _():
        near_copy(2).start()

    copies[9].wait()

    @pl.when(blocks > 3)
    def _():
        near_copy(3).start()

    level = lax.broadcasted_iota(jnp.int32, (VECTORS, LANES), 0) + 1
    column = BOXES - lax.shift_right_logical(jnp.full_like(level, BOXES), level - 1)
    column = column + lax.shift_right_logical(jnp.full_like(level, 1) * device, level)
    wanted = (lane_index(level.shape) == column).astype(F32)
    nothing = jnp.zeros_like(wanted)
    wanted = jnp.concatenate(
        [
            jnp.concatenate([wanted, nothing], axis=1),
            jnp.concatenate([nothing, wanted], axis=1),
        ],
        axis=0,
    ).astype(BF16)
    missing = jnp.zeros((3 * RANK, 4), BF16)
    for r in range(0, RANK, 2):
        columns = [
            jnp.concatenate([top_coupling[r + i], missing], axis=1) for i in range(2)
        ]
        result = dot_nt(wanted, jnp.concatenate(columns, axis=1))
        rows = slice(r * VECTORS, (r + 2) * VECTORS)
        chosen_low[rows, :] = result[:, :LANES]
        chosen_high[rows, 0:RANK] = result[:, LANES:]
    copies[8].wait()
    coupling[0] = box_coupling[0]
    for k in range(LEVELS):
        rows = pl.ds(k, RANK, stride=VECTORS)
        chosen = jnp.concatenate([chosen_low[rows, :], chosen_high[rows, :][:, :RANK]], axis=1)
        coupling[k + 1] = dot_nn(products[k], chosen.astype(BF16)).astype(BF16)
    coupling_out = pltpu.make_async_copy(coupling, coupling_hbm, out_sem.at[1])
    coupling_out.start()
    zeros_half = jnp.zeros((2 * VECTORS, LANES), BF16)

    def near_step(k, carry):
        near_copy(k).wait()
        sources = [near_from.at[2 * k + i] for i in range(2)]
        targets = [near_to.at[2 * k + i] for i in range(2)]
        for i in range(BLOCK // 16):
            rows, weights = [], []
            for g in range(4):
                first = 16 * i + 4 * g
                at = [rows_of(sources[first // LANES][first % LANES + j]) for j in range(4)]
                top = jnp.concatenate([x_low[at[0], :], x_high[at[1], :]], axis=0)
                bottom = jnp.concatenate([x_low[at[2], :], x_high[at[3], :]], axis=0)
                rows.append(jnp.concatenate([top.astype(BF16), zeros_half], axis=1))
                rows.append(jnp.concatenate([zeros_half, bottom.astype(BF16)], axis=1))
                weights.append(near[k, :, first * CAPACITY : (first + 4) * CAPACITY])
            result = dot_nt(jnp.concatenate(rows, axis=0), jnp.concatenate(weights, axis=0))
            for g in range(4):
                first = 16 * i + 4 * g
                for j in range(4):
                    to = rows_of(targets[first // LANES][first % LANES + j])
                    at = 32 * g + 8 * j
                    accumulators[g][to, :] += result[
                        at : at + 8, (g // 2) * LANES : (g // 2 + 1) * LANES
                    ]
        return carry

    lax.fori_loop(0, blocks, near_step, 0)
    for h in range(LEAVES // 2):
        low = rows_of(2 * h * VECTORS)
        high = rows_of((2 * h + 1) * VECTORS)
        placed = pick_two(lane, acc0[low, :] + acc2[low, :], acc1[high, :] + acc3[high, :])
        moved = pick_two(lane, acc0[high, :] + acc2[high, :], acc1[low, :] + acc3[low, :])
        field[h] = placed + pltpu.roll(moved, CAPACITY, 1)

    field_out = pltpu.make_async_copy(field, field_hbm, out_sem.at[0])
    field_out.start()

    field_out.wait()
    coupling_out.wait()


def down_kernel(
    every,
    top_hbm,
    coupling,
    mid_hbm,
    leaf_hbm,
    field,
    basis_hbm,
    out,
    top_transfer,
    mid_transfer,
    leaf_transfer,
    basis,
    sem,
    top_sem,
    pairs0,
    pairs1,
    pairs2,
    pairs3,
    pairs4,
    pairs5,
):
    pieces = [
        pltpu.make_async_copy(
            top_hbm.at[pl.ds(first, min(8, BOXES - 4 - first))],
            top_transfer.at[pl.ds(first, min(8, BOXES - 4 - first))],
            top_sem.at[first // 8],
        )
        for first in range(0, BOXES - 4, 8)
    ]
    copies = [
        pltpu.make_async_copy(source, target, sem.at[i])
        for i, (source, target) in enumerate(
            ((mid_hbm, mid_transfer), (leaf_hbm, leaf_transfer), (basis_hbm, basis))
        )
    ]
    for copy in pieces + copies:
        copy.start()
    device = lax.axis_index("clusters")
    lane = lane_index((VECTORS, LANES))
    zero = jnp.zeros((VECTORS, LANES), F32)
    empty = jnp.zeros((2 * VECTORS, LANES), BF16)

    pairs = (pairs0, pairs1, pairs2, pairs3, pairs4, pairs5)
    for level in range(LEVELS + 1):
        pairs[level][0] = zero
        pairs[level][(BOXES >> (level + 1)) + 1] = zero
    kept = (lane < RANK) == (lax.broadcasted_iota(jnp.int32, (VECTORS, LANES), 0) < 4)
    for p in range(BOXES // 2):
        tile = every[p].astype(F32)
        pairs0[p + 1] = jnp.where(kept, tile, pltpu.roll(pltpu.roll(tile, RANK, 1), 4, 0))
    for level in range(LEVELS):
        start = BOXES - (BOXES >> level)
        count = BOXES >> (level + 1)
        for g in range(0, count, 8):
            pieces[(start + g) // 8].wait()
            left, right = [], []
            for quad in range(g, min(g + 8, count), 4):
                low = jnp.concatenate([pairs[level][1 + quad], pairs[level][2 + quad]], axis=0)
                high = jnp.concatenate([pairs[level][3 + quad], pairs[level][4 + quad]], axis=0)
                left.append(jnp.concatenate([low.astype(BF16), empty], axis=1))
                left.append(jnp.concatenate([empty, high.astype(BF16)], axis=1))
                at = start + quad
                right.append(jnp.concatenate([top_transfer[at], top_transfer[at + 2]], axis=1))
                right.append(jnp.concatenate([top_transfer[at + 1], top_transfer[at + 3]], axis=1))
            result = dot_nt(jnp.concatenate(left, axis=0), jnp.concatenate(right, axis=0))
            for i in range(len(left)):
                span = slice((i // 2) * LANES, (i // 2 + 1) * LANES)
                pairs[level + 1][1 + g // 2 + i] = pick_two(
                    lane, result[16 * i : 16 * i + 8, span], result[16 * i + 8 : 16 * i + 16, span]
                )
    down = jnp.zeros((VECTORS, RANK), F32)
    for level in range(LEVELS + 1):
        cluster = device >> level
        parent = cluster >> 1
        before = pairs[level][parent]
        after = pltpu.roll(pairs[level][parent + 2], 64, 1)
        middle = jnp.where((cluster & 1) == 1, before, after)
        stacked = jnp.concatenate([pick_two(lane, before, middle), after[:, :64]], axis=1)
        down = down + dot_nt(stacked.astype(BF16), coupling[level])

    copies[0].wait()
    mid_push = dot_nn(down.astype(BF16), mid_transfer[0])
    copies[1].wait()
    rows = []
    for c in range(GROUPS):
        h = c // 2
        tile = field[MID_AT + h] + mid_push[:, h * LANES : (h + 1) * LANES]
        half_tile = pick_two(lane, tile, zero) if c % 2 == 0 else pick_two(lane, zero, tile)
        rows.append(
            jnp.concatenate([half_tile if i == h else zero for i in range(GROUPS // 2)], axis=1)
        )
    leaf_push = dot_nn(
        jnp.concatenate(rows, axis=0).astype(BF16),
        leaf_transfer[...].reshape(GROUPS * RANK, CHILDREN * RANK_LEAF),
    )
    copies[2].wait()
    lane_group = lane // RANK_LEAF
    for first in range(0, LEAVES // 4, 8):
        rows, weights = [], []
        for g in range(first, first + 8):
            push = leaf_push[(g // 2) * 8 : (g // 2) * 8 + 8, (g % 2) * LANES : (g % 2 + 1) * LANES]
            leaf_down = field[LEAF_AT + g] + push
            for j in range(4):
                block = jnp.where(lane_group == g % 4, turn(leaf_down, g % 4 - j), 0.0)
                rows.append(
                    jnp.concatenate([block, zero] if g % 8 < 4 else [zero, block], axis=1)
                )
            weights.append(basis[:, pl.ds(g * 4 * CAPACITY, 4 * CAPACITY)])
        result = dot_nn(
            jnp.concatenate(rows, axis=0).astype(BF16), jnp.concatenate(weights, axis=0)
        )
        for g in range(first, first + 8):
            for h in range(2):
                span = slice(h * LANES, (h + 1) * LANES)
                at = 32 * (g % 8) + 16 * h
                far_tile = pick_two(lane, result[at : at + 8, span], result[at + 8 : at + 16, span])
                out[:, pl.ds((2 * g + h) * LANES, LANES)] = (far_tile + field[2 * g + h]).astype(
                    BF16
                )


def up_call(*operands):
    hbm, shape, scratch = HBM, jax.ShapeDtypeStruct, pltpu.VMEM
    dma = pltpu.SemaphoreType.DMA
    return pl.pallas_call(
        up_kernel,
        out_shape=(
            shape((VECTORS, WIDE), BF16),
            shape((BOXES // 2, VECTORS, LANES), BF16),
            shape((VECTORS, LOCAL), BF16),
        ),
        in_specs=[hbm] * 5,
        out_specs=(hbm, hbm, hbm),
        scratch_shapes=[
            scratch((VECTORS, POINTS), BF16),
            scratch((RANK_LEAF, POINTS), BF16),
            scratch((GROUPS, RANK, CHILDREN * RANK_LEAF), BF16),
            scratch((1, RANK, GROUPS * RANK), BF16),
            scratch((VECTORS, LEAF_LANES + MID_LANES), BF16),
            scratch((MESSAGES, VECTORS, LANES), BF16),
            scratch((LEVELS, RANK, 2 * RANK), BF16),
            scratch((VECTORS, LOCAL), BF16),
            dma((4,)),
            dma((2 + BOXES // 2 // MESSAGES,)),
            dma((LEVELS + 1,)),
        ],
        cost_estimate=pl.CostEstimate(flops=10**9, bytes_accessed=10**6, transcendentals=0),
        compiler_params=pltpu.CompilerParams(vmem_limit_bytes=UP_LIMIT),
        name="upward",
    )(*operands)


def side_call(
    near_source,
    near_target,
    near_count,
    far_source,
    mid_source,
    local,
    packed_pair,
    packed_other,
    far_coupling,
    mid_coupling,
    top_coupling,
    box_coupling,
    near_blocks,
):
    hbm, shape, scratch = HBM, jax.ShapeDtypeStruct, pltpu.VMEM
    dma = pltpu.SemaphoreType.DMA
    table = scratch((3 * LEAVES * VECTORS, LANES), F32)
    accumulator = scratch(((LEAVES + 1) * VECTORS, LANES), F32)
    indices = [
        (VECTORS, LANES),
        (VECTORS, LANES),
        (FAR, LEAVES),
        (GROUPS, MID_FAR),
    ]
    wide = scratch((VECTORS, WIDE), BF16)
    return pl.pallas_call(
        side_kernel,
        out_shape=(
            shape((FIELDS, VECTORS, LANES), F32),
            shape((LEVELS + 1, RANK, 3 * RANK), BF16),
        ),
        in_specs=[hbm] * 8 + [pl.BlockSpec(memory_space=pltpu.VMEM)] * 2 + [hbm] * 3,
        out_specs=(hbm, hbm),
        scratch_shapes=[scratch(i, jnp.int32) for i in indices]
        + [
            scratch((VECTORS, LOCAL), BF16),
            wide,
            wide,
            scratch((RANK, 3 * RANK, BOXES - 4), BF16),
            scratch((1, RANK, 3 * RANK), BF16),
            scratch((PARTS, CAPACITY, PART), BF16),
            scratch((FIELDS, VECTORS, LANES), F32),
            scratch((LEVELS + 1, RANK, 3 * RANK), BF16),
            table,
            table,
            table,
            scratch((3 * GROUPS * VECTORS, LANES), F32),
            accumulator,
            accumulator,
            accumulator,
            accumulator,
            scratch((RANK * VECTORS, LANES), F32),
            scratch((RANK * VECTORS, LANES), F32),
        ]
        + [scratch(i, jnp.int32) for i in indices]
        + [pltpu.SMEM((1, 1), jnp.int32)]
        + [pltpu.SMEM(i, jnp.int32) for i in indices]
        + [dma((PARTS,)), dma((10,)), dma((4,)), dma((2,))],
        cost_estimate=pl.CostEstimate(flops=2 * 10**9, bytes_accessed=10**7, transcendentals=0),
        compiler_params=pltpu.CompilerParams(vmem_limit_bytes=SIDE_LIMIT),
        name="side",
    )(
        near_source.reshape(VECTORS, LANES),
        near_target.reshape(VECTORS, LANES),
        near_count.reshape(1, 1),
        far_source.T,
        mid_source,
        local,
        packed_pair,
        packed_other,
        far_coupling,
        mid_coupling,
        jnp.transpose(top_coupling, (1, 2, 0)),
            box_coupling,
        near_blocks,
    )


def down_call(*operands):
    hbm, shape, scratch = HBM, jax.ShapeDtypeStruct, pltpu.VMEM
    dma = pltpu.SemaphoreType.DMA
    vmem = pl.BlockSpec(memory_space=pltpu.VMEM)
    return pl.pallas_call(
        down_kernel,
        out_shape=shape((VECTORS, POINTS), BF16),
        in_specs=[vmem, hbm, vmem, hbm, hbm, vmem, hbm],
        out_specs=pl.BlockSpec(memory_space=pltpu.VMEM),
        scratch_shapes=[
            scratch((BOXES - 4, RANK, 2 * RANK), BF16),
            scratch((1, RANK, GROUPS * RANK), BF16),
            scratch((GROUPS, RANK, CHILDREN * RANK_LEAF), BF16),
            scratch((RANK_LEAF, POINTS), BF16),
            dma((3,)),
            dma((BOXES // 8,)),
        ]
        + [
            scratch(((BOXES >> (level + 1)) + 2, VECTORS, LANES), F32)
            for level in range(LEVELS + 1)
        ],
        cost_estimate=pl.CostEstimate(flops=10**9, bytes_accessed=10**6, transcendentals=0),
        compiler_params=pltpu.CompilerParams(vmem_limit_bytes=DOWN_LIMIT),
        name="down",
    )(*operands)


def body(
    charges,
    leaf_basis,
    leaf_transfer,
    mid_transfer,
    far_source,
    far_coupling,
    mid_source,
    mid_coupling,
    box_coupling,
    top_transfer,
    top_coupling,
    near_target,
    near_source,
    near_count,
    near_blocks,
):
    pair = [(i, i ^ 1) for i in range(BOXES)]
    other = [(i, min(max(((i + 1) ^ 1) - 1, 0), BOXES - 1)) for i in range(BOXES)]
    packed, message, local = up_call(
        charges, leaf_basis, leaf_transfer, mid_transfer, top_transfer
    )
    packed_other = lax.ppermute(packed, "clusters", other)
    packed_pair = lax.ppermute(packed, "clusters", pair)
    every = lax.all_to_all(message.reshape(BOXES, VECTORS // 2, LANES), "clusters", 0, 0)
    field, coupling = side_call(
        near_source,
        near_target,
        near_count,
        far_source,
        mid_source,
        local,
        packed_pair,
        packed_other,
        far_coupling,
        mid_coupling,
        top_coupling,
        box_coupling,
        near_blocks,
    )
    return down_call(
        every.reshape(BOXES // 2, VECTORS, LANES),
        top_transfer,
        coupling,
        mid_transfer,
        leaf_transfer,
        field,
        leaf_basis,
    )


def solution(mesh):
    in_specs = (
        P(None, "clusters"),
        P(None, "clusters"),
        P("clusters", None, None),
        P("clusters", None, None),
        P("clusters", None),
        P("clusters", None, None),
        P("clusters", None),
        P("clusters", None, None),
        P("clusters", None, None),
        P(),
        P(),
        P("clusters"),
        P("clusters"),
        P("clusters"),
        P(None, "clusters"),
    )
    out_specs = P(None, "clusters")
    return jax.shard_map(body, mesh=mesh, in_specs=in_specs, out_specs=out_specs, check_vma=False)
```

```python
import jax
import jax.numpy as jnp
from jax import lax
from jax.experimental import pallas as pl
from jax.experimental.pallas import tpu as pltpu
from jax.sharding import PartitionSpec as P

F32 = jnp.float32
BF16 = jnp.bfloat16

VECTORS = 8
LEAVES = 64
CAPACITY = 64
RANK_LEAF = 32
RANK = 64
GROUPS = 8
CHILDREN = 8
FAR = 16
MID_FAR = 8
SLOTS = 1024
BOXES = 128
LEVELS = 5
POINTS = LEAVES * CAPACITY
LEAF_LANES = LEAVES * RANK_LEAF
MID_LANES = GROUPS * RANK
PARTS = 4
PART = SLOTS * CAPACITY // PARTS
BLOCK = SLOTS // PARTS
WIDE = POINTS + LEAF_LANES + MID_LANES
LANES = 128
VMEM_LIMIT = 60 * 1024 * 1024
LOCAL = WIDE + LEVELS * RANK * LANES // VECTORS
UP_LIMIT = 60 * 1024 * 1024
SIDE_LIMIT = 51500 * 1024
DOWN_LIMIT = 54400 * 1024
MESSAGES = 16
LEAF_AT = LEAVES // 2
MID_AT = LEAF_AT + LEAVES // 4
FIELDS = MID_AT + GROUPS // 2


HBM = pl.BlockSpec(memory_space=pltpu.HBM)


def dot_nt(left, right):
    return lax.dot_general(left, right, (((1,), (1,)), ((), ())), preferred_element_type=F32)


def dot_nn(left, right):
    return lax.dot_general(left, right, (((1,), (0,)), ((), ())), preferred_element_type=F32)


def lane_index(shape):
    return lax.broadcasted_iota(jnp.int32, shape, len(shape) - 1)


def pick_two(lane, first, second):
    return jnp.where(lane < 64, first, second)


def pick_four(lane, a, b, c, d):
    return jnp.where(lane < 64, jnp.where(lane < 32, a, b), jnp.where(lane < 96, c, d))


def turn(tile, groups):
    return tile if groups % 4 == 0 else pltpu.roll(tile, RANK_LEAF * (groups % 4), 1)


def rows_of(first):
    return pl.ds(pl.multiple_of(first, VECTORS), VECTORS)


def up_kernel(
    charges_hbm,
    basis_hbm,
    leaf_hbm,
    mid_hbm,
    top_hbm,
    packed_hbm,
    message_hbm,
    local_hbm,
    charges,
    basis,
    leaf_transfer,
    mid_transfer,
    coefficients,
    message,
    parents,
    local,
    sem,
    out_sem,
    parent_sem,
):
    device = lax.axis_index("clusters")
    copies = [
        pltpu.make_async_copy(a, b, sem.at[i])
        for i, (a, b) in enumerate(
            (
                (charges_hbm, charges),
                (basis_hbm, basis),
                (leaf_hbm, leaf_transfer),
                (mid_hbm, mid_transfer),
            )
        )
    ]
    for copy in copies:
        copy.start()
    parent_copies = []
    for level in range(LEVELS):
        start = BOXES - (BOXES >> level)
        parent_copies.append(
            pltpu.make_async_copy(
                top_hbm.at[start + (device >> (level + 1))],
                parents.at[level],
                parent_sem.at[level],
            )
        )
        parent_copies[level].start()
    lane = lane_index((VECTORS, LANES))
    wide_lane = lane_index((VECTORS, 4 * CAPACITY)) // CAPACITY
    copies[0].wait()
    charges_out = pltpu.make_async_copy(
        charges, packed_hbm.at[:, pl.ds(0, POINTS)], out_sem.at[0]
    )
    charges_out.start()
    copies[1].wait()
    for copy in parent_copies:
        copy.wait()
    local[:, pl.ds(0, POINTS)] = charges[...]
    for level in range(LEVELS):
        for i in range(RANK // VECTORS):
            at = WIDE + (level * (RANK // VECTORS) + i) * LANES
            local[:, pl.ds(at, LANES)] = parents[level, i * VECTORS : (i + 1) * VECTORS, :]
    tiles = []
    for first in range(0, LEAVES // 4, 8):
        rows, weights = [], []
        for g in range(first, first + 8):
            span = pl.ds(g * 4 * CAPACITY, 4 * CAPACITY)
            x = charges[:, span].astype(F32)
            rows += [jnp.where(wide_lane == j, x, 0.0) for j in range(4)]
            weights.append(basis[:, span])
        result = dot_nt(
            jnp.concatenate(rows, axis=0).astype(BF16), jnp.concatenate(weights, axis=0)
        )
        for g in range(8):
            tile = result[32 * g : 32 * (g + 1), (g // 4) * LANES : (g // 4 + 1) * LANES]
            tiles.append(
                pick_four(lane, *[turn(tile[8 * j : 8 * (j + 1)], j - g % 4) for j in range(4)])
            )
    for g in range(LEAVES // 4):
        coefficients[:, pl.ds(g * LANES, LANES)] = tiles[g].astype(BF16)
    stacked = jnp.concatenate(
        [jnp.concatenate([tiles[2 * c], tiles[2 * c + 1]], axis=1) for c in range(GROUPS)], axis=0
    ).astype(BF16)
    copies[2].wait()
    result = dot_nt(stacked, leaf_transfer[...].reshape(GROUPS * RANK, CHILDREN * RANK_LEAF))
    mid = []
    for h in range(GROUPS // 2):
        span = slice(h * LANES, (h + 1) * LANES)
        low = result[16 * h : 16 * h + 8, span]
        high = result[16 * h + 8 : 16 * h + 16, span]
        mid.append(pick_two(lane, low, high).astype(BF16))
        coefficients[:, pl.ds(LEAF_LANES + h * LANES, LANES)] = mid[h]
    coefficients_out = pltpu.make_async_copy(
        coefficients, packed_hbm.at[:, pl.ds(POINTS, LEAF_LANES + MID_LANES)], out_sem.at[1]
    )
    coefficients_out.start()
    local[:, pl.ds(POINTS, LEAF_LANES + MID_LANES)] = coefficients[...]
    local_out = pltpu.make_async_copy(local, local_hbm, parent_sem.at[LEVELS])
    local_out.start()
    copies[3].wait()
    box = dot_nt(jnp.concatenate(mid, axis=1), mid_transfer[0])
    box = jnp.concatenate([box[:4], box[4:]], axis=1)
    box = jnp.concatenate([box, box], axis=0).astype(BF16)
    message[...] = jnp.broadcast_to(box[None], message.shape)
    messages_out = [
        pltpu.make_async_copy(
            message, message_hbm.at[pl.ds(i * MESSAGES, MESSAGES)], out_sem.at[2 + i]
        )
        for i in range(BOXES // 2 // MESSAGES)
    ]
    for copy in messages_out:
        copy.start()
    charges_out.wait()
    coefficients_out.wait()
    local_out.wait()
    for copy in messages_out:
        copy.wait()


def side_kernel(
    near_source_hbm,
    near_target_hbm,
    near_count_hbm,
    far_source_hbm,
    mid_source_hbm,
    own_hbm,
    pair_hbm,
    other_hbm,
    far,
    mid_coupling,
    top_coupling_hbm,
    box_coupling_hbm,
    near_hbm,
    field_hbm,
    coupling_hbm,
    near_source,
    near_target,
    far_source,
    mid_source,
    own,
    pair,
    other,
    top_coupling,
    box_coupling,
    near,
    field,
    coupling,
    x_low,
    x_high,
    leaf_table,
    mid_table,
    acc0,
    acc1,
    acc2,
    acc3,
    chosen_low,
    chosen_high,
    source_rows,
    target_rows,
    far_rows,
    mid_rows,
    near_count,
    near_from,
    near_to,
    far_from,
    mid_from,
    near_sem,
    sem,
    index_sem,
    out_sem,
):
    device = lax.axis_index("clusters")

    def near_copy(k):
        return pltpu.make_async_copy(
            near_hbm.at[:, pl.ds(pl.multiple_of(k * PART, PART), PART)], near.at[k], near_sem.at[k]
        )

    copies = [
        pltpu.make_async_copy(a, b, sem.at[i])
        for i, (a, b) in enumerate(
            (
                (near_count_hbm, near_count),
                (near_source_hbm, near_source),
                (near_target_hbm, near_target),
                (far_source_hbm, far_source),
                (mid_source_hbm, mid_source),
                (own_hbm, own),
                (pair_hbm, pair),
                (other_hbm, other),
                (box_coupling_hbm, box_coupling),
                (top_coupling_hbm, top_coupling),
            )
        )
    ]
    for copy in copies[:8]:
        copy.start()
    copies[9].start()
    near_copy(0).start()
    copies[8].start()

    for copy in copies[:5]:
        copy.wait()
    live = near_count[0, 0]
    leaf_base = (device - 1) * LEAVES
    shape = (VECTORS, LANES)
    slot = lax.broadcasted_iota(jnp.int32, shape, 0) * LANES + lane_index(shape)
    used = slot < live
    source_rows[...] = jnp.where(used, near_source[...] - leaf_base, LEAVES) * VECTORS
    target_rows[...] = jnp.where(used, near_target[...], LEAVES) * VECTORS
    far_rows[...] = (far_source[...] - leaf_base) * VECTORS
    mid_rows[...] = (mid_source[...] - (device - 1) * GROUPS) * VECTORS
    index_copies = [
        pltpu.make_async_copy(a, b, index_sem.at[i])
        for i, (a, b) in enumerate(
            (
                (source_rows, near_from),
                (target_rows, near_to),
                (far_rows, far_from),
                (mid_rows, mid_from),
            )
        )
    ]
    for copy in index_copies:
        copy.start()
    blocks = jnp.clip((live + BLOCK - 1) // BLOCK, 1, PARTS)

    lane = lane_index((VECTORS, LANES))
    zero = jnp.zeros((VECTORS, LANES), F32)
    odd = device % 2
    accumulators = (acc0, acc1, acc2, acc3)
    for acc in accumulators:
        acc[...] = jnp.zeros(acc.shape, F32)
    for copy in copies[5:8]:
        copy.wait()
    for source, region in ((own, 1), (pair, (1 - odd) * 2), (other, odd * 2)):
        base = region * LEAVES * VECTORS
        for h in range(LEAVES // 2):
            tile = source[:, pl.ds(h * LANES, LANES)].astype(F32)
            turned = pltpu.roll(tile, 64, 1)
            at = base + 2 * h * VECTORS
            x_low[rows_of(at), :] = pick_two(lane, tile, zero)
            x_high[rows_of(at), :] = pick_two(lane, zero, turned)
            x_low[rows_of(at + VECTORS), :] = pick_two(lane, turned, zero)
            x_high[rows_of(at + VECTORS), :] = pick_two(lane, zero, tile)
        for h in range(LEAVES // 4):
            tile = source[:, pl.ds(POINTS + h * LANES, LANES)].astype(F32)
            turns = [tile] + [pltpu.roll(tile, 32 * i, 1) for i in range(1, 4)]
            for j in range(4):
                leaf_table[rows_of(base + (4 * h + j) * VECTORS), :] = pick_four(
                    lane, *[turns[(group - j) % 4] for group in range(4)]
                )
        base = region * GROUPS * VECTORS
        for h in range(GROUPS // 2):
            tile = source[:, pl.ds(POINTS + LEAF_LANES + h * LANES, LANES)].astype(F32)
            turned = pltpu.roll(tile, 64, 1)
            at = base + 2 * h * VECTORS
            mid_table[rows_of(at), :] = pick_two(lane, tile, turned)
            mid_table[rows_of(at + VECTORS), :] = pick_two(lane, turned, tile)
    for copy in index_copies:
        copy.wait()

    @pl.when(blocks > 1)
    def _():
        near_copy(1).start()

    square = (RANK, RANK)
    product = (
        lax.broadcasted_iota(jnp.int32, square, 0) == lax.broadcasted_iota(jnp.int32, square, 1)
    ).astype(F32)
    products = []
    for level in range(LEVELS):
        at = WIDE + level * RANK * LANES // VECTORS
        parent = jnp.concatenate(
            [own[:, pl.ds(at + i * LANES, LANES)].astype(F32) for i in range(RANK // VECTORS)],
            axis=0,
        )
        own_half = jnp.where(
            ((device >> level) & 1) == 1, pltpu.roll(parent, RANK, 1), parent
        )[:, :RANK]
        product = dot_nt(product.astype(BF16), own_half.astype(BF16))
        products.append(product.astype(BF16))

    for group in range(LEAVES // 8):
        rows = []
        for i in range(8):
            leaf = group * 8 + i
            rows.append(
                jnp.concatenate(
                    [
                        pick_four(
                            lane,
                            *[leaf_table[rows_of(far_from[4 * q + m, leaf]), :] for m in range(4)],
                        )
                        for q in range(FAR // 4)
                    ],
                    axis=1,
                )
            )
        result = dot_nt(
            jnp.concatenate(rows, axis=0).astype(BF16),
            far[group * 8 : group * 8 + 8].reshape(8 * RANK_LEAF, FAR * RANK_LEAF),
        )
        for h in range(2):
            field[LEAF_AT + group * 2 + h] = pick_four(
                lane,
                *[
                    result[(4 * h + j) * 8 : (4 * h + j + 1) * 8, h * LANES : (h + 1) * LANES]
                    for j in range(4)
                ],
            )
    rows = []
    for c in range(GROUPS):
        rows.append(
            jnp.concatenate(
                [
                    pick_two(
                        lane,
                        mid_table[rows_of(mid_from[c, 2 * q]), :],
                        mid_table[rows_of(mid_from[c, 2 * q + 1]), :],
                    )
                    for q in range(MID_FAR // 2)
                ],
                axis=1,
            )
        )
    result = dot_nt(
        jnp.concatenate(rows, axis=0).astype(BF16),
        mid_coupling[...].reshape(GROUPS * RANK, MID_FAR * RANK),
    )
    for h in range(GROUPS // 2):
        span = slice(h * LANES, (h + 1) * LANES)
        field[MID_AT + h] = pick_two(
            lane, result[16 * h : 16 * h + 8, span], result[16 * h + 8 : 16 * h + 16, span]
        )
    @pl.when(blocks > 2)
    def _():
        near_copy(2).start()

    copies[9].wait()

    @pl.when(blocks > 3)
    def _():
        near_copy(3).start()

    level = lax.broadcasted_iota(jnp.int32, (VECTORS, LANES), 0) + 1
    column = BOXES - lax.shift_right_logical(jnp.full_like(level, BOXES), level - 1)
    column = column + lax.shift_right_logical(jnp.full_like(level, 1) * device, level)
    wanted = (lane_index(level.shape) == column).astype(F32)
    nothing = jnp.zeros_like(wanted)
    wanted = jnp.concatenate(
        [
            jnp.concatenate([wanted, nothing], axis=1),
            jnp.concatenate([nothing, wanted], axis=1),
        ],
        axis=0,
    ).astype(BF16)
    missing = jnp.zeros((3 * RANK, 4), BF16)
    for r in range(0, RANK, 2):
        columns = [
            jnp.concatenate([top_coupling[r + i], missing], axis=1) for i in range(2)
        ]
        result = dot_nt(wanted, jnp.concatenate(columns, axis=1))
        rows = slice(r * VECTORS, (r + 2) * VECTORS)
        chosen_low[rows, :] = result[:, :LANES]
        chosen_high[rows, 0:RANK] = result[:, LANES:]
    copies[8].wait()
    coupling[0] = box_coupling[0]
    for k in range(LEVELS):
        rows = pl.ds(k, RANK, stride=VECTORS)
        chosen = jnp.concatenate([chosen_low[rows, :], chosen_high[rows, :][:, :RANK]], axis=1)
        coupling[k + 1] = dot_nn(products[k], chosen.astype(BF16)).astype(BF16)
    coupling_out = pltpu.make_async_copy(coupling, coupling_hbm, out_sem.at[1])
    coupling_out.start()
    zeros_half = jnp.zeros((2 * VECTORS, LANES), BF16)

    def near_step(k, carry):
        near_copy(k).wait()
        sources = [near_from.at[2 * k + i] for i in range(2)]
        targets = [near_to.at[2 * k + i] for i in range(2)]
        for i in range(BLOCK // 16):
            rows, weights = [], []
            for g in range(4):
                first = 16 * i + 4 * g
                at = [rows_of(sources[first // LANES][first % LANES + j]) for j in range(4)]
                top = jnp.concatenate([x_low[at[0], :], x_high[at[1], :]], axis=0)
                bottom = jnp.concatenate([x_low[at[2], :], x_high[at[3], :]], axis=0)
                rows.append(jnp.concatenate([top.astype(BF16), zeros_half], axis=1))
                rows.append(jnp.concatenate([zeros_half, bottom.astype(BF16)], axis=1))
                weights.append(near[k, :, first * CAPACITY : (first + 4) * CAPACITY])
            result = dot_nt(jnp.concatenate(rows, axis=0), jnp.concatenate(weights, axis=0))
            for g in range(4):
                first = 16 * i + 4 * g
                for j in range(4):
                    to = rows_of(targets[first // LANES][first % LANES + j])
                    at = 32 * g + 8 * j
                    accumulators[g][to, :] += result[
                        at : at + 8, (g // 2) * LANES : (g // 2 + 1) * LANES
                    ]
        return carry

    lax.fori_loop(0, blocks, near_step, 0)
    for h in range(LEAVES // 2):
        low = rows_of(2 * h * VECTORS)
        high = rows_of((2 * h + 1) * VECTORS)
        placed = pick_two(lane, acc0[low, :] + acc2[low, :], acc1[high, :] + acc3[high, :])
        moved = pick_two(lane, acc0[high, :] + acc2[high, :], acc1[low, :] + acc3[low, :])
        field[h] = placed + pltpu.roll(moved, CAPACITY, 1)

    field_out = pltpu.make_async_copy(field, field_hbm, out_sem.at[0])
    field_out.start()

    field_out.wait()
    coupling_out.wait()


def down_kernel(
    every,
    top_hbm,
    coupling,
    mid_hbm,
    leaf_hbm,
    field,
    basis_hbm,
    out,
    top_transfer,
    mid_transfer,
    leaf_transfer,
    basis,
    sem,
    pairs0,
    pairs1,
    pairs2,
    pairs3,
    pairs4,
    pairs5,
):
    half = pl.ds(0, BOXES // 2)
    rest = pl.ds(BOXES // 2, BOXES // 2 - 4)
    copies = [
        pltpu.make_async_copy(source, target, sem.at[i])
        for i, (source, target) in enumerate(
            (
                (mid_hbm, mid_transfer),
                (leaf_hbm, leaf_transfer),
                (basis_hbm, basis),
                (top_hbm.at[half], top_transfer.at[half]),
                (top_hbm.at[rest], top_transfer.at[rest]),
            )
        )
    ]
    for copy in copies[3:] + copies[:3]:
        copy.start()
    device = lax.axis_index("clusters")
    lane = lane_index((VECTORS, LANES))
    zero = jnp.zeros((VECTORS, LANES), F32)
    empty = jnp.zeros((2 * VECTORS, LANES), BF16)

    pairs = (pairs0, pairs1, pairs2, pairs3, pairs4, pairs5)
    for level in range(LEVELS + 1):
        pairs[level][0] = zero
        pairs[level][(BOXES >> (level + 1)) + 1] = zero
    kept = (lane < RANK) == (lax.broadcasted_iota(jnp.int32, (VECTORS, LANES), 0) < 4)
    for p in range(BOXES // 2):
        tile = every[p].astype(F32)
        pairs0[p + 1] = jnp.where(kept, tile, pltpu.roll(pltpu.roll(tile, RANK, 1), 4, 0))
    for level in range(LEVELS):
        if level < 2:
            copies[3 + level].wait()
        start = BOXES - (BOXES >> level)
        count = BOXES >> (level + 1)
        for g in range(0, count, 8):
            left, right = [], []
            for quad in range(g, min(g + 8, count), 4):
                low = jnp.concatenate([pairs[level][1 + quad], pairs[level][2 + quad]], axis=0)
                high = jnp.concatenate([pairs[level][3 + quad], pairs[level][4 + quad]], axis=0)
                left.append(jnp.concatenate([low.astype(BF16), empty], axis=1))
                left.append(jnp.concatenate([empty, high.astype(BF16)], axis=1))
                at = start + quad
                right.append(jnp.concatenate([top_transfer[at], top_transfer[at + 2]], axis=1))
                right.append(jnp.concatenate([top_transfer[at + 1], top_transfer[at + 3]], axis=1))
            result = dot_nt(jnp.concatenate(left, axis=0), jnp.concatenate(right, axis=0))
            for i in range(len(left)):
                span = slice((i // 2) * LANES, (i // 2 + 1) * LANES)
                pairs[level + 1][1 + g // 2 + i] = pick_two(
                    lane, result[16 * i : 16 * i + 8, span], result[16 * i + 8 : 16 * i + 16, span]
                )
    down = jnp.zeros((VECTORS, RANK), F32)
    for level in range(LEVELS + 1):
        cluster = device >> level
        parent = cluster >> 1
        before = pairs[level][parent]
        after = pltpu.roll(pairs[level][parent + 2], 64, 1)
        middle = jnp.where((cluster & 1) == 1, before, after)
        stacked = jnp.concatenate([pick_two(lane, before, middle), after[:, :64]], axis=1)
        down = down + dot_nt(stacked.astype(BF16), coupling[level])

    copies[0].wait()
    mid_push = dot_nn(down.astype(BF16), mid_transfer[0])
    copies[1].wait()
    rows = []
    for c in range(GROUPS):
        h = c // 2
        tile = field[MID_AT + h] + mid_push[:, h * LANES : (h + 1) * LANES]
        half_tile = pick_two(lane, tile, zero) if c % 2 == 0 else pick_two(lane, zero, tile)
        rows.append(
            jnp.concatenate([half_tile if i == h else zero for i in range(GROUPS // 2)], axis=1)
        )
    leaf_push = dot_nn(
        jnp.concatenate(rows, axis=0).astype(BF16),
        leaf_transfer[...].reshape(GROUPS * RANK, CHILDREN * RANK_LEAF),
    )
    copies[2].wait()
    lane_group = lane // RANK_LEAF
    for first in range(0, LEAVES // 4, 8):
        rows, weights = [], []
        for g in range(first, first + 8):
            push = leaf_push[(g // 2) * 8 : (g // 2) * 8 + 8, (g % 2) * LANES : (g % 2 + 1) * LANES]
            leaf_down = field[LEAF_AT + g] + push
            for j in range(4):
                block = jnp.where(lane_group == g % 4, turn(leaf_down, g % 4 - j), 0.0)
                rows.append(
                    jnp.concatenate([block, zero] if g % 8 < 4 else [zero, block], axis=1)
                )
            weights.append(basis[:, pl.ds(g * 4 * CAPACITY, 4 * CAPACITY)])
        result = dot_nn(
            jnp.concatenate(rows, axis=0).astype(BF16), jnp.concatenate(weights, axis=0)
        )
        for g in range(first, first + 8):
            for h in range(2):
                span = slice(h * LANES, (h + 1) * LANES)
                at = 32 * (g % 8) + 16 * h
                far_tile = pick_two(lane, result[at : at + 8, span], result[at + 8 : at + 16, span])
                out[:, pl.ds((2 * g + h) * LANES, LANES)] = (far_tile + field[2 * g + h]).astype(
                    BF16
                )


def up_call(*operands):
    hbm, shape, scratch = HBM, jax.ShapeDtypeStruct, pltpu.VMEM
    dma = pltpu.SemaphoreType.DMA
    return pl.pallas_call(
        up_kernel,
        out_shape=(
            shape((VECTORS, WIDE), BF16),
            shape((BOXES // 2, VECTORS, LANES), BF16),
            shape((VECTORS, LOCAL), BF16),
        ),
        in_specs=[hbm] * 5,
        out_specs=(hbm, hbm, hbm),
        scratch_shapes=[
            scratch((VECTORS, POINTS), BF16),
            scratch((RANK_LEAF, POINTS), BF16),
            scratch((GROUPS, RANK, CHILDREN * RANK_LEAF), BF16),
            scratch((1, RANK, GROUPS * RANK), BF16),
            scratch((VECTORS, LEAF_LANES + MID_LANES), BF16),
            scratch((MESSAGES, VECTORS, LANES), BF16),
            scratch((LEVELS, RANK, 2 * RANK), BF16),
            scratch((VECTORS, LOCAL), BF16),
            dma((4,)),
            dma((2 + BOXES // 2 // MESSAGES,)),
            dma((LEVELS + 1,)),
        ],
        cost_estimate=pl.CostEstimate(flops=10**9, bytes_accessed=10**6, transcendentals=0),
        compiler_params=pltpu.CompilerParams(vmem_limit_bytes=UP_LIMIT),
        name="upward",
    )(*operands)


def side_call(
    near_source,
    near_target,
    near_count,
    far_source,
    mid_source,
    local,
    packed_pair,
    packed_other,
    far_coupling,
    mid_coupling,
    top_coupling,
    box_coupling,
    near_blocks,
):
    hbm, shape, scratch = HBM, jax.ShapeDtypeStruct, pltpu.VMEM
    dma = pltpu.SemaphoreType.DMA
    table = scratch((3 * LEAVES * VECTORS, LANES), F32)
    accumulator = scratch(((LEAVES + 1) * VECTORS, LANES), F32)
    indices = [
        (VECTORS, LANES),
        (VECTORS, LANES),
        (FAR, LEAVES),
        (GROUPS, MID_FAR),
    ]
    wide = scratch((VECTORS, WIDE), BF16)
    return pl.pallas_call(
        side_kernel,
        out_shape=(
            shape((FIELDS, VECTORS, LANES), F32),
            shape((LEVELS + 1, RANK, 3 * RANK), BF16),
        ),
        in_specs=[hbm] * 8 + [pl.BlockSpec(memory_space=pltpu.VMEM)] * 2 + [hbm] * 3,
        out_specs=(hbm, hbm),
        scratch_shapes=[scratch(i, jnp.int32) for i in indices]
        + [
            scratch((VECTORS, LOCAL), BF16),
            wide,
            wide,
            scratch((RANK, 3 * RANK, BOXES - 4), BF16),
            scratch((1, RANK, 3 * RANK), BF16),
            scratch((PARTS, CAPACITY, PART), BF16),
            scratch((FIELDS, VECTORS, LANES), F32),
            scratch((LEVELS + 1, RANK, 3 * RANK), BF16),
            table,
            table,
            table,
            scratch((3 * GROUPS * VECTORS, LANES), F32),
            accumulator,
            accumulator,
            accumulator,
            accumulator,
            scratch((RANK * VECTORS, LANES), F32),
            scratch((RANK * VECTORS, LANES), F32),
        ]
        + [scratch(i, jnp.int32) for i in indices]
        + [pltpu.SMEM((1, 1), jnp.int32)]
        + [pltpu.SMEM(i, jnp.int32) for i in indices]
        + [dma((PARTS,)), dma((10,)), dma((4,)), dma((2,))],
        cost_estimate=pl.CostEstimate(flops=2 * 10**9, bytes_accessed=10**7, transcendentals=0),
        compiler_params=pltpu.CompilerParams(vmem_limit_bytes=SIDE_LIMIT),
        name="side",
    )(
        near_source.reshape(VECTORS, LANES),
        near_target.reshape(VECTORS, LANES),
        near_count.reshape(1, 1),
        far_source.T,
        mid_source,
        local,
        packed_pair,
        packed_other,
        far_coupling,
        mid_coupling,
        jnp.transpose(top_coupling, (1, 2, 0)),
            box_coupling,
        near_blocks,
    )


def down_call(*operands):
    hbm, shape, scratch = HBM, jax.ShapeDtypeStruct, pltpu.VMEM
    dma = pltpu.SemaphoreType.DMA
    vmem = pl.BlockSpec(memory_space=pltpu.VMEM)
    return pl.pallas_call(
        down_kernel,
        out_shape=shape((VECTORS, POINTS), BF16),
        in_specs=[vmem, hbm, vmem, hbm, hbm, vmem, hbm],
        out_specs=pl.BlockSpec(memory_space=pltpu.VMEM),
        scratch_shapes=[
            scratch((BOXES - 4, RANK, 2 * RANK), BF16),
            scratch((1, RANK, GROUPS * RANK), BF16),
            scratch((GROUPS, RANK, CHILDREN * RANK_LEAF), BF16),
            scratch((RANK_LEAF, POINTS), BF16),
            dma((5,)),
        ]
        + [
            scratch(((BOXES >> (level + 1)) + 2, VECTORS, LANES), F32)
            for level in range(LEVELS + 1)
        ],
        cost_estimate=pl.CostEstimate(flops=10**9, bytes_accessed=10**6, transcendentals=0),
        compiler_params=pltpu.CompilerParams(vmem_limit_bytes=DOWN_LIMIT),
        name="down",
    )(*operands)


def body(
    charges,
    leaf_basis,
    leaf_transfer,
    mid_transfer,
    far_source,
    far_coupling,
    mid_source,
    mid_coupling,
    box_coupling,
    top_transfer,
    top_coupling,
    near_target,
    near_source,
    near_count,
    near_blocks,
):
    pair = [(i, i ^ 1) for i in range(BOXES)]
    other = [(i, min(max(((i + 1) ^ 1) - 1, 0), BOXES - 1)) for i in range(BOXES)]
    packed, message, local = up_call(
        charges, leaf_basis, leaf_transfer, mid_transfer, top_transfer
    )
    packed_other = lax.ppermute(packed, "clusters", other)
    packed_pair = lax.ppermute(packed, "clusters", pair)
    every = lax.all_to_all(message.reshape(BOXES, VECTORS // 2, LANES), "clusters", 0, 0)
    field, coupling = side_call(
        near_source,
        near_target,
        near_count,
        far_source,
        mid_source,
        local,
        packed_pair,
        packed_other,
        far_coupling,
        mid_coupling,
        top_coupling,
        box_coupling,
        near_blocks,
    )
    return down_call(
        every.reshape(BOXES // 2, VECTORS, LANES),
        top_transfer,
        coupling,
        mid_transfer,
        leaf_transfer,
        field,
        leaf_basis,
    )


def solution(mesh):
    in_specs = (
        P(None, "clusters"),
        P(None, "clusters"),
        P("clusters", None, None),
        P("clusters", None, None),
        P("clusters", None),
        P("clusters", None, None),
        P("clusters", None),
        P("clusters", None, None),
        P("clusters", None, None),
        P(),
        P(),
        P("clusters"),
        P("clusters"),
        P("clusters"),
        P(None, "clusters"),
    )
    out_specs = P(None, "clusters")
    return jax.shard_map(body, mesh=mesh, in_specs=in_specs, out_specs=out_specs, check_vma=False)
```

```python
import jax
import jax.numpy as jnp
from jax import lax
from jax.experimental import pallas as pl
from jax.experimental.pallas import tpu as pltpu
from jax.sharding import PartitionSpec as P

F32 = jnp.float32
BF16 = jnp.bfloat16

VECTORS = 8
LEAVES = 64
CAPACITY = 64
RANK_LEAF = 32
RANK = 64
GROUPS = 8
CHILDREN = 8
FAR = 16
MID_FAR = 8
SLOTS = 1024
BOXES = 128
LEVELS = 5
POINTS = LEAVES * CAPACITY
LEAF_LANES = LEAVES * RANK_LEAF
MID_LANES = GROUPS * RANK
PARTS = 4
PART = SLOTS * CAPACITY // PARTS
BLOCK = SLOTS // PARTS
WIDE = POINTS + LEAF_LANES + MID_LANES
LANES = 128
VMEM_LIMIT = 60 * 1024 * 1024
LOCAL = WIDE + LEVELS * RANK * LANES // VECTORS
UP_LIMIT = 60 * 1024 * 1024
SIDE_LIMIT = 51500 * 1024
DOWN_LIMIT = 54400 * 1024
MESSAGES = 16
LEAF_AT = LEAVES // 2
MID_AT = LEAF_AT + LEAVES // 4
FIELDS = MID_AT + GROUPS // 2


HBM = pl.BlockSpec(memory_space=pltpu.HBM)


def dot_nt(left, right):
    return lax.dot_general(left, right, (((1,), (1,)), ((), ())), preferred_element_type=F32)


def dot_nn(left, right):
    return lax.dot_general(left, right, (((1,), (0,)), ((), ())), preferred_element_type=F32)


def lane_index(shape):
    return lax.broadcasted_iota(jnp.int32, shape, len(shape) - 1)


def pick_two(lane, first, second):
    return jnp.where(lane < 64, first, second)


def pick_four(lane, a, b, c, d):
    return jnp.where(lane < 64, jnp.where(lane < 32, a, b), jnp.where(lane < 96, c, d))


def turn(tile, groups):
    return tile if groups % 4 == 0 else pltpu.roll(tile, RANK_LEAF * (groups % 4), 1)


def rows_of(first):
    return pl.ds(pl.multiple_of(first, VECTORS), VECTORS)


def up_kernel(
    charges_hbm,
    basis_hbm,
    leaf_hbm,
    mid_hbm,
    top_hbm,
    packed_hbm,
    message_hbm,
    local_hbm,
    charges,
    basis,
    leaf_transfer,
    mid_transfer,
    coefficients,
    message,
    parents,
    local,
    sem,
    out_sem,
    parent_sem,
):
    device = lax.axis_index("clusters")
    copies = [
        pltpu.make_async_copy(a, b, sem.at[i])
        for i, (a, b) in enumerate(
            (
                (charges_hbm, charges),
                (basis_hbm, basis),
                (leaf_hbm, leaf_transfer),
                (mid_hbm, mid_transfer),
            )
        )
    ]
    for copy in copies:
        copy.start()
    parent_copies = []
    for level in range(LEVELS):
        start = BOXES - (BOXES >> level)
        parent_copies.append(
            pltpu.make_async_copy(
                top_hbm.at[start + (device >> (level + 1))],
                parents.at[level],
                parent_sem.at[level],
            )
        )
        parent_copies[level].start()
    lane = lane_index((VECTORS, LANES))
    wide_lane = lane_index((VECTORS, 4 * CAPACITY)) // CAPACITY
    copies[0].wait()
    charges_out = pltpu.make_async_copy(
        charges, packed_hbm.at[:, pl.ds(0, POINTS)], out_sem.at[0]
    )
    charges_out.start()
    copies[1].wait()
    for copy in parent_copies:
        copy.wait()
    local[:, pl.ds(0, POINTS)] = charges[...]
    for level in range(LEVELS):
        for i in range(RANK // VECTORS):
            at = WIDE + (level * (RANK // VECTORS) + i) * LANES
            local[:, pl.ds(at, LANES)] = parents[level, i * VECTORS : (i + 1) * VECTORS, :]
    tiles = []
    for first in range(0, LEAVES // 4, 8):
        rows, weights = [], []
        for g in range(first, first + 8):
            span = pl.ds(g * 4 * CAPACITY, 4 * CAPACITY)
            x = charges[:, span].astype(F32)
            rows += [jnp.where(wide_lane == j, x, 0.0) for j in range(4)]
            weights.append(basis[:, span])
        result = dot_nt(
            jnp.concatenate(rows, axis=0).astype(BF16), jnp.concatenate(weights, axis=0)
        )
        for g in range(8):
            tile = result[32 * g : 32 * (g + 1), (g // 4) * LANES : (g // 4 + 1) * LANES]
            tiles.append(
                pick_four(lane, *[turn(tile[8 * j : 8 * (j + 1)], j - g % 4) for j in range(4)])
            )
    for g in range(LEAVES // 4):
        coefficients[:, pl.ds(g * LANES, LANES)] = tiles[g].astype(BF16)
    stacked = jnp.concatenate(
        [jnp.concatenate([tiles[2 * c], tiles[2 * c + 1]], axis=1) for c in range(GROUPS)], axis=0
    ).astype(BF16)
    copies[2].wait()
    result = dot_nt(stacked, leaf_transfer[...].reshape(GROUPS * RANK, CHILDREN * RANK_LEAF))
    mid = []
    for h in range(GROUPS // 2):
        span = slice(h * LANES, (h + 1) * LANES)
        low = result[16 * h : 16 * h + 8, span]
        high = result[16 * h + 8 : 16 * h + 16, span]
        mid.append(pick_two(lane, low, high).astype(BF16))
        coefficients[:, pl.ds(LEAF_LANES + h * LANES, LANES)] = mid[h]
    coefficients_out = pltpu.make_async_copy(
        coefficients, packed_hbm.at[:, pl.ds(POINTS, LEAF_LANES + MID_LANES)], out_sem.at[1]
    )
    coefficients_out.start()
    local[:, pl.ds(POINTS, LEAF_LANES + MID_LANES)] = coefficients[...]
    local_out = pltpu.make_async_copy(local, local_hbm, parent_sem.at[LEVELS])
    local_out.start()
    copies[3].wait()
    box = dot_nt(jnp.concatenate(mid, axis=1), mid_transfer[0])
    box = jnp.concatenate([box[:4], box[4:]], axis=1)
    box = jnp.concatenate([box, box], axis=0).astype(BF16)
    message[...] = jnp.broadcast_to(box[None], message.shape)
    messages_out = [
        pltpu.make_async_copy(
            message, message_hbm.at[pl.ds(i * MESSAGES, MESSAGES)], out_sem.at[2 + i]
        )
        for i in range(BOXES // 2 // MESSAGES)
    ]
    for copy in messages_out:
        copy.start()
    charges_out.wait()
    coefficients_out.wait()
    local_out.wait()
    for copy in messages_out:
        copy.wait()


def side_kernel(
    near_source_hbm,
    near_target_hbm,
    near_count_hbm,
    far_source_hbm,
    mid_source_hbm,
    own_hbm,
    pair_hbm,
    other_hbm,
    far,
    mid_coupling,
    top_coupling_hbm,
    box_coupling_hbm,
    near_hbm,
    field_hbm,
    coupling_hbm,
    near_source,
    near_target,
    far_source,
    mid_source,
    own,
    pair,
    other,
    top_coupling,
    box_coupling,
    near,
    field,
    coupling,
    x_low,
    x_high,
    leaf_table,
    mid_table,
    acc0,
    acc1,
    acc2,
    acc3,
    chosen_low,
    chosen_high,
    source_rows,
    target_rows,
    far_rows,
    mid_rows,
    near_count,
    near_from,
    near_to,
    far_from,
    mid_from,
    near_sem,
    sem,
    index_sem,
    out_sem,
):
    device = lax.axis_index("clusters")

    def near_copy(k):
        return pltpu.make_async_copy(
            near_hbm.at[:, pl.ds(pl.multiple_of(k * PART, PART), PART)], near.at[k], near_sem.at[k]
        )

    copies = [
        pltpu.make_async_copy(a, b, sem.at[i])
        for i, (a, b) in enumerate(
            (
                (near_count_hbm, near_count),
                (near_source_hbm, near_source),
                (near_target_hbm, near_target),
                (far_source_hbm, far_source),
                (mid_source_hbm, mid_source),
                (own_hbm, own),
                (pair_hbm, pair),
                (other_hbm, other),
                (box_coupling_hbm, box_coupling),
                (top_coupling_hbm, top_coupling),
            )
        )
    ]
    for copy in copies[:8]:
        copy.start()
    copies[9].start()
    near_copy(0).start()
    copies[8].start()

    for copy in copies[:5]:
        copy.wait()
    live = near_count[0, 0]
    leaf_base = (device - 1) * LEAVES
    shape = (VECTORS, LANES)
    slot = lax.broadcasted_iota(jnp.int32, shape, 0) * LANES + lane_index(shape)
    used = slot < live
    source_rows[...] = jnp.where(used, near_source[...] - leaf_base, LEAVES) * VECTORS
    target_rows[...] = jnp.where(used, near_target[...], LEAVES) * VECTORS
    far_rows[...] = (far_source[...] - leaf_base) * VECTORS
    mid_rows[...] = (mid_source[...] - (device - 1) * GROUPS) * VECTORS
    index_copies = [
        pltpu.make_async_copy(a, b, index_sem.at[i])
        for i, (a, b) in enumerate(
            (
                (source_rows, near_from),
                (target_rows, near_to),
                (far_rows, far_from),
                (mid_rows, mid_from),
            )
        )
    ]
    for copy in index_copies:
        copy.start()
    blocks = jnp.clip((live + BLOCK - 1) // BLOCK, 1, PARTS)

    lane = lane_index((VECTORS, LANES))
    zero = jnp.zeros((VECTORS, LANES), F32)
    odd = device % 2
    accumulators = (acc0, acc1, acc2, acc3)
    for acc in accumulators:
        acc[...] = jnp.zeros(acc.shape, F32)
    for copy in copies[5:8]:
        copy.wait()
    for source, region in ((own, 1), (pair, (1 - odd) * 2), (other, odd * 2)):
        base = region * LEAVES * VECTORS
        for h in range(LEAVES // 2):
            tile = source[:, pl.ds(h * LANES, LANES)].astype(F32)
            turned = pltpu.roll(tile, 64, 1)
            at = base + 2 * h * VECTORS
            x_low[rows_of(at), :] = pick_two(lane, tile, zero)
            x_high[rows_of(at), :] = pick_two(lane, zero, turned)
            x_low[rows_of(at + VECTORS), :] = pick_two(lane, turned, zero)
            x_high[rows_of(at + VECTORS), :] = pick_two(lane, zero, tile)
        for h in range(LEAVES // 4):
            tile = source[:, pl.ds(POINTS + h * LANES, LANES)].astype(F32)
            turns = [tile] + [pltpu.roll(tile, 32 * i, 1) for i in range(1, 4)]
            for j in range(4):
                leaf_table[rows_of(base + (4 * h + j) * VECTORS), :] = pick_four(
                    lane, *[turns[(group - j) % 4] for group in range(4)]
                )
        base = region * GROUPS * VECTORS
        for h in range(GROUPS // 2):
            tile = source[:, pl.ds(POINTS + LEAF_LANES + h * LANES, LANES)].astype(F32)
            turned = pltpu.roll(tile, 64, 1)
            at = base + 2 * h * VECTORS
            mid_table[rows_of(at), :] = pick_two(lane, tile, turned)
            mid_table[rows_of(at + VECTORS), :] = pick_two(lane, turned, tile)
    for copy in index_copies:
        copy.wait()

    @pl.when(blocks > 1)
    def _():
        near_copy(1).start()

    square = (RANK, RANK)
    product = (
        lax.broadcasted_iota(jnp.int32, square, 0) == lax.broadcasted_iota(jnp.int32, square, 1)
    ).astype(F32)
    products = []
    for level in range(LEVELS):
        at = WIDE + level * RANK * LANES // VECTORS
        parent = jnp.concatenate(
            [own[:, pl.ds(at + i * LANES, LANES)].astype(F32) for i in range(RANK // VECTORS)],
            axis=0,
        )
        own_half = jnp.where(
            ((device >> level) & 1) == 1, pltpu.roll(parent, RANK, 1), parent
        )[:, :RANK]
        product = dot_nt(product.astype(BF16), own_half.astype(BF16))
        products.append(product.astype(BF16))

    for group in range(LEAVES // 8):
        rows = []
        for i in range(8):
            leaf = group * 8 + i
            rows.append(
                jnp.concatenate(
                    [
                        pick_four(
                            lane,
                            *[leaf_table[rows_of(far_from[4 * q + m, leaf]), :] for m in range(4)],
                        )
                        for q in range(FAR // 4)
                    ],
                    axis=1,
                )
            )
        result = dot_nt(
            jnp.concatenate(rows, axis=0).astype(BF16),
            far[group * 8 : group * 8 + 8].reshape(8 * RANK_LEAF, FAR * RANK_LEAF),
        )
        for h in range(2):
            field[LEAF_AT + group * 2 + h] = pick_four(
                lane,
                *[
                    result[(4 * h + j) * 8 : (4 * h + j + 1) * 8, h * LANES : (h + 1) * LANES]
                    for j in range(4)
                ],
            )
    rows = []
    for c in range(GROUPS):
        rows.append(
            jnp.concatenate(
                [
                    pick_two(
                        lane,
                        mid_table[rows_of(mid_from[c, 2 * q]), :],
                        mid_table[rows_of(mid_from[c, 2 * q + 1]), :],
                    )
                    for q in range(MID_FAR // 2)
                ],
                axis=1,
            )
        )
    result = dot_nt(
        jnp.concatenate(rows, axis=0).astype(BF16),
        mid_coupling[...].reshape(GROUPS * RANK, MID_FAR * RANK),
    )
    for h in range(GROUPS // 2):
        span = slice(h * LANES, (h + 1) * LANES)
        field[MID_AT + h] = pick_two(
            lane, result[16 * h : 16 * h + 8, span], result[16 * h + 8 : 16 * h + 16, span]
        )
    @pl.when(blocks > 2)
    def _():
        near_copy(2).start()

    copies[9].wait()

    @pl.when(blocks > 3)
    def _():
        near_copy(3).start()

    level = lax.broadcasted_iota(jnp.int32, (VECTORS, LANES), 0) + 1
    column = BOXES - lax.shift_right_logical(jnp.full_like(level, BOXES), level - 1)
    column = column + lax.shift_right_logical(jnp.full_like(level, 1) * device, level)
    wanted = (lane_index(level.shape) == column).astype(F32)
    nothing = jnp.zeros_like(wanted)
    wanted = jnp.concatenate(
        [
            jnp.concatenate([wanted, nothing], axis=1),
            jnp.concatenate([nothing, wanted], axis=1),
        ],
        axis=0,
    ).astype(BF16)
    missing = jnp.zeros((3 * RANK, 4), BF16)
    for r in range(0, RANK, 2):
        columns = [
            jnp.concatenate([top_coupling[r + i], missing], axis=1) for i in range(2)
        ]
        result = dot_nt(wanted, jnp.concatenate(columns, axis=1))
        rows = slice(r * VECTORS, (r + 2) * VECTORS)
        chosen_low[rows, :] = result[:, :LANES]
        chosen_high[rows, 0:RANK] = result[:, LANES:]
    copies[8].wait()
    coupling[0] = box_coupling[0]
    for k in range(LEVELS):
        rows = pl.ds(k, RANK, stride=VECTORS)
        chosen = jnp.concatenate([chosen_low[rows, :], chosen_high[rows, :][:, :RANK]], axis=1)
        coupling[k + 1] = dot_nn(products[k], chosen.astype(BF16)).astype(BF16)
    coupling_out = pltpu.make_async_copy(coupling, coupling_hbm, out_sem.at[1])
    coupling_out.start()
    zeros_half = jnp.zeros((2 * VECTORS, LANES), BF16)

    def near_step(k, carry):
        near_copy(k).wait()
        sources = [near_from.at[2 * k + i] for i in range(2)]
        targets = [near_to.at[2 * k + i] for i in range(2)]
        for i in range(BLOCK // 16):
            rows, weights = [], []
            for g in range(4):
                first = 16 * i + 4 * g
                at = [rows_of(sources[first // LANES][first % LANES + j]) for j in range(4)]
                top = jnp.concatenate([x_low[at[0], :], x_high[at[1], :]], axis=0)
                bottom = jnp.concatenate([x_low[at[2], :], x_high[at[3], :]], axis=0)
                rows.append(jnp.concatenate([top.astype(BF16), zeros_half], axis=1))
                rows.append(jnp.concatenate([zeros_half, bottom.astype(BF16)], axis=1))
                weights.append(near[k, :, first * CAPACITY : (first + 4) * CAPACITY])
            result = dot_nt(jnp.concatenate(rows, axis=0), jnp.concatenate(weights, axis=0))
            for g in range(4):
                first = 16 * i + 4 * g
                for j in range(4):
                    to = rows_of(targets[first // LANES][first % LANES + j])
                    at = 32 * g + 8 * j
                    accumulators[g][to, :] += result[
                        at : at + 8, (g // 2) * LANES : (g // 2 + 1) * LANES
                    ]
        return carry

    lax.fori_loop(0, blocks, near_step, 0)
    for h in range(LEAVES // 2):
        low = rows_of(2 * h * VECTORS)
        high = rows_of((2 * h + 1) * VECTORS)
        placed = pick_two(lane, acc0[low, :] + acc2[low, :], acc1[high, :] + acc3[high, :])
        moved = pick_two(lane, acc0[high, :] + acc2[high, :], acc1[low, :] + acc3[low, :])
        field[h] = placed + pltpu.roll(moved, CAPACITY, 1)

    field_out = pltpu.make_async_copy(field, field_hbm, out_sem.at[0])
    field_out.start()

    field_out.wait()
    coupling_out.wait()


def down_kernel(
    every,
    top_hbm,
    coupling,
    mid_hbm,
    leaf_hbm,
    field,
    basis_hbm,
    out,
    top_transfer,
    mid_transfer,
    leaf_transfer,
    basis,
    sem,
    pairs0,
    pairs1,
    pairs2,
    pairs3,
    pairs4,
    pairs5,
):
    quarter = pl.ds(0, BOXES // 4)
    half = pl.ds(BOXES // 4, BOXES // 4)
    rest = pl.ds(BOXES // 2, BOXES // 2 - 4)
    copies = [
        pltpu.make_async_copy(source, target, sem.at[i])
        for i, (source, target) in enumerate(
            (
                (mid_hbm, mid_transfer),
                (leaf_hbm, leaf_transfer),
                (basis_hbm, basis),
                (top_hbm.at[quarter], top_transfer.at[quarter]),
                (top_hbm.at[half], top_transfer.at[half]),
                (top_hbm.at[rest], top_transfer.at[rest]),
            )
        )
    ]
    for copy in copies[3:] + copies[:3]:
        copy.start()
    device = lax.axis_index("clusters")
    lane = lane_index((VECTORS, LANES))
    zero = jnp.zeros((VECTORS, LANES), F32)
    empty = jnp.zeros((2 * VECTORS, LANES), BF16)

    pairs = (pairs0, pairs1, pairs2, pairs3, pairs4, pairs5)
    for level in range(LEVELS + 1):
        pairs[level][0] = zero
        pairs[level][(BOXES >> (level + 1)) + 1] = zero
    kept = (lane < RANK) == (lax.broadcasted_iota(jnp.int32, (VECTORS, LANES), 0) < 4)
    for p in range(BOXES // 2):
        tile = every[p].astype(F32)
        pairs0[p + 1] = jnp.where(kept, tile, pltpu.roll(pltpu.roll(tile, RANK, 1), 4, 0))
    for level in range(LEVELS):
        if level == 1:
            copies[5].wait()
        start = BOXES - (BOXES >> level)
        count = BOXES >> (level + 1)
        for g in range(0, count, 8):
            if level == 0 and g % (BOXES // 4) == 0:
                copies[3 + g // (BOXES // 4)].wait()
            left, right = [], []
            for quad in range(g, min(g + 8, count), 4):
                low = jnp.concatenate([pairs[level][1 + quad], pairs[level][2 + quad]], axis=0)
                high = jnp.concatenate([pairs[level][3 + quad], pairs[level][4 + quad]], axis=0)
                left.append(jnp.concatenate([low.astype(BF16), empty], axis=1))
                left.append(jnp.concatenate([empty, high.astype(BF16)], axis=1))
                at = start + quad
                right.append(jnp.concatenate([top_transfer[at], top_transfer[at + 2]], axis=1))
                right.append(jnp.concatenate([top_transfer[at + 1], top_transfer[at + 3]], axis=1))
            result = dot_nt(jnp.concatenate(left, axis=0), jnp.concatenate(right, axis=0))
            for i in range(len(left)):
                span = slice((i // 2) * LANES, (i // 2 + 1) * LANES)
                pairs[level + 1][1 + g // 2 + i] = pick_two(
                    lane, result[16 * i : 16 * i + 8, span], result[16 * i + 8 : 16 * i + 16, span]
                )
    down = jnp.zeros((VECTORS, RANK), F32)
    for level in range(LEVELS + 1):
        cluster = device >> level
        parent = cluster >> 1
        before = pairs[level][parent]
        after = pltpu.roll(pairs[level][parent + 2], 64, 1)
        middle = jnp.where((cluster & 1) == 1, before, after)
        stacked = jnp.concatenate([pick_two(lane, before, middle), after[:, :64]], axis=1)
        down = down + dot_nt(stacked.astype(BF16), coupling[level])

    copies[0].wait()
    mid_push = dot_nn(down.astype(BF16), mid_transfer[0])
    copies[1].wait()
    rows = []
    for c in range(GROUPS):
        h = c // 2
        tile = field[MID_AT + h] + mid_push[:, h * LANES : (h + 1) * LANES]
        half_tile = pick_two(lane, tile, zero) if c % 2 == 0 else pick_two(lane, zero, tile)
        rows.append(
            jnp.concatenate([half_tile if i == h else zero for i in range(GROUPS // 2)], axis=1)
        )
    leaf_push = dot_nn(
        jnp.concatenate(rows, axis=0).astype(BF16),
        leaf_transfer[...].reshape(GROUPS * RANK, CHILDREN * RANK_LEAF),
    )
    copies[2].wait()
    lane_group = lane // RANK_LEAF
    for first in range(0, LEAVES // 4, 8):
        rows, weights = [], []
        for g in range(first, first + 8):
            push = leaf_push[(g // 2) * 8 : (g // 2) * 8 + 8, (g % 2) * LANES : (g % 2 + 1) * LANES]
            leaf_down = field[LEAF_AT + g] + push
            for j in range(4):
                block = jnp.where(lane_group == g % 4, turn(leaf_down, g % 4 - j), 0.0)
                rows.append(
                    jnp.concatenate([block, zero] if g % 8 < 4 else [zero, block], axis=1)
                )
            weights.append(basis[:, pl.ds(g * 4 * CAPACITY, 4 * CAPACITY)])
        result = dot_nn(
            jnp.concatenate(rows, axis=0).astype(BF16), jnp.concatenate(weights, axis=0)
        )
        for g in range(first, first + 8):
            for h in range(2):
                span = slice(h * LANES, (h + 1) * LANES)
                at = 32 * (g % 8) + 16 * h
                far_tile = pick_two(lane, result[at : at + 8, span], result[at + 8 : at + 16, span])
                out[:, pl.ds((2 * g + h) * LANES, LANES)] = (far_tile + field[2 * g + h]).astype(
                    BF16
                )


def up_call(*operands):
    hbm, shape, scratch = HBM, jax.ShapeDtypeStruct, pltpu.VMEM
    dma = pltpu.SemaphoreType.DMA
    return pl.pallas_call(
        up_kernel,
        out_shape=(
            shape((VECTORS, WIDE), BF16),
            shape((BOXES // 2, VECTORS, LANES), BF16),
            shape((VECTORS, LOCAL), BF16),
        ),
        in_specs=[hbm] * 5,
        out_specs=(hbm, hbm, hbm),
        scratch_shapes=[
            scratch((VECTORS, POINTS), BF16),
            scratch((RANK_LEAF, POINTS), BF16),
            scratch((GROUPS, RANK, CHILDREN * RANK_LEAF), BF16),
            scratch((1, RANK, GROUPS * RANK), BF16),
            scratch((VECTORS, LEAF_LANES + MID_LANES), BF16),
            scratch((MESSAGES, VECTORS, LANES), BF16),
            scratch((LEVELS, RANK, 2 * RANK), BF16),
            scratch((VECTORS, LOCAL), BF16),
            dma((4,)),
            dma((2 + BOXES // 2 // MESSAGES,)),
            dma((LEVELS + 1,)),
        ],
        cost_estimate=pl.CostEstimate(flops=10**9, bytes_accessed=10**6, transcendentals=0),
        compiler_params=pltpu.CompilerParams(vmem_limit_bytes=UP_LIMIT),
        name="upward",
    )(*operands)


def side_call(
    near_source,
    near_target,
    near_count,
    far_source,
    mid_source,
    local,
    packed_pair,
    packed_other,
    far_coupling,
    mid_coupling,
    top_coupling,
    box_coupling,
    near_blocks,
):
    hbm, shape, scratch = HBM, jax.ShapeDtypeStruct, pltpu.VMEM
    dma = pltpu.SemaphoreType.DMA
    table = scratch((3 * LEAVES * VECTORS, LANES), F32)
    accumulator = scratch(((LEAVES + 1) * VECTORS, LANES), F32)
    indices = [
        (VECTORS, LANES),
        (VECTORS, LANES),
        (FAR, LEAVES),
        (GROUPS, MID_FAR),
    ]
    wide = scratch((VECTORS, WIDE), BF16)
    return pl.pallas_call(
        side_kernel,
        out_shape=(
            shape((FIELDS, VECTORS, LANES), F32),
            shape((LEVELS + 1, RANK, 3 * RANK), BF16),
        ),
        in_specs=[hbm] * 8 + [pl.BlockSpec(memory_space=pltpu.VMEM)] * 2 + [hbm] * 3,
        out_specs=(hbm, hbm),
        scratch_shapes=[scratch(i, jnp.int32) for i in indices]
        + [
            scratch((VECTORS, LOCAL), BF16),
            wide,
            wide,
            scratch((RANK, 3 * RANK, BOXES - 4), BF16),
            scratch((1, RANK, 3 * RANK), BF16),
            scratch((PARTS, CAPACITY, PART), BF16),
            scratch((FIELDS, VECTORS, LANES), F32),
            scratch((LEVELS + 1, RANK, 3 * RANK), BF16),
            table,
            table,
            table,
            scratch((3 * GROUPS * VECTORS, LANES), F32),
            accumulator,
            accumulator,
            accumulator,
            accumulator,
            scratch((RANK * VECTORS, LANES), F32),
            scratch((RANK * VECTORS, LANES), F32),
        ]
        + [scratch(i, jnp.int32) for i in indices]
        + [pltpu.SMEM((1, 1), jnp.int32)]
        + [pltpu.SMEM(i, jnp.int32) for i in indices]
        + [dma((PARTS,)), dma((10,)), dma((4,)), dma((2,))],
        cost_estimate=pl.CostEstimate(flops=2 * 10**9, bytes_accessed=10**7, transcendentals=0),
        compiler_params=pltpu.CompilerParams(vmem_limit_bytes=SIDE_LIMIT),
        name="side",
    )(
        near_source.reshape(VECTORS, LANES),
        near_target.reshape(VECTORS, LANES),
        near_count.reshape(1, 1),
        far_source.T,
        mid_source,
        local,
        packed_pair,
        packed_other,
        far_coupling,
        mid_coupling,
        jnp.transpose(top_coupling, (1, 2, 0)),
            box_coupling,
        near_blocks,
    )


def down_call(*operands):
    hbm, shape, scratch = HBM, jax.ShapeDtypeStruct, pltpu.VMEM
    dma = pltpu.SemaphoreType.DMA
    vmem = pl.BlockSpec(memory_space=pltpu.VMEM)
    return pl.pallas_call(
        down_kernel,
        out_shape=shape((VECTORS, POINTS), BF16),
        in_specs=[vmem, hbm, vmem, hbm, hbm, vmem, hbm],
        out_specs=pl.BlockSpec(memory_space=pltpu.VMEM),
        scratch_shapes=[
            scratch((BOXES - 4, RANK, 2 * RANK), BF16),
            scratch((1, RANK, GROUPS * RANK), BF16),
            scratch((GROUPS, RANK, CHILDREN * RANK_LEAF), BF16),
            scratch((RANK_LEAF, POINTS), BF16),
            dma((6,)),
        ]
        + [
            scratch(((BOXES >> (level + 1)) + 2, VECTORS, LANES), F32)
            for level in range(LEVELS + 1)
        ],
        cost_estimate=pl.CostEstimate(flops=10**9, bytes_accessed=10**6, transcendentals=0),
        compiler_params=pltpu.CompilerParams(vmem_limit_bytes=DOWN_LIMIT),
        name="down",
    )(*operands)


def body(
    charges,
    leaf_basis,
    leaf_transfer,
    mid_transfer,
    far_source,
    far_coupling,
    mid_source,
    mid_coupling,
    box_coupling,
    top_transfer,
    top_coupling,
    near_target,
    near_source,
    near_count,
    near_blocks,
):
    pair = [(i, i ^ 1) for i in range(BOXES)]
    other = [(i, min(max(((i + 1) ^ 1) - 1, 0), BOXES - 1)) for i in range(BOXES)]
    packed, message, local = up_call(
        charges, leaf_basis, leaf_transfer, mid_transfer, top_transfer
    )
    packed_other = lax.ppermute(packed, "clusters", other)
    packed_pair = lax.ppermute(packed, "clusters", pair)
    every = lax.all_to_all(message.reshape(BOXES, VECTORS // 2, LANES), "clusters", 0, 0)
    field, coupling = side_call(
        near_source,
        near_target,
        near_count,
        far_source,
        mid_source,
        local,
        packed_pair,
        packed_other,
        far_coupling,
        mid_coupling,
        top_coupling,
        box_coupling,
        near_blocks,
    )
    return down_call(
        every.reshape(BOXES // 2, VECTORS, LANES),
        top_transfer,
        coupling,
        mid_transfer,
        leaf_transfer,
        field,
        leaf_basis,
    )


def solution(mesh):
    in_specs = (
        P(None, "clusters"),
        P(None, "clusters"),
        P("clusters", None, None),
        P("clusters", None, None),
        P("clusters", None),
        P("clusters", None, None),
        P("clusters", None),
        P("clusters", None, None),
        P("clusters", None, None),
        P(),
        P(),
        P("clusters"),
        P("clusters"),
        P("clusters"),
        P(None, "clusters"),
    )
    out_specs = P(None, "clusters")
    return jax.shard_map(body, mesh=mesh, in_specs=in_specs, out_specs=out_specs, check_vma=False)
```
